32 devices in a mesh: tm: 16 (over z, x, core), space: 2 (over y).
Axes of the slice: x: 2, y: 2, z: 4, core: 2. Of those that a mesh axis runs over, the one named last changes fastest.
Arguments:
- fine_nodes: float32 [16, 3, 3, 32, 4096], P('tm', None, None, 'space'), may hold values from -6 to 6
- init_state: float32 [3, 32, 4096], P(None, 'space'), may hold values from -6 to 6
- mean_depth: float32 [32, 4096], P('space'), may hold values from 0.5 to 2
Outputs:
- new_nodes: float32 [16, 3, 3, 32, 4096], P('tm', None, None, 'space')
The draws below stay inside these ranges and needn't reach their ends.
All inputs are finite; a program needn't handle non-finite values.
Results may differ from the reference program's by a relative error of at most 0.00002.
Values sent between devices are 32-bit elements; how exact they have to be, the bound alone decides.
A program may use at most 64 MiB of HBM per device.

```python
import math
import jax
import jax.numpy as jnp
from jax import lax

NX = 4096
NODES = 3
FIELDS = 3
NY = 32
SLICES = 16


def steps_of(rng, shape, pieces, least, largest):
    level, own = 1.0, jax.random.fold_in(rng, 6)
    for position, parts in pieces:
        heights = jnp.exp(jax.random.uniform(jax.random.fold_in(own, position), (parts,), jnp.float32, least / len(pieces), largest / len(pieces)))
        level = level * jnp.repeat(heights, shape[position] // parts).reshape([-1 if axis == position else 1 for axis in range(len(shape))])
    return level


def noise(key, extent, scale, limit, split=(), held_as=jnp.bfloat16):
    array = scale * jax.random.normal(key, extent, jnp.float32)
    if split:
        array = array * steps_of(key, extent, split, -0.22, 0.18)
    return jnp.clip(array, -limit, limit).astype(held_as)


def setup_inputs(seed: int = 0) -> dict:
    seeds = jax.random.split(jax.random.key(seed), 4)
    return {
        "fine_nodes": noise(seeds[0], (SLICES, NODES, FIELDS, NY, NX), 1.0, 6.0, ((0, 16), (3, 2)), jnp.float32),
        "init_state": noise(seeds[1], (FIELDS, NY, NX), 1.0, 6.0, ((1, 2),), jnp.float32),
        "mean_depth": jnp.clip(jnp.exp(math.log(2.0) - 1.3862944 * jax.random.uniform(seeds[2], (NY, NX), jnp.float32) ** steps_of(seeds[2], (NY, NX), ((0, 2),), -0.2, 0.2)), 0.5, 2.0),
    }


step_size = 0.3
viscosity = 1.0 / 3.0
coriolis = 0.5
quad_near = 5.0 / 24.0
quad_mid = 1.0 / 3.0
quad_far = -1.0 / 24.0


def column_slope(values):
    return (jnp.roll(values, -1, -1) - jnp.roll(values, 1, -1)) * 0.5


def row_slope(values):
    return (values[..., 2:, :] - values[..., :-2, :]) * 0.5


def diffuse(values, centre):
    return values[..., 2:, :] + values[..., :-2, :] + jnp.roll(centre, -1, -1) + jnp.roll(centre, 1, -1) - 4.0 * centre


def tendency(padded, depth_rows):
    height = padded[..., 0, :, :]
    east_flow = padded[..., 1, :, :]
    north_flow = padded[..., 2, :, :]
    centre = padded[..., 1:-1, :]
    height_c = centre[..., 0, :, :]
    east_c = centre[..., 1, :, :]
    north_c = centre[..., 2, :, :]
    depth_c = depth_rows[1:-1]
    height_rate = -column_slope(depth_c * east_c) - row_slope(depth_rows * north_flow) + viscosity * diffuse(height, height_c)
    east_rate = -column_slope(height_c) + coriolis * north_c + viscosity * diffuse(east_flow, east_c)
    north_rate = -row_slope(height) - coriolis * east_c + viscosity * diffuse(north_flow, north_c)
    return jnp.stack([height_rate, east_rate, north_rate], axis=-3)


def padded_rows(values):
    return jnp.concatenate([values[..., -1:, :], values, values[..., :1, :]], axis=-2)


def full_rate(values, mean_depth):
    return tendency(padded_rows(values), padded_rows(mean_depth))


def reference(fine_nodes, init_state, mean_depth):
    half_step = step_size * 0.5
    starts = jnp.concatenate([init_state[None], fine_nodes[:-1, 2]], axis=0)
    first_flags = jnp.arange(fine_nodes.shape[0], dtype=jnp.int32) == 0

    def slice_work(slice_items):
        points, section_zero, is_first = slice_items
        old_rates = full_rate(points, mean_depth)
        rate_zero = full_rate(section_zero, mean_depth)
        section_one = section_zero + half_step * (rate_zero - old_rates[0]) + step_size * (quad_near * old_rates[0] + quad_mid * old_rates[1] + quad_far * old_rates[2])
        rate_one = full_rate(section_one, mean_depth)
        section_two = section_one + half_step * (rate_one - old_rates[1]) + step_size * (quad_far * old_rates[0] + quad_mid * old_rates[1] + quad_near * old_rates[2])
        rate_two = full_rate(section_two, mean_depth)
        fas_term = -(step_size / 3.0) * (rate_zero - 2.0 * rate_one + rate_two)
        drift_total = half_step * (rate_two - rate_zero) + fas_term
        boosted = drift_total + jnp.where(is_first, section_zero + step_size * rate_zero, 0.0)
        return section_one, section_two, boosted

    section_ones, section_twos, boosts = lax.map(slice_work, (fine_nodes, starts, first_flags))

    def chain_turn(current, boosted):
        updated = boosted + (current + step_size * full_rate(current, mean_depth))
        return updated, updated

    _, coarse_end = lax.scan(chain_turn, jnp.zeros_like(init_state), boosts)
    coarse_begin = jnp.concatenate([init_state[None], coarse_end[:-1]], axis=0)
    middle = section_ones + 0.5 * ((coarse_begin - starts) + (coarse_end - section_twos))
    return jnp.stack([coarse_begin, middle, coarse_end], axis=1)
```

```python
import functools

import jax
import jax.numpy as jnp
from jax import lax
from jax.experimental import pallas as pl
from jax.experimental.pallas import tpu as pltpu
from jax.sharding import PartitionSpec as P

MESH = pl.DeviceIdType.MESH
DT = 0.3
NU = 1.0 / 3.0
FC = 0.5
LANES = 128
GROUPS = 4


def shift_left(v):
    return pltpu.roll(v, v.shape[1] - 1, 1)


def shift_right(v):
    return pltpu.roll(v, 1, 1)


def shift_up(v):
    return pltpu.roll(v, v.shape[0] - 1, 0)


def shift_down(v):
    return pltpu.roll(v, 1, 0)


def row_terms(h, e, n, depth):
    dn = 0.5 * (depth * n)
    nh, ne, nn, hh = NU * h, NU * e, NU * n, 0.5 * h
    return (nh - dn, ne, nn - hh), (nh + dn, ne, nn + hh)


def column_terms(h, e, n, depth):
    de = 0.5 * (depth * e)
    nh, ne, nn, hh = NU * h, NU * e, NU * n, 0.5 * h
    return (
        shift_left(nh - de) + shift_right(nh + de) - 4.0 * nh,
        shift_left(ne - hh) + shift_right(ne + hh) - 4.0 * ne + FC * n,
        shift_left(nn) + shift_right(nn) - 4.0 * nn - FC * e,
    )


def kernel(
    cfg, u_hbm, init_hbm, depth_hbm, out_ref, u_ref, init_ref, depth_ref,
    s0, g, s1, mid, b, halo_src, dsrc, dep, isrc, ini, main, halo, cs, ce, cb, esrc, edst, cin, chalo, chalo_src, state,
    shift_s, shift_r, edge_s, edge_r, dep_s, dep_r, ini_s, ini_r, a2a_s, a2a_r, ret_s, ret_r, fwd_s, fwd_r,
    c_s, c_r, beg_s, beg_r, in_s,
):
    T, SP, RL, NX, W, K, stride, hw, per, nh, NG = cfg
    TG = T // NG
    p, y = lax.axis_index("tm"), lax.axis_index("space")
    me = p * SP + y
    total = T * SP
    block = p // TG
    pb = p - block * TG
    local = pb * SP + y
    mine = local // stride
    is_owner = lax.rem(local, stride) == 0
    even = lax.rem(p, 2) == 0

    def where(flat):
        return (flat // SP, lax.rem(flat, SP))

    barrier = pltpu.get_barrier_semaphore()

    @pl.loop(1, total)
    def _(i):
        pl.semaphore_signal(barrier, inc=1, device_id=where(lax.rem(me + i, total)), device_id_type=MESH)

    loads = [pltpu.make_async_copy(u_hbm.at[0, i], u_ref.at[i], in_s.at[i]) for i in (2, 0, 1)]
    loads.append(pltpu.make_async_copy(depth_hbm, depth_ref, in_s.at[3]))
    loads.append(pltpu.make_async_copy(init_hbm, init_ref, in_s.at[4]))
    for copy in loads:
        copy.start()
    loads[0].wait()
    pl.semaphore_wait(barrier, total - 1)

    shift = pltpu.make_async_remote_copy(
        src_ref=u_ref.at[2], dst_ref=s0, send_sem=shift_s, recv_sem=shift_r,
        device_id=(lax.rem(p + 1, T), y), device_id_type=MESH,
    )

    @pl.when(p < T - 1)
    def _():
        shift.start()

    for copy in loads[1:]:
        copy.wait()

    lane_h = lax.broadcasted_iota(jnp.int32, (RL, LANES), 1)

    def dep_copy(yo):
        return pltpu.make_async_remote_copy(
            src_ref=dsrc.at[yo], dst_ref=dep.at[pl.ds(pl.multiple_of(y * RL, 8), RL)],
            send_sem=dep_s.at[yo], recv_sem=dep_r, device_id=(p, yo), device_id_type=MESH,
        )

    def ini_copy(yo):
        return pltpu.make_async_remote_copy(
            src_ref=isrc.at[yo], dst_ref=ini.at[:, pl.ds(pl.multiple_of(y * RL, 8), RL)],
            send_sem=ini_s.at[yo], recv_sem=ini_r, device_id=(p, yo), device_id_type=MESH,
        )

    for yo in range(SP):
        flat = pb * SP + yo
        k = flat // stride

        @pl.when(lax.rem(flat, stride) == 0)
        def _():
            here = depth_ref[:, pl.ds(pl.multiple_of(k * W, LANES), W)]
            after = depth_ref[:, pl.ds(pl.multiple_of(lax.rem((k + 1) * W, NX), LANES), LANES)]
            before = depth_ref[:, pl.ds(pl.multiple_of(lax.rem(k * W + NX - LANES, NX), LANES), LANES)]
            dsrc[yo, :, :W] = here
            dsrc[yo, :, W:] = jnp.where(lane_h < LANES // 2, after, before)

            @pl.when(yo != y)
            def _():
                dep_copy(yo).start()

            @pl.when(yo == y)
            def _():
                pltpu.make_async_copy(
                    dsrc.at[yo], dep.at[pl.ds(pl.multiple_of(y * RL, 8), RL)], dep_r
                ).start()

        @pl.when(jnp.logical_and(lax.rem(flat, stride) == 0, block == 0))
        def _():
            for f in range(3):
                after = init_ref[f, :, pl.ds(pl.multiple_of(lax.rem((k + 1) * W, NX), LANES), LANES)]
                before = init_ref[f, :, pl.ds(pl.multiple_of(lax.rem(k * W + NX - LANES, NX), LANES), LANES)]
                isrc[yo, f, :, :W] = init_ref[f, :, pl.ds(pl.multiple_of(k * W, LANES), W)]
                isrc[yo, f, :, W:] = jnp.where(lane_h < LANES // 2, after, before)

            @pl.when(yo != y)
            def _():
                ini_copy(yo).start()

            @pl.when(yo == y)
            def _():
                pltpu.make_async_copy(
                    isrc.at[yo], ini.at[:, pl.ds(pl.multiple_of(y * RL, 8), RL)], ini_r
                ).start()

    for f in range(3):
        g[f] = (-7.0 / 24.0) * u_ref[0, f] + (1.0 / 3.0) * u_ref[1, f] - (1.0 / 24.0) * u_ref[2, f]

    @pl.when(p > 0)
    def _():
        shift.wait_recv()

    @pl.when(p == 0)
    def _():
        s0[...] = init_ref[...]

    for f in range(3):
        g[f] = g[f] + 0.5 * s0[f]

    row = lax.broadcasted_iota(jnp.int32, (RL, NX), 0)

    def edge_copy(stage, side):
        to = lax.rem(y + SP - 1, SP) if side == 0 else lax.rem(y + 1, SP)
        return pltpu.make_async_remote_copy(
            src_ref=esrc.at[stage, side], dst_ref=edst.at[stage, side],
            send_sem=edge_s.at[stage, side], recv_sem=edge_r.at[stage, side],
            device_id=(p, to), device_id_type=MESH,
        )

    def rate_of_g(stage):
        up0, _ = row_terms(g[0, 0:1], g[1, 0:1], g[2, 0:1], depth_ref[0:1])
        _, down1 = row_terms(g[0, RL - 1 : RL], g[1, RL - 1 : RL], g[2, RL - 1 : RL], depth_ref[RL - 1 : RL])
        for f in range(3):
            esrc[stage, 0, f] = up0[f]
            esrc[stage, 1, f] = down1[f]
        for side in range(2):
            edge_copy(stage, side).start()
        h, e, n, depth = g[0], g[1], g[2], depth_ref[...]
        rates = column_terms(h, e, n, depth)
        ups, downs = row_terms(h, e, n, depth)
        for side in range(2):
            edge_copy(stage, side).wait_recv()
        return [
            rates[f]
            + jnp.where(row == RL - 1, edst[stage, 0, f], shift_up(ups[f]))
            + jnp.where(row == 0, edst[stage, 1, f], shift_down(downs[f]))
            for f in range(3)
        ]

    rates = rate_of_g(0)
    for f in range(3):
        s1[f] = s0[f] + DT * rates[f]
    for f in range(3):
        g[f] = (
            0.5 * s1[f]
            - (1.0 / 24.0) * u_ref[0, f] - (1.0 / 6.0) * u_ref[1, f] + (5.0 / 24.0) * u_ref[2, f]
        )
    rates = rate_of_g(1)
    for f in range(3):
        s2 = s1[f] + DT * rates[f]
        b[f] = (1.0 / 6.0) * s2 + (2.0 / 3.0) * s1[f] - (5.0 / 6.0) * s0[f]
        mid[f] = s1[f] - 0.5 * (s0[f] + s2)

    slot_of = lax.rem(lane_h + hw, LANES) // (2 * hw)
    for k in range(K):
        lo, hi = ((k + 1) % K) * W, (k * W - LANES) % NX
        packed = [jnp.zeros((RL, LANES), jnp.float32) for _ in range(nh)]
        for f in range(3):
            z = jnp.where(lane_h < LANES // 2, b[f, :, lo : lo + LANES], b[f, :, hi : hi + LANES])
            slot = f % per
            if slot:
                z = pltpu.roll(z, 2 * hw * slot, 1)
            packed[f // per] = jnp.where(slot_of == slot, z, packed[f // per])
        for i in range(nh):
            halo_src[i, :, k * LANES : (k + 1) * LANES] = packed[i]

    my_rows = pl.ds(pl.multiple_of(y * RL, 8), RL)

    def a2a(k):
        ends = (
            (b.at[:, :, pl.ds(pl.multiple_of(k * W, LANES), W)], main.at[pb, :, my_rows]),
            (halo_src.at[:, :, pl.ds(pl.multiple_of(k * LANES, LANES), LANES)], halo.at[pb, :, my_rows]),
        )
        there = [
            pltpu.make_async_remote_copy(
                src_ref=src, dst_ref=dst, send_sem=a2a_s.at[i], recv_sem=a2a_r.at[i, pb],
                device_id=where(block * TG * SP + k * stride), device_id_type=MESH,
            )
            for i, (src, dst) in enumerate(ends)
        ]
        here = [pltpu.make_async_copy(src, dst, a2a_r.at[i, pb]) for i, (src, dst) in enumerate(ends)]
        return there, here

    @pl.loop(0, K)
    def _(i):
        k = lax.rem(mine + i, K)
        there, here = a2a(k)

        @pl.when(k * stride != local)
        def _():
            for copy in there:
                copy.start()

        @pl.when(k * stride == local)
        def _():
            for copy in here:
                copy.start()

    my_tile = pl.ds(pl.multiple_of(mine * W, LANES), W)
    my_group = mine // (K // GROUPS)

    def give_back(t):
        for yo in range(SP):
            src, dst = cs.at[t * SP + yo], ce.at[:, :, my_tile]
            here = jnp.logical_and(t == pb, y == yo)

            @pl.when(jnp.logical_not(here))
            def _():
                pltpu.make_async_remote_copy(
                    src_ref=src, dst_ref=dst, send_sem=ret_s, recv_sem=ret_r.at[my_group],
                    device_id=(block * TG + t, yo), device_id_type=MESH,
                ).start()

            @pl.when(here)
            def _():
                pltpu.make_async_copy(src, dst, ret_r.at[my_group]).start()

    def give_begin(t, src):
        for yo in range(SP):
            dst = cb.at[:, :, my_tile]
            here = jnp.logical_and(t == pb, y == yo)

            @pl.when(jnp.logical_not(here))
            def _():
                pltpu.make_async_remote_copy(
                    src_ref=src.at[yo], dst_ref=dst, send_sem=beg_s.at[t * SP + yo], recv_sem=beg_r,
                    device_id=(block * TG + t, yo), device_id_type=MESH,
                ).start()

            @pl.when(here)
            def _():
                pltpu.make_async_copy(src.at[yo], dst, beg_r).start()

    def give(t):
        give_back(t)

        @pl.when(jnp.logical_and(lax.rem(t, 2) == 1, t < TG - 1))
        def _():
            give_begin(t + 1, cs.at[pl.ds(t * SP, SP)])

    def carry():
        ends = ((cs.at[pl.ds((TG - 1) * SP, SP)], cin), (chalo_src, chalo))
        return [
            pltpu.make_async_remote_copy(
                src_ref=src, dst_ref=dst, send_sem=c_s.at[i], recv_sem=c_r.at[i],
                device_id=(lax.rem(p + TG, T), y), device_id_type=MESH,
            )
            for i, (src, dst) in enumerate(ends)
        ]

    def unpack(tile, f):
        return pltpu.roll(tile, LANES - 2 * hw * (f % per), 1) if f % per else tile

    def whole(ref, sem):
        pltpu.make_async_copy(ref, ref, sem).wait()

    @pl.when(is_owner)
    def _():
        whole(dep, dep_r)
        depth = dep[...]

        def turn(t, cur):
            whole(main.at[t], a2a_r.at[0, t])
            whole(halo.at[t], a2a_r.at[1, t])
            h, e, n = (
                cur[f] + jnp.concatenate([main[t, f], unpack(halo[t, f // per], f)], axis=1) for f in range(3)
            )
            rates = column_terms(h, e, n, depth)
            ups, downs = row_terms(h, e, n, depth)
            new = []
            for f in range(3):
                value = cur[f] + DT * (rates[f] + shift_up(ups[f]) + shift_down(downs[f]))
                for yo in range(SP):
                    cs[t * SP + yo, f] = value[yo * RL : (yo + 1) * RL, :W]
                new.append(value)

            @pl.when(jnp.logical_and(t > 0, block == NG - 1))
            def _():
                give(t - 1)

            return tuple(new)

        @pl.when(block == 0)
        def _():
            whole(ini, ini_r)
            state[...] = ini[...]

        @pl.when(block > 0)
        def _():
            for copy in carry():
                copy.wait_recv()
            give_begin(0, cin)
            for f in range(3):
                for yo in range(SP):
                    state[f, yo * RL : (yo + 1) * RL, :W] = cin[yo, f]
                state[f, :, W:] = unpack(chalo[f // per], f)

        last = lax.fori_loop(0, TG, turn, tuple(state[f] for f in range(3)))

        @pl.when(block == NG - 1)
        def _():
            give(TG - 1)

        @pl.when(block < NG - 1)
        def _():
            lanes = lax.broadcasted_iota(jnp.int32, (SP * RL, LANES), 1)
            slots = lax.rem(lanes + hw, LANES) // (2 * hw)
            for i in range(nh):
                packed = jnp.zeros((SP * RL, LANES), jnp.float32)
                for f in range(i * per, min(3, (i + 1) * per)):
                    z = last[f][:, W:]
                    if f % per:
                        z = pltpu.roll(z, 2 * hw * (f % per), 1)
                    packed = jnp.where(slots == f % per, z, packed)
                chalo_src[i] = packed
            for copy in carry():
                copy.start()

            @pl.loop(0, TG)
            def _(t):
                give(t)

    width = NX // GROUPS

    def fwd(q):
        cols = pl.ds(q * width, width)
        return pltpu.make_async_remote_copy(
            src_ref=ce.at[:, :, cols], dst_ref=cb.at[:, :, cols],
            send_sem=fwd_s.at[q], recv_sem=fwd_r.at[q], device_id=(lax.rem(p + 1, T), y), device_id_type=MESH,
        )

    for q in range(GROUPS):
        whole(ce.at[:, :, pl.ds(q * width, width)], ret_r.at[q])

        @pl.when(even)
        def _():
            fwd(q).start()

    @pl.when(p == 0)
    def _():
        cb[...] = init_ref[...]

    @pl.when(jnp.logical_and(even, p > 0))
    def _():
        whole(cb, beg_r)

    for q in range(GROUPS):
        @pl.when(jnp.logical_not(even))
        def _():
            fwd(q).wait_recv()

        cols = pl.ds(q * width, width)
        for f in range(3):
            start, end = cb[f, :, cols], ce[f, :, cols]
            out_ref[0, 0, f, :, cols] = start
            out_ref[0, 1, f, :, cols] = mid[f, :, cols] + 0.5 * (start + end)
            out_ref[0, 2, f, :, cols] = end

    @pl.when(p < T - 1)
    def _():
        shift.wait_send()

    @pl.when(even)
    def _():
        for q in range(GROUPS):
            fwd(q).wait_send()

    for stage in range(2):
        for side in range(2):
            edge_copy(stage, side).wait_send()
    for yo in range(SP):
        flat = pb * SP + yo

        @pl.when(jnp.logical_and(lax.rem(flat, stride) == 0, yo != y))
        def _():
            dep_copy(yo).wait_send()

            @pl.when(block == 0)
            def _():
                ini_copy(yo).wait_send()

    @pl.when(is_owner)
    def _():
        whole(b.at[:, :, pl.ds(0, (K - 1) * W)], a2a_s.at[0])
        whole(halo_src.at[:, :, pl.ds(0, (K - 1) * LANES)], a2a_s.at[1])
        whole(cs.at[pl.ds(0, TG * SP - 1)], ret_s)

        @pl.when(block < NG - 1)
        def _():
            for copy in carry():
                copy.wait_send()

        for t in range(0, TG, 2):
            for yo in range(SP):
                sent = jnp.logical_not(jnp.logical_and(t == pb, y == yo))
                if t == 0:
                    sent = jnp.logical_and(sent, block > 0)

                @pl.when(sent)
                def _():
                    pltpu.make_async_copy(cin.at[yo], cin.at[yo], beg_s.at[t * SP + yo]).wait()

    @pl.when(jnp.logical_not(is_owner))
    def _():
        whole(b, a2a_s.at[0])
        whole(halo_src, a2a_s.at[1])


def solution(mesh):
    T, SP = mesh.shape["tm"], mesh.shape["space"]

    def per_device(fine_nodes, init_state, mean_depth):
        RL, NX = mean_depth.shape
        NG = 2 if T % 4 == 0 else 1
        members = T // NG * SP
        W = max(LANES, NX // members)
        K = NX // W
        stride = members // K
        hw = 8
        while hw < T:
            hw *= 2
        per = LANES // (2 * hw)
        nh = -(-3 // per)
        cfg = (T, SP, RL, NX, W, K, stride, hw, per, nh, NG)
        f32, dma = jnp.float32, pltpu.SemaphoreType.DMA
        state = pltpu.VMEM((3, RL, NX), f32)
        R = RL * SP
        vmem = pl.BlockSpec(memory_space=pltpu.VMEM)
        return pl.pallas_call(
            functools.partial(kernel, cfg),
            out_shape=pltpu.VMEM(fine_nodes.shape, f32),
            in_specs=[pl.BlockSpec(memory_space=pl.ANY)] * 3,
            out_specs=vmem,
            scratch_shapes=[
                pltpu.VMEM((3, 3, RL, NX), f32), state, pltpu.VMEM((RL, NX), f32),
                state, state, state, state, state,
                pltpu.VMEM((nh, RL, K * LANES), f32),
                pltpu.VMEM((SP, RL, W + LANES), f32),
                pltpu.VMEM((R, W + LANES), f32),
                pltpu.VMEM((SP, 3, RL, W + LANES), f32),
                pltpu.VMEM((3, R, W + LANES), f32),
                pltpu.VMEM((T // NG, 3, R, W), f32),
                pltpu.VMEM((T // NG, nh, R, LANES), f32),
                pltpu.VMEM((members, 3, RL, W), f32),
                state, state,
                pltpu.VMEM((2, 2, 3, 1, NX), f32),
                pltpu.VMEM((2, 2, 3, 1, NX), f32),
                pltpu.VMEM((SP, 3, RL, W), f32),
                pltpu.VMEM((nh, R, LANES), f32),
                pltpu.VMEM((nh, R, LANES), f32),
                pltpu.VMEM((3, R, W + LANES), f32),
                dma, dma, dma((2, 2)), dma((2, 2)), dma((SP,)), dma, dma((SP,)), dma, dma((2,)), dma((2, T // NG)),
                dma, dma((GROUPS,)), dma((GROUPS,)), dma((GROUPS,)),
                dma((2,)), dma((2,)), dma((members,)), dma, dma((5,)),
            ],
            compiler_params=pltpu.CompilerParams(
                collective_id=0, has_side_effects=True, vmem_limit_bytes=60 * 1024 * 1024
            ),
        )(fine_nodes, init_state, mean_depth)

    return jax.shard_map(
        per_device,
        mesh=mesh,
        in_specs=(P("tm", None, None, "space", None), P(None, "space", None), P("space", None)),
        out_specs=P("tm", None, None, "space", None),
        check_vma=False,
    )
```

```python
import functools

import jax
import jax.numpy as jnp
from jax import lax
from jax.experimental import pallas as pl
from jax.experimental.pallas import tpu as pltpu
from jax.sharding import PartitionSpec as P

MESH = pl.DeviceIdType.MESH
DT = 0.3
NU = 1.0 / 3.0
FC = 0.5
DIFF = DT * NU
HALF = DT * 0.5
TURN = DT * FC
LANES = 128
SUB = 8
CHUNKS = 4
GROUPS = 4


def shift_left(v):
    return pltpu.roll(v, v.shape[1] - 1, 1)


def shift_right(v):
    return pltpu.roll(v, 1, 1)


def shift_up(v):
    return pltpu.roll(v, v.shape[0] - 1, 0)


def shift_down(v):
    return pltpu.roll(v, 1, 0)


def row_terms(h, e, n, depth):
    dn = depth * n
    nh, ne, nn, hh = DIFF * h, DIFF * e, DIFF * n, HALF * h
    return (nh - dn, ne, nn - hh), (nh + dn, ne, nn + hh)


def column_terms(h, e, n, depth):
    de = depth * e
    nh, ne, nn, hh = DIFF * h, DIFF * e, DIFF * n, HALF * h
    return (
        shift_left(nh - de) + shift_right(nh + de) - 4.0 * nh,
        shift_left(ne - hh) + shift_right(ne + hh) - 4.0 * ne + TURN * n,
        shift_left(nn) + shift_right(nn) - 4.0 * nn - TURN * e,
    )


def periodic_rate(state, depth):
    rates = column_terms(*state, depth)
    ups, downs = row_terms(*state, depth)
    return [rates[f] + shift_up(ups[f]) + shift_down(downs[f]) for f in range(3)]


def kernel(
    cfg, u_hbm, init_hbm, depth_hbm, out_ref, u_ref, init_ref, depth_ref,
    w, s0, g, s1, mid, b, halo_src, rsrc, rdst, dhsrc, dhdst, dsrc, dep, isrc, ini, main, halo, cs, ce, cb,
    esrc, edst, eo, redge, cin, chalo, chalo_src, state,
    shift_s, shift_r, rel_s, rel_r, dh_s, dh_r, edge_s, edge_r, dep_s, dep_r, ini_s, ini_r, a2a_s, a2a_r, ret_s, ret_r,
    fwd_s, fwd_r, c_s, c_r, beg_s, beg_r, in_s,
):
    T, SP, RL, NX, W, K, stride, hw, per, nh, NG, NC = cfg
    TG = T // NG
    WC = NX // NC
    tpc = K // NC
    sides = 1 if SP == 2 else 2
    p, y = lax.axis_index("tm"), lax.axis_index("space")
    me = p * SP + y
    total = T * SP
    block = p // TG
    pb = p - block * TG
    local = pb * SP + y
    is_owner = lax.rem(local, stride) == 0
    even = lax.rem(p, 2) == 0
    odd = jnp.logical_not(even)
    late = jnp.logical_and(even, p > 0)

    def tile_of(j):
        return lax.rem(j, NC) * tpc + j // NC

    def owner_of(k):
        return lax.rem(k, tpc) * NC + k // tpc

    mine = tile_of(local // stride)

    def where(flat):
        return (flat // SP, lax.rem(flat, SP))

    def row_neighbour(side):
        return lax.rem(y + SP - 1, SP) if side == 0 else lax.rem(y + 1, SP)

    barrier = pltpu.get_barrier_semaphore()

    @pl.loop(1, total)
    def _(i):
        pl.semaphore_signal(barrier, inc=1, device_id=where(lax.rem(me + i, total)), device_id_type=MESH)

    loads = [pltpu.make_async_copy(u_hbm.at[0, i], u_ref.at[i], in_s.at[i]) for i in (2, 0, 1)]
    loads.append(pltpu.make_async_copy(depth_hbm, depth_ref, in_s.at[3]))
    loads.append(pltpu.make_async_copy(init_hbm, init_ref, in_s.at[4]))
    for copy in loads:
        copy.start()
    loads[0].wait()
    pl.semaphore_wait(barrier, total - 1)

    def chunk(c):
        return pl.ds(c * WC, WC)

    def shift(c, dst):
        return pltpu.make_async_remote_copy(
            src_ref=u_ref.at[2, :, :, chunk(c)], dst_ref=dst.at[:, :, chunk(c)],
            send_sem=shift_s.at[c], recv_sem=shift_r.at[c],
            device_id=(lax.rem(p + 1, T), y), device_id_type=MESH,
        )

    @pl.when(jnp.logical_and(odd, p < T - 1))
    def _():
        for c in range(NC):
            shift(c, w).start()

    @pl.when(even)
    def _():
        for c in range(NC):
            shift(c, s0).start()

    for copy in loads[1:]:
        copy.wait()

    depth_ref[...] = HALF * depth_ref[...]

    lane_h = lax.broadcasted_iota(jnp.int32, (RL, LANES), 1)
    row8 = lax.broadcasted_iota(jnp.int32, (SUB, NX), 0)
    row8c = lax.broadcasted_iota(jnp.int32, (SUB, WC), 0)

    def margin(ref, c):
        after = ref[:, pl.ds((c + 1) % NC * WC, LANES)]
        before = ref[:, pl.ds((c * WC - LANES) % NX, LANES)]
        lanes = lax.broadcasted_iota(jnp.int32, after.shape, 1)
        return jnp.where(lanes < LANES // 2, after, before)

    def window(ref, c):
        return jnp.concatenate([ref[:, chunk(c)], margin(ref, c)], axis=1)

    def depth_halo(side):
        return pltpu.make_async_remote_copy(
            src_ref=dhsrc, dst_ref=dhdst.at[side], send_sem=dh_s.at[side], recv_sem=dh_r.at[side],
            device_id=(p, row_neighbour(side)), device_id_type=MESH,
        )

    @pl.when(late)
    def _():
        dhsrc[...] = jnp.where(row8 < SUB // 2, depth_ref[:SUB], depth_ref[RL - SUB :])
        for side in range(sides):
            depth_halo(side).start()
        s0[...] = jnp.zeros_like(s0)

    @pl.when(p == 0)
    def _():
        s0[...] = init_ref[...]

    @pl.when(odd)
    def _():
        for c in range(NC):
            shift(c, s0).wait_recv()

    row = lax.broadcasted_iota(jnp.int32, (RL, NX), 0)

    def edge_copy(stage, side):
        return pltpu.make_async_remote_copy(
            src_ref=esrc.at[stage, side], dst_ref=edst.at[stage, side],
            send_sem=edge_s.at[stage, side], recv_sem=edge_r.at[stage, side],
            device_id=(p, row_neighbour(side)), device_id_type=MESH,
        )

    def send_edges(stage, rows_of):
        top, bottom = rows_of(0), rows_of(RL - 1)
        up0, _ = row_terms(*top, depth_ref[0:1])
        _, down1 = row_terms(*bottom, depth_ref[RL - 1 : RL])
        for f in range(3):
            esrc[stage, 0, f] = up0[f]
            esrc[stage, 1, f] = down1[f]
        for side in range(2):
            edge_copy(stage, side).start()

    def rate_of_g(stage, between):
        between()
        h, e, n, depth = g[0], g[1], g[2], depth_ref[...]
        rates = column_terms(h, e, n, depth)
        ups, downs = row_terms(h, e, n, depth)
        for side in range(2):
            edge_copy(stage, side).wait_recv()
        return [
            rates[f]
            + jnp.where(row == RL - 1, edst[stage, 0, f], shift_up(ups[f]))
            + jnp.where(row == 0, edst[stage, 1, f], shift_down(downs[f]))
            for f in range(3)
        ]

    def relay(c, side):
        return pltpu.make_async_remote_copy(
            src_ref=rsrc.at[:, :, chunk(c)], dst_ref=rdst.at[side, :, :, chunk(c)],
            send_sem=rel_s.at[side, c], recv_sem=rel_r.at[side, c],
            device_id=(p, row_neighbour(side)), device_id_type=MESH,
        )

    def relay_chunks(chunks):
        @pl.when(late)
        def _():
            for c in chunks:
                shift(c, w).wait_recv()
                for f in range(3):
                    rsrc[f, :, chunk(c)] = jnp.where(row8c < SUB // 2, w[f, :SUB, chunk(c)], w[f, RL - SUB :, chunk(c)])
                for side in range(sides):
                    relay(c, side).start()

    def first_g(rows, f):
        return (
            (-7.0 / 24.0) * u_ref[0, f, rows] + (1.0 / 3.0) * u_ref[1, f, rows] - (1.0 / 24.0) * u_ref[2, f, rows]
            + 0.5 * s0[f, rows]
        )

    send_edges(0, lambda r: [first_g(slice(r, r + 1), f) for f in range(3)])
    for f in range(3):
        g[f] = first_g(slice(0, RL), f)

    def dep_copy(yo):
        return pltpu.make_async_remote_copy(
            src_ref=dsrc.at[yo], dst_ref=dep.at[pl.ds(pl.multiple_of(y * RL, 8), RL)],
            send_sem=dep_s.at[yo], recv_sem=dep_r, device_id=(p, yo), device_id_type=MESH,
        )

    def ini_copy(yo):
        return pltpu.make_async_remote_copy(
            src_ref=isrc.at[yo], dst_ref=ini.at[:, pl.ds(pl.multiple_of(y * RL, 8), RL)],
            send_sem=ini_s.at[yo], recv_sem=ini_r, device_id=(p, yo), device_id_type=MESH,
        )

    def owner_tables():
        for yo in range(SP):
            flat = pb * SP + yo
            k = tile_of(flat // stride)
            at_k = pl.ds(pl.multiple_of(k * W, LANES), W)
            at_after = pl.ds(pl.multiple_of(lax.rem((k + 1) * W, NX), LANES), LANES)
            at_before = pl.ds(pl.multiple_of(lax.rem(k * W + NX - LANES, NX), LANES), LANES)

            @pl.when(lax.rem(flat, stride) == 0)
            def _():
                dsrc[yo, :, :W] = depth_ref[:, at_k]
                dsrc[yo, :, W:] = jnp.where(lane_h < LANES // 2, depth_ref[:, at_after], depth_ref[:, at_before])

                @pl.when(yo != y)
                def _():
                    dep_copy(yo).start()

                @pl.when(yo == y)
                def _():
                    pltpu.make_async_copy(
                        dsrc.at[yo], dep.at[pl.ds(pl.multiple_of(y * RL, 8), RL)], dep_r
                    ).start()

            @pl.when(jnp.logical_and(lax.rem(flat, stride) == 0, block == 0))
            def _():
                for f in range(3):
                    isrc[yo, f, :, :W] = init_ref[f, :, at_k]
                    isrc[yo, f, :, W:] = jnp.where(
                        lane_h < LANES // 2, init_ref[f, :, at_after], init_ref[f, :, at_before]
                    )

                @pl.when(yo != y)
                def _():
                    ini_copy(yo).start()

                @pl.when(yo == y)
                def _():
                    pltpu.make_async_copy(
                        isrc.at[yo], ini.at[:, pl.ds(pl.multiple_of(y * RL, 8), RL)], ini_r
                    ).start()

    def between_zero():
        owner_tables()
        relay_chunks(range(0, NC // 4))

    rates = rate_of_g(0, between_zero)
    for f in range(3):
        s1[f] = s0[f] + rates[f]
    for f in range(3):
        g[f] = (
            0.5 * s1[f]
            - (1.0 / 24.0) * u_ref[0, f] - (1.0 / 6.0) * u_ref[1, f] + (5.0 / 24.0) * u_ref[2, f]
        )
    send_edges(1, lambda r: [g[f, r : r + 1] for f in range(3)])
    rates = rate_of_g(1, lambda: relay_chunks(range(NC // 4, NC)))
    for f in range(3):
        s2 = s1[f] + rates[f]
        b[f] = (1.0 / 6.0) * s2 + (2.0 / 3.0) * s1[f] - (5.0 / 6.0) * s0[f]
        mid[f] = s1[f] - 0.5 * (s0[f] + s2)

    my_rows = pl.ds(pl.multiple_of(y * RL, 8), RL)

    def a2a(i, k):
        j = owner_of(k)
        if i == 0:
            src, dst = b.at[:, :, pl.ds(pl.multiple_of(k * W, LANES), W)], main.at[pb, :, my_rows]
        else:
            src, dst = halo_src.at[:, :, pl.ds(pl.multiple_of(k * LANES, LANES), LANES)], halo.at[pb, :, my_rows]

        @pl.when(j * stride != local)
        def _():
            pltpu.make_async_remote_copy(
                src_ref=src, dst_ref=dst, send_sem=a2a_s.at[i], recv_sem=a2a_r.at[i, pb],
                device_id=where(block * TG * SP + j * stride), device_id_type=MESH,
            ).start()

        @pl.when(j * stride == local)
        def _():
            pltpu.make_async_copy(src, dst, a2a_r.at[i, pb]).start()

    def extended(own, tile):
        return jnp.concatenate([own, tile], axis=0)

    def late_chunk(c):
        if sides == 1:
            tiles = [window(rdst.at[0, f], c) for f in range(3)]
            depth_tile = window(dhdst.at[0], c)
        else:
            rows8 = lax.broadcasted_iota(jnp.int32, (SUB, WC + LANES), 0)
            tiles = [
                jnp.where(rows8 < SUB // 2, window(rdst.at[0, f], c), window(rdst.at[1, f], c)) for f in range(3)
            ]
            depth_tile = jnp.where(rows8 < SUB // 2, window(dhdst.at[0], c), window(dhdst.at[1], c))
        depth = extended(window(depth_ref, c), depth_tile)
        start = [extended(window(w.at[f], c), tiles[f]) for f in range(3)]
        once = periodic_rate(start, depth)
        twice = periodic_rate(once, depth)
        for f in range(3):
            one, two = once[f][:RL, :WC], twice[f][:RL, :WC]
            b[f, :, chunk(c)] = b[f, :, chunk(c)] + (0.5 * one + (1.0 / 24.0) * two)
            mid[f, :, chunk(c)] = mid[f, :, chunk(c)] - 0.125 * two

        @pl.loop(0, tpc)
        def _(i):
            a2a(0, c * tpc + lax.rem(mine + i, tpc))

    @pl.when(late)
    def _():
        for side in range(sides):
            depth_halo(side).wait_recv()
        arrived = 0
        for step in range(1, NC + 1):
            c = step % NC
            while arrived < min(step + 2, NC):
                for side in range(sides):
                    relay(arrived, side).wait_recv()
                arrived += 1
            late_chunk(c)

    @pl.when(jnp.logical_not(late))
    def _():
        @pl.loop(0, K)
        def _(i):
            a2a(0, lax.rem(mine + i, K))

    slot_of = lax.rem(lane_h + hw, LANES) // (2 * hw)
    for k in range(K):
        lo, hi = ((k + 1) % K) * W, (k * W - LANES) % NX
        packed = [jnp.zeros((RL, LANES), jnp.float32) for _ in range(nh)]
        for f in range(3):
            z = jnp.where(lane_h < LANES // 2, b[f, :, lo : lo + LANES], b[f, :, hi : hi + LANES])
            slot = f % per
            if slot:
                z = pltpu.roll(z, 2 * hw * slot, 1)
            packed[f // per] = jnp.where(slot_of == slot, z, packed[f // per])
        for i in range(nh):
            halo_src[i, :, k * LANES : (k + 1) * LANES] = packed[i]

    @pl.loop(0, K)
    def _(i):
        a2a(1, lax.rem(mine + i, K))

    my_tile = pl.ds(pl.multiple_of(mine * W, LANES), W)
    my_group = mine // (K // GROUPS)

    def give_edges(t):
        for yo in range(SP):
            src, dst = eo.at[t * SP + yo], redge.at[:, :, :, my_tile]
            here = jnp.logical_and(t == pb, y == yo)

            @pl.when(jnp.logical_not(here))
            def _():
                pltpu.make_async_remote_copy(
                    src_ref=src, dst_ref=dst, send_sem=ret_s, recv_sem=ret_r.at[my_group],
                    device_id=(block * TG + t, yo), device_id_type=MESH,
                ).start()

            @pl.when(here)
            def _():
                pltpu.make_async_copy(src, dst, ret_r.at[my_group]).start()

    def give_begin(t, src):
        for yo in range(SP):
            dst = cb.at[:, :, my_tile]
            here = jnp.logical_and(t == pb, y == yo)

            @pl.when(jnp.logical_not(here))
            def _():
                pltpu.make_async_remote_copy(
                    src_ref=src.at[yo], dst_ref=dst, send_sem=beg_s.at[t * SP + yo], recv_sem=beg_r.at[my_group],
                    device_id=(block * TG + t, yo), device_id_type=MESH,
                ).start()

            @pl.when(here)
            def _():
                pltpu.make_async_copy(src.at[yo], dst, beg_r.at[my_group]).start()

    def give(t):
        give_edges(t)

        @pl.when(jnp.logical_and(lax.rem(t, 2) == 1, t < TG - 1))
        def _():
            give_begin(t + 1, cs.at[pl.ds(t * SP, SP)])

    def carry():
        ends = ((cs.at[pl.ds((TG - 1) * SP, SP)], cin), (chalo_src, chalo))
        return [
            pltpu.make_async_remote_copy(
                src_ref=src, dst_ref=dst, send_sem=c_s.at[i], recv_sem=c_r.at[i],
                device_id=(lax.rem(p + TG, T), y), device_id_type=MESH,
            )
            for i, (src, dst) in enumerate(ends)
        ]

    def unpack(tile, f):
        return pltpu.roll(tile, LANES - 2 * hw * (f % per), 1) if f % per else tile

    def whole(ref, sem):
        pltpu.make_async_copy(ref, ref, sem).wait()

    R = SP * RL

    @pl.when(is_owner)
    def _():
        whole(dep, dep_r)
        depth = dep[...]

        def turn(t, cur):
            whole(main.at[t], a2a_r.at[0, t])
            whole(halo.at[t], a2a_r.at[1, t])
            h, e, n = (
                cur[f] + jnp.concatenate([main[t, f], unpack(halo[t, f // per], f)], axis=1) for f in range(3)
            )
            rates = column_terms(h, e, n, depth)
            ups, downs = row_terms(h, e, n, depth)
            new = []
            for f in range(3):
                value = cur[f] + (rates[f] + shift_up(ups[f]) + shift_down(downs[f]))
                for yo in range(SP):
                    cs[t * SP + yo, f] = value[yo * RL : (yo + 1) * RL, :W]
                    below, above = (yo + 1) * RL % R, (yo * RL - 1) % R
                    eo[t * SP + yo, 0, f] = ups[f][below : below + 1, :W]
                    eo[t * SP + yo, 1, f] = downs[f][above : above + 1, :W]
                new.append(value)

            @pl.when(jnp.logical_and(t > 0, block == NG - 1))
            def _():
                give(t - 1)

            return tuple(new)

        @pl.when(block == 0)
        def _():
            whole(ini, ini_r)
            state[...] = ini[...]

        @pl.when(block > 0)
        def _():
            for copy in carry():
                copy.wait_recv()
            give_begin(0, cin)
            for f in range(3):
                for yo in range(SP):
                    state[f, yo * RL : (yo + 1) * RL, :W] = cin[yo, f]
                state[f, :, W:] = unpack(chalo[f // per], f)

        last = lax.fori_loop(0, TG, turn, tuple(state[f] for f in range(3)))

        @pl.when(block == NG - 1)
        def _():
            give(TG - 1)

        @pl.when(block < NG - 1)
        def _():
            lanes = lax.broadcasted_iota(jnp.int32, (SP * RL, LANES), 1)
            slots = lax.rem(lanes + hw, LANES) // (2 * hw)
            for i in range(nh):
                packed = jnp.zeros((SP * RL, LANES), jnp.float32)
                for f in range(i * per, min(3, (i + 1) * per)):
                    z = last[f][:, W:]
                    if f % per:
                        z = pltpu.roll(z, 2 * hw * (f % per), 1)
                    packed = jnp.where(slots == f % per, z, packed)
                chalo_src[i] = packed
            for copy in carry():
                copy.start()

            @pl.loop(0, TG)
            def _(t):
                give(t)

    width = NX // GROUPS

    def fwd(q):
        cols = pl.ds(q * width, width)
        return pltpu.make_async_remote_copy(
            src_ref=ce.at[:, :, cols], dst_ref=cb.at[:, :, cols],
            send_sem=fwd_s.at[q], recv_sem=fwd_r.at[q], device_id=(lax.rem(p + 1, T), y), device_id_type=MESH,
        )

    for q in range(GROUPS):
        whole(redge.at[:, :, :, pl.ds(q * width, width)], ret_r.at[q])

    @pl.when(p == 0)
    def _():
        cb[...] = init_ref[...]

    @pl.when(late)
    def _():
        for q in range(GROUPS):
            whole(cb.at[:, :, pl.ds(q * width, width)], beg_r.at[q])

    rowc = lax.broadcasted_iota(jnp.int32, (RL, WC), 0)

    def finish(q):
        cols = chunk(q)
        v = [window(cb.at[f], q) + window(b.at[f], q) for f in range(3)]
        rates = column_terms(*v, window(depth_ref, q))
        ups, downs = row_terms(*(v[f][:, :WC] for f in range(3)), depth_ref[:, cols])
        for f in range(3):
            start = cb[f, :, cols]
            end = (
                start + rates[f][:, :WC]
                + jnp.where(rowc == RL - 1, redge[0, f, :, cols], shift_up(ups[f]))
                + jnp.where(rowc == 0, redge[1, f, :, cols], shift_down(downs[f]))
            )
            ce[f, :, cols] = end
            out_ref[0, 0, f, :, cols] = start
            out_ref[0, 1, f, :, cols] = mid[f, :, cols] + 0.5 * (start + end)
            out_ref[0, 2, f, :, cols] = end

    @pl.when(even)
    def _():
        for q in range(NC):
            finish(q)
            fwd(q).start()

    @pl.when(odd)
    def _():
        arrived = 0
        for step in range(1, NC + 1):
            while arrived < min(step + 2, NC):
                fwd(arrived).wait_recv()
                arrived += 1
            finish(step % NC)

    @pl.when(even)
    def _():
        for q in range(GROUPS):
            fwd(q).wait_send()

    @pl.when(p < T - 1)
    def _():
        for c in range(NC):
            shift(c, w).wait_send()

    @pl.when(late)
    def _():
        for side in range(sides):
            depth_halo(side).wait_send()
            for c in range(NC):
                relay(c, side).wait_send()

    for stage in range(2):
        for side in range(2):
            edge_copy(stage, side).wait_send()
    for yo in range(SP):
        flat = pb * SP + yo

        @pl.when(jnp.logical_and(lax.rem(flat, stride) == 0, yo != y))
        def _():
            dep_copy(yo).wait_send()

            @pl.when(block == 0)
            def _():
                ini_copy(yo).wait_send()

    @pl.when(is_owner)
    def _():
        whole(b.at[:, :, pl.ds(0, (K - 1) * W)], a2a_s.at[0])
        whole(halo_src.at[:, :, pl.ds(0, (K - 1) * LANES)], a2a_s.at[1])
        whole(eo.at[pl.ds(0, TG * SP - 1)], ret_s)

        @pl.when(block < NG - 1)
        def _():
            for copy in carry():
                copy.wait_send()

        for t in range(0, TG, 2):
            for yo in range(SP):
                sent = jnp.logical_not(jnp.logical_and(t == pb, y == yo))
                if t == 0:
                    sent = jnp.logical_and(sent, block > 0)

                @pl.when(sent)
                def _():
                    pltpu.make_async_copy(cin.at[yo], cin.at[yo], beg_s.at[t * SP + yo]).wait()

    @pl.when(jnp.logical_not(is_owner))
    def _():
        whole(b, a2a_s.at[0])
        whole(halo_src, a2a_s.at[1])


def solution(mesh):
    T, SP = mesh.shape["tm"], mesh.shape["space"]

    def per_device(fine_nodes, init_state, mean_depth):
        RL, NX = mean_depth.shape
        NG = 2 if T % 4 == 0 else 1
        members = T // NG * SP
        W = max(LANES, NX // members)
        K = NX // W
        NC = CHUNKS if K % CHUNKS == 0 else 1
        stride = members // K
        hw = 8
        while hw < T:
            hw *= 2
        per = LANES // (2 * hw)
        nh = -(-3 // per)
        cfg = (T, SP, RL, NX, W, K, stride, hw, per, nh, NG, NC)
        f32, dma = jnp.float32, pltpu.SemaphoreType.DMA
        state = pltpu.VMEM((3, RL, NX), f32)
        R = RL * SP
        sides = 1 if SP == 2 else 2
        edges = pltpu.VMEM((2, 2, 3, 1, NX), f32)
        vmem = pl.BlockSpec(memory_space=pltpu.VMEM)
        return pl.pallas_call(
            functools.partial(kernel, cfg),
            out_shape=pltpu.VMEM(fine_nodes.shape, f32),
            in_specs=[pl.BlockSpec(memory_space=pl.ANY)] * 3,
            out_specs=vmem,
            scratch_shapes=[
                pltpu.VMEM((3, 3, RL, NX), f32), state, pltpu.VMEM((RL, NX), f32),
                state, state, state, state, state, state,
                pltpu.VMEM((nh, RL, K * LANES), f32),
                pltpu.VMEM((3, SUB, NX), f32),
                pltpu.VMEM((sides, 3, SUB, NX), f32),
                pltpu.VMEM((SUB, NX), f32),
                pltpu.VMEM((sides, SUB, NX), f32),
                pltpu.VMEM((SP, RL, W + LANES), f32),
                pltpu.VMEM((R, W + LANES), f32),
                pltpu.VMEM((SP, 3, RL, W + LANES), f32),
                pltpu.VMEM((3, R, W + LANES), f32),
                pltpu.VMEM((T // NG, 3, R, W), f32),
                pltpu.VMEM((T // NG, nh, R, LANES), f32),
                pltpu.VMEM((members, 3, RL, W), f32),
                state, state,
                edges, edges,
                pltpu.VMEM((members, 2, 3, 1, W), f32),
                pltpu.VMEM((2, 3, 1, NX), f32),
                pltpu.VMEM((SP, 3, RL, W), f32),
                pltpu.VMEM((nh, R, LANES), f32),
                pltpu.VMEM((nh, R, LANES), f32),
                pltpu.VMEM((3, R, W + LANES), f32),
                dma((NC,)), dma((NC,)), dma((sides, NC)), dma((sides, NC)), dma((sides,)), dma((sides,)),
                dma((2, 2)), dma((2, 2)), dma((SP,)), dma, dma((SP,)), dma, dma((2,)), dma((2, T // NG)),
                dma, dma((GROUPS,)), dma((GROUPS,)), dma((GROUPS,)),
                dma((2,)), dma((2,)), dma((members,)), dma((GROUPS,)), dma((5,)),
            ],
            compiler_params=pltpu.CompilerParams(
                collective_id=0, has_side_effects=True, vmem_limit_bytes=60 * 1024 * 1024
            ),
        )(fine_nodes, init_state, mean_depth)

    return jax.shard_map(
        per_device,
        mesh=mesh,
        in_specs=(P("tm", None, None, "space", None), P(None, "space", None), P("space", None)),
        out_specs=P("tm", None, None, "space", None),
        check_vma=False,
    )
```

```python
import functools

import jax
import jax.numpy as jnp
from jax import lax
from jax.experimental import pallas as pl
from jax.experimental.pallas import tpu as pltpu
from jax.sharding import PartitionSpec as P

MESH = pl.DeviceIdType.MESH
DT = 0.3
NU = 1.0 / 3.0
FC = 0.5
DIFF = DT * NU
HALF = DT * 0.5
TURN = DT * FC
LANES = 128
SUB = 8
DEEP = 2
CHUNKS = 4
GROUPS = 4
PARTS = 8


def shift_left(v):
    return pltpu.roll(v, v.shape[1] - 1, 1)


def shift_right(v):
    return pltpu.roll(v, 1, 1)


def shift_up(v):
    return pltpu.roll(v, v.shape[0] - 1, 0)


def shift_down(v):
    return pltpu.roll(v, 1, 0)


def row_terms(h, e, n, depth):
    dn = depth * n
    nh, ne, nn, hh = DIFF * h, DIFF * e, DIFF * n, HALF * h
    return (nh - dn, ne, nn - hh), (nh + dn, ne, nn + hh)


def column_terms(h, e, n, depth):
    de = depth * e
    nh, ne, nn, hh = DIFF * h, DIFF * e, DIFF * n, HALF * h
    return (
        shift_left(nh - de) + shift_right(nh + de) - 4.0 * nh,
        shift_left(ne - hh) + shift_right(ne + hh) - 4.0 * ne + TURN * n,
        shift_left(nn) + shift_right(nn) - 4.0 * nn - TURN * e,
    )


def periodic_rate(state, depth):
    rates = column_terms(*state, depth)
    ups, downs = row_terms(*state, depth)
    return [rates[f] + shift_up(ups[f]) + shift_down(downs[f]) for f in range(3)]


def kernel(
    cfg, u_hbm, init_hbm, depth_hbm, out_ref, u_ref, init_ref, depth_ref,
    w, s0, g, s1, mid, b, halo_src, rsrc, rdst, dhsrc, dhdst, dsrc, dep, isrc, ini, main, halo, cs, ce, cb,
    esrc, edst, eo, redge, cin, chalo, chalo_src, state,
    shift_s, shift_r, rel_s, rel_r, dh_s, dh_r, edge_s, edge_r, dep_s, dep_r, ini_s, ini_r, a2a_s, a2a_r, ret_s, ret_r,
    fwd_s, fwd_r, c_s, c_r, beg_s, beg_r, in_s, go_carry, go_shift,
):
    T, SP, RL, NX, W, K, stride, hw, per, nh, NG, NC = cfg
    TG = T // NG
    WC = NX // NC
    tpc = K // NC
    sides = 1 if SP == 2 else 2
    p, y = lax.axis_index("tm"), lax.axis_index("space")
    block = p // TG
    pb = p - block * TG
    local = pb * SP + y
    is_owner = lax.rem(local, stride) == 0
    even = lax.rem(p, 2) == 0
    odd = jnp.logical_not(even)
    late = jnp.logical_and(even, p > 0)

    def tile_of(j):
        return lax.rem(j, NC) * tpc + j // NC

    def owner_of(k):
        return lax.rem(k, tpc) * NC + k // tpc

    mine = tile_of(local // stride)

    def where(flat):
        return (flat // SP, lax.rem(flat, SP))

    def row_neighbour(side):
        return lax.rem(y + SP - 1, SP) if side == 0 else lax.rem(y + 1, SP)

    barrier = pltpu.get_barrier_semaphore()

    members = TG * SP
    has_next, has_last = block < NG - 1, block > 0
    crosses = jnp.logical_and(has_next, pb == TG - 1)

    def announce(sem, pp):
        pl.semaphore_signal(sem, inc=1, device_id=(pp, y), device_id_type=MESH)

    @pl.loop(1, members)
    def _(i):
        pl.semaphore_signal(
            barrier, inc=1, device_id=where(block * members + lax.rem(local + i, members)), device_id_type=MESH
        )

    @pl.when(has_next)
    def _():
        announce(barrier, lax.rem(p + TG, T))

    @pl.when(crosses)
    def _():
        announce(barrier, lax.rem(p + 1, T))

    loads = [pltpu.make_async_copy(u_hbm.at[0, i], u_ref.at[i], in_s.at[i]) for i in (2, 0, 1)]
    loads.append(pltpu.make_async_copy(depth_hbm, depth_ref, in_s.at[3]))
    loads.append(pltpu.make_async_copy(init_hbm, init_ref, in_s.at[4]))
    for copy in loads:
        copy.start()
    loads[0].wait()
    first_of_block = jnp.logical_and(has_last, pb == 0)
    pl.semaphore_wait(barrier, members - 1 + has_last.astype(jnp.int32) + first_of_block.astype(jnp.int32))

    @pl.when(has_last)
    def _():
        announce(go_carry, lax.rem(p + T - TG, T))

    @pl.when(first_of_block)
    def _():
        announce(go_shift, lax.rem(p + T - 1, T))

    def chunk(c):
        return pl.ds(c * WC, WC)

    def shift(c, dst):
        return pltpu.make_async_remote_copy(
            src_ref=u_ref.at[2, :, :, chunk(c)], dst_ref=dst.at[:, :, chunk(c)],
            send_sem=shift_s.at[c], recv_sem=shift_r.at[c],
            device_id=(lax.rem(p + 1, T), y), device_id_type=MESH,
        )

    @pl.when(jnp.logical_and(odd, pb < TG - 1))
    def _():
        for c in range(NC):
            shift(c, w).start()

    @pl.when(even)
    def _():
        for c in range(NC):
            shift(c, s0).start()

    for copy in loads[1:]:
        copy.wait()

    depth_ref[...] = HALF * depth_ref[...]

    lane_h = lax.broadcasted_iota(jnp.int32, (RL, LANES), 1)

    def outer_rows(own):
        sub = lax.broadcasted_iota(jnp.int32, (SUB, own.shape[1]), 0)
        return jnp.where(sub < DEEP, own[:SUB], pltpu.roll(own[RL - SUB :], SUB - 2 * DEEP, 0))[: 2 * DEEP]

    def outer_tile(parts):
        if sides == 1:
            both = parts[0]
        else:
            sub = lax.broadcasted_iota(jnp.int32, parts[0].shape, 0)
            both = jnp.where(sub < DEEP, parts[0], parts[1])
        return jnp.concatenate([both] * (SUB // (2 * DEEP)), axis=0)


    def margin(ref, c, size):
        after = ref[:, pl.ds((c + 1) * size % NX, LANES)]
        before = ref[:, pl.ds((c * size - LANES) % NX, LANES)]
        lanes = lax.broadcasted_iota(jnp.int32, after.shape, 1)
        return jnp.where(lanes < LANES // 2, after, before)

    def window(ref, c, size=WC):
        return jnp.concatenate([ref[:, pl.ds(c * size, size)], margin(ref, c, size)], axis=1)

    def depth_halo(side):
        return pltpu.make_async_remote_copy(
            src_ref=dhsrc, dst_ref=dhdst.at[side], send_sem=dh_s.at[side], recv_sem=dh_r.at[side],
            device_id=(p, row_neighbour(side)), device_id_type=MESH,
        )

    @pl.when(late)
    def _():
        dhsrc[...] = outer_rows(depth_ref[...])
        for side in range(sides):
            depth_halo(side).start()
        s0[...] = jnp.zeros_like(s0)

    @pl.when(p == 0)
    def _():
        s0[...] = init_ref[...]

    @pl.when(odd)
    def _():
        for c in range(NC):
            shift(c, s0).wait_recv()

    row = lax.broadcasted_iota(jnp.int32, (RL, NX), 0)

    def edge_copy(stage, side):
        return pltpu.make_async_remote_copy(
            src_ref=esrc.at[stage, side], dst_ref=edst.at[stage, side],
            send_sem=edge_s.at[stage, side], recv_sem=edge_r.at[stage, side],
            device_id=(p, row_neighbour(side)), device_id_type=MESH,
        )

    def send_edges(stage, rows_of):
        top, bottom = rows_of(0), rows_of(RL - 1)
        up0, _ = row_terms(*top, depth_ref[0:1])
        _, down1 = row_terms(*bottom, depth_ref[RL - 1 : RL])
        for f in range(3):
            esrc[stage, 0, f] = up0[f]
            esrc[stage, 1, f] = down1[f]
        for side in range(2):
            edge_copy(stage, side).start()

    def rate_of_g(stage, between):
        between()
        h, e, n, depth = g[0], g[1], g[2], depth_ref[...]
        rates = column_terms(h, e, n, depth)
        ups, downs = row_terms(h, e, n, depth)
        for side in range(2):
            edge_copy(stage, side).wait_recv()
        return [
            rates[f]
            + jnp.where(row == RL - 1, edst[stage, 0, f], shift_up(ups[f]))
            + jnp.where(row == 0, edst[stage, 1, f], shift_down(downs[f]))
            for f in range(3)
        ]

    def relay(c, side):
        return pltpu.make_async_remote_copy(
            src_ref=rsrc.at[:, :, chunk(c)], dst_ref=rdst.at[side, :, :, chunk(c)],
            send_sem=rel_s.at[side, c], recv_sem=rel_r.at[side, c],
            device_id=(p, row_neighbour(side)), device_id_type=MESH,
        )

    def relay_chunks(chunks):
        @pl.when(late)
        def _():
            for c in chunks:
                shift(c, w).wait_recv()
                for f in range(3):
                    rsrc[f, :, chunk(c)] = outer_rows(w[f, :, chunk(c)])
                for side in range(sides):
                    relay(c, side).start()

    def first_g(rows, f):
        return (
            (-7.0 / 24.0) * u_ref[0, f, rows] + (1.0 / 3.0) * u_ref[1, f, rows] - (1.0 / 24.0) * u_ref[2, f, rows]
            + 0.5 * s0[f, rows]
        )

    send_edges(0, lambda r: [first_g(slice(r, r + 1), f) for f in range(3)])
    for f in range(3):
        g[f] = first_g(slice(0, RL), f)

    def dep_copy(yo):
        return pltpu.make_async_remote_copy(
            src_ref=dsrc.at[yo], dst_ref=dep.at[pl.ds(pl.multiple_of(y * RL, 8), RL)],
            send_sem=dep_s.at[yo], recv_sem=dep_r, device_id=(p, yo), device_id_type=MESH,
        )

    def ini_copy(yo):
        return pltpu.make_async_remote_copy(
            src_ref=isrc.at[yo], dst_ref=ini.at[:, pl.ds(pl.multiple_of(y * RL, 8), RL)],
            send_sem=ini_s.at[yo], recv_sem=ini_r, device_id=(p, yo), device_id_type=MESH,
        )

    def owner_tables():
        for yo in range(SP):
            flat = pb * SP + yo
            k = tile_of(flat // stride)
            at_k = pl.ds(pl.multiple_of(k * W, LANES), W)
            at_after = pl.ds(pl.multiple_of(lax.rem((k + 1) * W, NX), LANES), LANES)
            at_before = pl.ds(pl.multiple_of(lax.rem(k * W + NX - LANES, NX), LANES), LANES)

            @pl.when(lax.rem(flat, stride) == 0)
            def _():
                dsrc[yo, :, :W] = depth_ref[:, at_k]
                dsrc[yo, :, W:] = jnp.where(lane_h < LANES // 2, depth_ref[:, at_after], depth_ref[:, at_before])

                @pl.when(yo != y)
                def _():
                    dep_copy(yo).start()

                @pl.when(yo == y)
                def _():
                    pltpu.make_async_copy(
                        dsrc.at[yo], dep.at[pl.ds(pl.multiple_of(y * RL, 8), RL)], dep_r
                    ).start()

            @pl.when(jnp.logical_and(lax.rem(flat, stride) == 0, block == 0))
            def _():
                for f in range(3):
                    isrc[yo, f, :, :W] = init_ref[f, :, at_k]
                    isrc[yo, f, :, W:] = jnp.where(
                        lane_h < LANES // 2, init_ref[f, :, at_after], init_ref[f, :, at_before]
                    )

                @pl.when(yo != y)
                def _():
                    ini_copy(yo).start()

                @pl.when(yo == y)
                def _():
                    pltpu.make_async_copy(
                        isrc.at[yo], ini.at[:, pl.ds(pl.multiple_of(y * RL, 8), RL)], ini_r
                    ).start()

    def between_zero():
        owner_tables()
        relay_chunks(range(0, NC // 4))

    rates = rate_of_g(0, between_zero)
    for f in range(3):
        s1[f] = s0[f] + rates[f]
    for f in range(3):
        g[f] = (
            0.5 * s1[f]
            - (1.0 / 24.0) * u_ref[0, f] - (1.0 / 6.0) * u_ref[1, f] + (5.0 / 24.0) * u_ref[2, f]
        )
    send_edges(1, lambda r: [g[f, r : r + 1] for f in range(3)])
    def between_one():
        @pl.when(crosses)
        def _():
            pl.semaphore_wait(go_shift, 1)
            for c in range(NC):
                shift(c, w).start()

        relay_chunks(range(NC // 4, NC))

    rates = rate_of_g(1, between_one)
    for f in range(3):
        s2 = s1[f] + rates[f]
        b[f] = (1.0 / 6.0) * s2 + (2.0 / 3.0) * s1[f] - (5.0 / 6.0) * s0[f]
        mid[f] = s1[f] - 0.5 * (s0[f] + s2)

    my_rows = pl.ds(pl.multiple_of(y * RL, 8), RL)

    def a2a(i, k):
        j = owner_of(k)
        if i == 0:
            src, dst = b.at[:, :, pl.ds(pl.multiple_of(k * W, LANES), W)], main.at[pb, :, my_rows]
        else:
            src, dst = halo_src.at[:, :, pl.ds(pl.multiple_of(k * LANES, LANES), LANES)], halo.at[pb, :, my_rows]

        @pl.when(j * stride != local)
        def _():
            pltpu.make_async_remote_copy(
                src_ref=src, dst_ref=dst, send_sem=a2a_s.at[i], recv_sem=a2a_r.at[i, pb],
                device_id=where(block * TG * SP + j * stride), device_id_type=MESH,
            ).start()

        @pl.when(j * stride == local)
        def _():
            pltpu.make_async_copy(src, dst, a2a_r.at[i, pb]).start()

    def extended(own, tile):
        return jnp.concatenate([own, tile], axis=0)

    def late_chunk(c):
        tiles = [outer_tile([window(rdst.at[side, f], c) for side in range(sides)]) for f in range(3)]
        depth_tile = outer_tile([window(dhdst.at[side], c) for side in range(sides)])
        depth = extended(window(depth_ref, c), depth_tile)
        start = [extended(window(w.at[f], c), tiles[f]) for f in range(3)]
        once = periodic_rate(start, depth)
        twice = periodic_rate(once, depth)
        for f in range(3):
            one, two = once[f][:RL, :WC], twice[f][:RL, :WC]
            b[f, :, chunk(c)] = b[f, :, chunk(c)] + (0.5 * one + (1.0 / 24.0) * two)
            mid[f, :, chunk(c)] = mid[f, :, chunk(c)] - 0.125 * two

        @pl.loop(0, tpc)
        def _(i):
            a2a(0, c * tpc + lax.rem(mine + i, tpc))

    @pl.when(late)
    def _():
        for side in range(sides):
            depth_halo(side).wait_recv()
        arrived = 0
        for step in range(1, NC + 1):
            c = step % NC
            while arrived < min(step + 2, NC):
                for side in range(sides):
                    relay(arrived, side).wait_recv()
                arrived += 1
            late_chunk(c)

    @pl.when(jnp.logical_not(late))
    def _():
        @pl.loop(0, K)
        def _(i):
            a2a(0, lax.rem(mine + i, K))

    slot_of = lax.rem(lane_h + hw, LANES) // (2 * hw)
    for k in range(K):
        lo, hi = ((k + 1) % K) * W, (k * W - LANES) % NX
        packed = [jnp.zeros((RL, LANES), jnp.float32) for _ in range(nh)]
        for f in range(3):
            z = jnp.where(lane_h < LANES // 2, b[f, :, lo : lo + LANES], b[f, :, hi : hi + LANES])
            slot = f % per
            if slot:
                z = pltpu.roll(z, 2 * hw * slot, 1)
            packed[f // per] = jnp.where(slot_of == slot, z, packed[f // per])
        for i in range(nh):
            halo_src[i, :, k * LANES : (k + 1) * LANES] = packed[i]

    @pl.loop(0, K)
    def _(i):
        a2a(1, lax.rem(mine + i, K))

    my_tile = pl.ds(pl.multiple_of(mine * W, LANES), W)
    my_group = mine // (K // GROUPS)

    def give_edges(t):
        for yo in range(SP):
            src, dst = eo.at[t * SP + yo], redge.at[:, :, :, my_tile]
            here = jnp.logical_and(t == pb, y == yo)

            @pl.when(jnp.logical_not(here))
            def _():
                pltpu.make_async_remote_copy(
                    src_ref=src, dst_ref=dst, send_sem=ret_s, recv_sem=ret_r.at[my_group],
                    device_id=(block * TG + t, yo), device_id_type=MESH,
                ).start()

            @pl.when(here)
            def _():
                pltpu.make_async_copy(src, dst, ret_r.at[my_group]).start()

    def give_begin(t, src):
        for yo in range(SP):
            dst = cb.at[:, :, my_tile]
            here = jnp.logical_and(t == pb, y == yo)

            @pl.when(jnp.logical_not(here))
            def _():
                pltpu.make_async_remote_copy(
                    src_ref=src.at[yo], dst_ref=dst, send_sem=beg_s.at[t * SP + yo], recv_sem=beg_r.at[my_group],
                    device_id=(block * TG + t, yo), device_id_type=MESH,
                ).start()

            @pl.when(here)
            def _():
                pltpu.make_async_copy(src.at[yo], dst, beg_r.at[my_group]).start()

    def give(t):
        give_edges(t)

        @pl.when(jnp.logical_and(lax.rem(t, 2) == 1, t < TG - 1))
        def _():
            give_begin(t + 1, cs.at[pl.ds(t * SP, SP)])

    def carry():
        ends = ((cs.at[pl.ds((TG - 1) * SP, SP)], cin), (chalo_src, chalo))
        return [
            pltpu.make_async_remote_copy(
                src_ref=src, dst_ref=dst, send_sem=c_s.at[i], recv_sem=c_r.at[i],
                device_id=(lax.rem(p + TG, T), y), device_id_type=MESH,
            )
            for i, (src, dst) in enumerate(ends)
        ]

    def unpack(tile, f):
        return pltpu.roll(tile, LANES - 2 * hw * (f % per), 1) if f % per else tile

    def whole(ref, sem):
        pltpu.make_async_copy(ref, ref, sem).wait()

    R = SP * RL

    @pl.when(is_owner)
    def _():
        whole(dep, dep_r)
        depth = dep[...]

        def turn(t, cur):
            whole(main.at[t], a2a_r.at[0, t])
            whole(halo.at[t], a2a_r.at[1, t])
            h, e, n = (
                cur[f] + jnp.concatenate([main[t, f], unpack(halo[t, f // per], f)], axis=1) for f in range(3)
            )
            rates = column_terms(h, e, n, depth)
            ups, downs = row_terms(h, e, n, depth)
            new = []
            for f in range(3):
                value = cur[f] + (rates[f] + shift_up(ups[f]) + shift_down(downs[f]))
                for yo in range(SP):
                    cs[t * SP + yo, f] = value[yo * RL : (yo + 1) * RL, :W]
                    below, above = (yo + 1) * RL % R, (yo * RL - 1) % R
                    eo[t * SP + yo, 0, f] = ups[f][below : below + 1, :W]
                    eo[t * SP + yo, 1, f] = downs[f][above : above + 1, :W]
                new.append(value)

            @pl.when(jnp.logical_and(t > 0, block == NG - 1))
            def _():
                give(t - 1)

            return tuple(new)

        @pl.when(block == 0)
        def _():
            whole(ini, ini_r)
            state[...] = ini[...]

        @pl.when(block > 0)
        def _():
            for copy in carry():
                copy.wait_recv()
            give_begin(0, cin)
            for f in range(3):
                for yo in range(SP):
                    state[f, yo * RL : (yo + 1) * RL, :W] = cin[yo, f]
                state[f, :, W:] = unpack(chalo[f // per], f)

        last = lax.fori_loop(0, TG, turn, tuple(state[f] for f in range(3)))

        @pl.when(block == NG - 1)
        def _():
            give(TG - 1)

        @pl.when(block < NG - 1)
        def _():
            lanes = lax.broadcasted_iota(jnp.int32, (SP * RL, LANES), 1)
            slots = lax.rem(lanes + hw, LANES) // (2 * hw)
            for i in range(nh):
                packed = jnp.zeros((SP * RL, LANES), jnp.float32)
                for f in range(i * per, min(3, (i + 1) * per)):
                    z = last[f][:, W:]
                    if f % per:
                        z = pltpu.roll(z, 2 * hw * (f % per), 1)
                    packed = jnp.where(slots == f % per, z, packed)
                chalo_src[i] = packed
            pl.semaphore_wait(go_carry, 1)
            for copy in carry():
                copy.start()

            @pl.loop(0, TG)
            def _(t):
                give(t)

    width, part = NX // GROUPS, NX // PARTS

    def fwd(q):
        cols = pl.ds(q * part, part)
        return pltpu.make_async_remote_copy(
            src_ref=ce.at[:, :, cols], dst_ref=cb.at[:, :, cols],
            send_sem=fwd_s.at[q], recv_sem=fwd_r.at[q], device_id=(lax.rem(p + 1, T), y), device_id_type=MESH,
        )

    for q in range(GROUPS):
        whole(redge.at[:, :, :, pl.ds(q * width, width)], ret_r.at[q])

    @pl.when(p == 0)
    def _():
        cb[...] = init_ref[...]

    @pl.when(late)
    def _():
        for q in range(GROUPS):
            whole(cb.at[:, :, pl.ds(q * width, width)], beg_r.at[q])

    row_part = lax.broadcasted_iota(jnp.int32, (RL, part), 0)

    def advance(q):
        cols = pl.ds(q * part, part)
        v = [window(cb.at[f], q, part) + window(b.at[f], q, part) for f in range(3)]
        rates = column_terms(*v, window(depth_ref, q, part))
        ups, downs = row_terms(*(v[f][:, :part] for f in range(3)), depth_ref[:, cols])
        return [
            cb[f, :, cols] + rates[f][:, :part]
            + jnp.where(row_part == RL - 1, redge[0, f, :, cols], shift_up(ups[f]))
            + jnp.where(row_part == 0, redge[1, f, :, cols], shift_down(downs[f]))
            for f in range(3)
        ]

    def emit(q, ends):
        cols = pl.ds(q * part, part)
        for f in range(3):
            start = cb[f, :, cols]
            out_ref[0, 0, f, :, cols] = start
            out_ref[0, 1, f, :, cols] = mid[f, :, cols] + 0.5 * (start + ends[f])
            out_ref[0, 2, f, :, cols] = ends[f]

    @pl.when(even)
    def _():
        for q in range(PARTS):
            ends = advance(q)
            for f in range(3):
                ce[f, :, pl.ds(q * part, part)] = ends[f]
            fwd(q).start()
        for q in range(PARTS):
            emit(q, [ce[f, :, pl.ds(q * part, part)] for f in range(3)])
            fwd(q).wait_send()

    @pl.when(odd)
    def _():
        arrived = 0
        for step in range(1, PARTS + 1):
            while arrived < min(step + 2, PARTS):
                fwd(arrived).wait_recv()
                arrived += 1
            emit(step % PARTS, advance(step % PARTS))

    @pl.when(p < T - 1)
    def _():
        for c in range(NC):
            shift(c, w).wait_send()

    @pl.when(late)
    def _():
        for side in range(sides):
            depth_halo(side).wait_send()
            for c in range(NC):
                relay(c, side).wait_send()

    for stage in range(2):
        for side in range(2):
            edge_copy(stage, side).wait_send()
    for yo in range(SP):
        flat = pb * SP + yo

        @pl.when(jnp.logical_and(lax.rem(flat, stride) == 0, yo != y))
        def _():
            dep_copy(yo).wait_send()

            @pl.when(block == 0)
            def _():
                ini_copy(yo).wait_send()

    @pl.when(is_owner)
    def _():
        whole(b.at[:, :, pl.ds(0, (K - 1) * W)], a2a_s.at[0])
        whole(halo_src.at[:, :, pl.ds(0, (K - 1) * LANES)], a2a_s.at[1])
        whole(eo.at[pl.ds(0, TG * SP - 1)], ret_s)

        @pl.when(block < NG - 1)
        def _():
            for copy in carry():
                copy.wait_send()

        for t in range(0, TG, 2):
            for yo in range(SP):
                sent = jnp.logical_not(jnp.logical_and(t == pb, y == yo))
                if t == 0:
                    sent = jnp.logical_and(sent, block > 0)

                @pl.when(sent)
                def _():
                    pltpu.make_async_copy(cin.at[yo], cin.at[yo], beg_s.at[t * SP + yo]).wait()

    @pl.when(jnp.logical_not(is_owner))
    def _():
        whole(b, a2a_s.at[0])
        whole(halo_src, a2a_s.at[1])


def solution(mesh):
    T, SP = mesh.shape["tm"], mesh.shape["space"]

    def per_device(fine_nodes, init_state, mean_depth):
        RL, NX = mean_depth.shape
        NG = 2 if T % 4 == 0 else 1
        members = T // NG * SP
        W = max(LANES, NX // members)
        K = NX // W
        NC = CHUNKS if K % CHUNKS == 0 else 1
        stride = members // K
        hw = 8
        while hw < T:
            hw *= 2
        per = LANES // (2 * hw)
        nh = -(-3 // per)
        cfg = (T, SP, RL, NX, W, K, stride, hw, per, nh, NG, NC)
        f32, dma = jnp.float32, pltpu.SemaphoreType.DMA
        state = pltpu.VMEM((3, RL, NX), f32)
        R = RL * SP
        sides = 1 if SP == 2 else 2
        edges = pltpu.VMEM((2, 2, 3, 1, NX), f32)
        vmem = pl.BlockSpec(memory_space=pltpu.VMEM)
        return pl.pallas_call(
            functools.partial(kernel, cfg),
            out_shape=pltpu.VMEM(fine_nodes.shape, f32),
            in_specs=[pl.BlockSpec(memory_space=pl.ANY)] * 3,
            out_specs=vmem,
            scratch_shapes=[
                pltpu.VMEM((3, 3, RL, NX), f32), state, pltpu.VMEM((RL, NX), f32),
                state, state, state, state, state, state,
                pltpu.VMEM((nh, RL, K * LANES), f32),
                pltpu.VMEM((3, 2 * DEEP, NX), f32),
                pltpu.VMEM((sides, 3, 2 * DEEP, NX), f32),
                pltpu.VMEM((2 * DEEP, NX), f32),
                pltpu.VMEM((sides, 2 * DEEP, NX), f32),
                pltpu.VMEM((SP, RL, W + LANES), f32),
                pltpu.VMEM((R, W + LANES), f32),
                pltpu.VMEM((SP, 3, RL, W + LANES), f32),
                pltpu.VMEM((3, R, W + LANES), f32),
                pltpu.VMEM((T // NG, 3, R, W), f32),
                pltpu.VMEM((T // NG, nh, R, LANES), f32),
                pltpu.VMEM((members, 3, RL, W), f32),
                state, state,
                edges, edges,
                pltpu.VMEM((members, 2, 3, 1, W), f32),
                pltpu.VMEM((2, 3, 1, NX), f32),
                pltpu.VMEM((SP, 3, RL, W), f32),
                pltpu.VMEM((nh, R, LANES), f32),
                pltpu.VMEM((nh, R, LANES), f32),
                pltpu.VMEM((3, R, W + LANES), f32),
                dma((NC,)), dma((NC,)), dma((sides, NC)), dma((sides, NC)), dma((sides,)), dma((sides,)),
                dma((2, 2)), dma((2, 2)), dma((SP,)), dma, dma((SP,)), dma, dma((2,)), dma((2, T // NG)),
                dma, dma((GROUPS,)), dma((PARTS,)), dma((PARTS,)),
                dma((2,)), dma((2,)), dma((members,)), dma((GROUPS,)), dma((5,)),
                pltpu.SemaphoreType.REGULAR, pltpu.SemaphoreType.REGULAR,
            ],
            compiler_params=pltpu.CompilerParams(
                collective_id=0, has_side_effects=True, vmem_limit_bytes=60 * 1024 * 1024
            ),
        )(fine_nodes, init_state, mean_depth)

    return jax.shard_map(
        per_device,
        mesh=mesh,
        in_specs=(P("tm", None, None, "space", None), P(None, "space", None), P("space", None)),
        out_specs=P("tm", None, None, "space", None),
        check_vma=False,
    )
```

```python
import functools

import jax
import jax.numpy as jnp
from jax import lax
from jax.experimental import pallas as pl
from jax.experimental.pallas import tpu as pltpu
from jax.sharding import PartitionSpec as P

MESH = pl.DeviceIdType.MESH
DT = 0.3
NU = 1.0 / 3.0
FC = 0.5
DIFF = DT * NU
HALF = DT * 0.5
TURN = DT * FC
LANES = 128
SUB = 8
DEEP = 2
CHUNKS = 4
GROUPS = 4
PARTS = 8
SPANS = 2


def shift_left(v):
    return pltpu.roll(v, v.shape[1] - 1, 1)


def shift_right(v):
    return pltpu.roll(v, 1, 1)


def shift_up(v):
    return pltpu.roll(v, v.shape[0] - 1, 0)


def shift_down(v):
    return pltpu.roll(v, 1, 0)


def row_terms(h, e, n, depth):
    dn = depth * n
    nh, ne, nn, hh = DIFF * h, DIFF * e, DIFF * n, HALF * h
    return (nh - dn, ne, nn - hh), (nh + dn, ne, nn + hh)


def column_terms(h, e, n, depth):
    de = depth * e
    nh, ne, nn, hh = DIFF * h, DIFF * e, DIFF * n, HALF * h
    return (
        shift_left(nh - de) + shift_right(nh + de) - 4.0 * nh,
        shift_left(ne - hh) + shift_right(ne + hh) - 4.0 * ne + TURN * n,
        shift_left(nn) + shift_right(nn) - 4.0 * nn - TURN * e,
    )


def periodic_rate(state, depth):
    rates = column_terms(*state, depth)
    ups, downs = row_terms(*state, depth)
    return [rates[f] + shift_up(ups[f]) + shift_down(downs[f]) for f in range(3)]


class Tile:
    def __init__(self, state, depth):
        h, e, n = state
        de, dn = depth * e, depth * n
        nh, ne, nn, hh = DIFF * h, DIFF * e, DIFF * n, HALF * h
        self.lefts = [shift_left(x) for x in (nh - de, ne - hh, nn)]
        self.rights = [shift_right(x) for x in (nh + de, ne + hh, nn)]
        self.ups, self.downs = (nh - dn, ne, nn - hh), (nh + dn, ne, nn + hh)
        self.own = (-4.0 * nh, TURN * n - 4.0 * ne, -4.0 * nn - TURN * e)


def column_sum(before, tile, after, f, lane):
    return (
        tile.own[f]
        + jnp.where(lane == LANES - 1, after.lefts[f], tile.lefts[f])
        + jnp.where(lane == 0, before.rights[f], tile.rights[f])
    )


def walk(load, tiles, count, visit, made=None):
    made = {} if made is None else made

    def tile(i):
        i %= count
        if i not in made:
            made[i] = Tile(*load(i))
        return made[i]

    for j in tiles:
        visit(j, tile(j - 1), tile(j), tile(j + 1))
        if count > 4:
            made.pop((j - 1) % count)


def kernel(
    cfg, u_hbm, init_hbm, depth_hbm, out_ref, u_ref, init_ref, depth_ref,
    w, s0, g, s1, mid, b, halo_src, rsrc, rdst, dhsrc, dhdst, dsrc, dep, isrc, ini, main, halo, cs, ce, cb,
    esrc, edst, eo, redge, cin, chalo, chalo_src, state,
    shift_s, shift_r, rel_s, rel_r, dh_s, dh_r, edge_s, edge_r, dep_s, dep_r, ini_s, ini_r, a2a_s, a2a_r, ret_s, ret_r,
    fwd_s, fwd_r, c_s, c_r, beg_s, beg_r, in_s, go_carry,
):
    T, SP, RL, NX, W, K, stride, hw, per, nh, NG, NC = cfg
    TG = T // NG
    WC = NX // NC
    tpc = K // NC
    sides = 1 if SP == 2 else 2
    p, y = lax.axis_index("tm"), lax.axis_index("space")
    block = p // TG
    pb = p - block * TG
    local = pb * SP + y
    is_owner = lax.rem(local, stride) == 0
    even = lax.rem(p, 2) == 0
    odd = jnp.logical_not(even)
    late = jnp.logical_and(even, p > 0)

    def tile_of(j):
        return lax.rem(j, NC) * tpc + j // NC

    def owner_of(k):
        return lax.rem(k, tpc) * NC + k // tpc

    mine = tile_of(local // stride)

    def where(flat):
        return (flat // SP, lax.rem(flat, SP))

    def row_neighbour(side):
        return lax.rem(y + SP - 1, SP) if side == 0 else lax.rem(y + 1, SP)

    barrier = pltpu.get_barrier_semaphore()

    members = TG * SP
    has_next, has_last = block < NG - 1, block > 0
    crosses = jnp.logical_and(has_next, pb == TG - 1)

    def announce(sem, pp):
        pl.semaphore_signal(sem, inc=1, device_id=(pp, y), device_id_type=MESH)

    @pl.loop(1, members)
    def _(i):
        pl.semaphore_signal(
            barrier, inc=1, device_id=where(block * members + lax.rem(local + i, members)), device_id_type=MESH
        )

    @pl.when(has_next)
    def _():
        announce(barrier, lax.rem(p + TG, T))

    @pl.when(crosses)
    def _():
        announce(barrier, lax.rem(p + 1, T))

    loads = [pltpu.make_async_copy(u_hbm.at[0, i], u_ref.at[i], in_s.at[i]) for i in (2, 0, 1)]
    loads.append(pltpu.make_async_copy(depth_hbm, depth_ref, in_s.at[3]))
    loads.append(pltpu.make_async_copy(init_hbm, init_ref, in_s.at[4]))
    for copy in loads:
        copy.start()
    loads[0].wait()
    first_of_block = jnp.logical_and(has_last, pb == 0)
    meets = jnp.logical_or(crosses, first_of_block)

    @pl.when(first_of_block)
    def _():
        announce(barrier, lax.rem(p + T - 1, T))

    pl.semaphore_wait(barrier, members - 1 + has_last.astype(jnp.int32) + meets.astype(jnp.int32))

    @pl.when(has_last)
    def _():
        announce(go_carry, lax.rem(p + T - TG, T))

    def chunk(c):
        return pl.ds(c * WC, WC)

    def shift(c, dst):
        return pltpu.make_async_remote_copy(
            src_ref=u_ref.at[2, :, :, chunk(c)], dst_ref=dst.at[:, :, chunk(c)],
            send_sem=shift_s.at[c], recv_sem=shift_r.at[c],
            device_id=(lax.rem(p + 1, T), y), device_id_type=MESH,
        )

    @pl.when(jnp.logical_and(odd, p < T - 1))
    def _():
        for c in range(NC):
            shift(c, w).start()

    @pl.when(even)
    def _():
        for c in range(NC):
            shift(c, s0).start()

    for copy in loads[1:]:
        copy.wait()

    depth_ref[...] = HALF * depth_ref[...]

    lane_h = lax.broadcasted_iota(jnp.int32, (RL, LANES), 1)

    def outer_rows(own):
        sub = lax.broadcasted_iota(jnp.int32, (SUB, own.shape[1]), 0)
        return jnp.where(sub < DEEP, own[:SUB], pltpu.roll(own[RL - SUB :], SUB - 2 * DEEP, 0))[: 2 * DEEP]

    def outer_tile(parts):
        if sides == 1:
            both = parts[0]
        else:
            sub = lax.broadcasted_iota(jnp.int32, parts[0].shape, 0)
            both = jnp.where(sub < DEEP, parts[0], parts[1])
        return jnp.concatenate([both] * (SUB // (2 * DEEP)), axis=0)


    def margin(ref, c, size):
        after = ref[:, pl.ds((c + 1) * size % NX, LANES)]
        before = ref[:, pl.ds((c * size - LANES) % NX, LANES)]
        lanes = lax.broadcasted_iota(jnp.int32, after.shape, 1)
        return jnp.where(lanes < LANES // 2, after, before)

    def window(ref, c, size=WC):
        return jnp.concatenate([ref[:, pl.ds(c * size, size)], margin(ref, c, size)], axis=1)

    def depth_halo(side):
        return pltpu.make_async_remote_copy(
            src_ref=dhsrc, dst_ref=dhdst.at[side], send_sem=dh_s.at[side], recv_sem=dh_r.at[side],
            device_id=(p, row_neighbour(side)), device_id_type=MESH,
        )

    @pl.when(late)
    def _():
        dhsrc[...] = outer_rows(depth_ref[...])
        for side in range(sides):
            depth_halo(side).start()
        s0[...] = jnp.zeros_like(s0)

    @pl.when(p == 0)
    def _():
        s0[...] = init_ref[...]

    @pl.when(odd)
    def _():
        for c in range(NC):
            shift(c, s0).wait_recv()

    row = lax.broadcasted_iota(jnp.int32, (RL, LANES), 0)
    lane = lax.broadcasted_iota(jnp.int32, (RL, LANES), 1)
    NT = NX // LANES
    SPAN = NX // SPANS

    def lanes_of(j):
        return slice(j * LANES, (j + 1) * LANES)

    def edge_copy(stage, side, part):
        cols = pl.ds(part * SPAN, SPAN)
        return pltpu.make_async_remote_copy(
            src_ref=esrc.at[stage, side, :, :, cols], dst_ref=edst.at[stage, side, :, :, cols],
            send_sem=edge_s.at[stage, side, part], recv_sem=edge_r.at[stage, side, part],
            device_id=(p, row_neighbour(side)), device_id_type=MESH,
        )

    def put_edges(stage, cols, top, bottom):
        ups, _ = row_terms(*top, depth_ref[0:1, cols])
        _, downs = row_terms(*bottom, depth_ref[RL - 1 : RL, cols])
        for f in range(3):
            esrc[stage, 0, f, :, cols] = ups[f]
            esrc[stage, 1, f, :, cols] = downs[f]

    def send_edges(stage, part):
        for side in range(2):
            edge_copy(stage, side, part).start()

    def wait_edges(stage, part):
        for side in range(2):
            edge_copy(stage, side, part).wait_recv()

    def inner_rate(load, out):
        def visit(j, before, tile, after):
            for f in range(3):
                out[f, :, lanes_of(j)] = (
                    column_sum(before, tile, after, f, lane)
                    + jnp.where(row == RL - 1, 0.0, shift_up(tile.ups[f]))
                    + jnp.where(row == 0, 0.0, shift_down(tile.downs[f]))
                )

        walk(load, range(NT), NT, visit)

    def outer_rate(stage, f, cols):
        return jnp.where(
            row == RL - 1, edst[stage, 0, f, :, cols], jnp.where(row == 0, edst[stage, 1, f, :, cols], 0.0)
        )

    def relay(c, side):
        return pltpu.make_async_remote_copy(
            src_ref=rsrc.at[:, :, chunk(c)], dst_ref=rdst.at[side, :, :, chunk(c)],
            send_sem=rel_s.at[side, c], recv_sem=rel_r.at[side, c],
            device_id=(p, row_neighbour(side)), device_id_type=MESH,
        )

    def relay_chunks(chunks):
        @pl.when(late)
        def _():
            for c in chunks:
                shift(c, w).wait_recv()
                for f in range(3):
                    rsrc[f, :, chunk(c)] = outer_rows(w[f, :, chunk(c)])
                for side in range(sides):
                    relay(c, side).start()

    def first_g(rows, cols, f):
        return (
            (-7.0 / 24.0) * u_ref[0, f, rows, cols] + (1.0 / 3.0) * u_ref[1, f, rows, cols]
            - (1.0 / 24.0) * u_ref[2, f, rows, cols] + 0.5 * s0[f, rows, cols]
        )

    every = slice(0, RL)
    for part in range(SPANS):
        for j in range(part * SPAN // LANES, (part + 1) * SPAN // LANES):
            put_edges(0, lanes_of(j), *([first_g(slice(r, r + 1), lanes_of(j), f) for f in range(3)] for r in (0, RL - 1)))
        send_edges(0, part)
    inner_rate(
        lambda j: ([first_g(every, lanes_of(j), f) for f in range(3)], depth_ref[:, lanes_of(j)]), s1
    )

    def dep_copy(yo):
        return pltpu.make_async_remote_copy(
            src_ref=dsrc.at[yo], dst_ref=dep.at[pl.ds(pl.multiple_of(y * RL, 8), RL)],
            send_sem=dep_s.at[yo], recv_sem=dep_r, device_id=(p, yo), device_id_type=MESH,
        )

    def ini_copy(yo):
        return pltpu.make_async_remote_copy(
            src_ref=isrc.at[yo], dst_ref=ini.at[:, pl.ds(pl.multiple_of(y * RL, 8), RL)],
            send_sem=ini_s.at[yo], recv_sem=ini_r, device_id=(p, yo), device_id_type=MESH,
        )

    def owner_tables():
        for yo in range(SP):
            flat = pb * SP + yo
            k = tile_of(flat // stride)
            at_k = pl.ds(pl.multiple_of(k * W, LANES), W)
            at_after = pl.ds(pl.multiple_of(lax.rem((k + 1) * W, NX), LANES), LANES)
            at_before = pl.ds(pl.multiple_of(lax.rem(k * W + NX - LANES, NX), LANES), LANES)

            @pl.when(lax.rem(flat, stride) == 0)
            def _():
                dsrc[yo, :, :W] = depth_ref[:, at_k]
                dsrc[yo, :, W:] = jnp.where(lane_h < LANES // 2, depth_ref[:, at_after], depth_ref[:, at_before])

                @pl.when(yo != y)
                def _():
                    dep_copy(yo).start()

                @pl.when(yo == y)
                def _():
                    pltpu.make_async_copy(
                        dsrc.at[yo], dep.at[pl.ds(pl.multiple_of(y * RL, 8), RL)], dep_r
                    ).start()

            @pl.when(jnp.logical_and(lax.rem(flat, stride) == 0, block == 0))
            def _():
                for f in range(3):
                    isrc[yo, f, :, :W] = init_ref[f, :, at_k]
                    isrc[yo, f, :, W:] = jnp.where(
                        lane_h < LANES // 2, init_ref[f, :, at_after], init_ref[f, :, at_before]
                    )

                @pl.when(yo != y)
                def _():
                    ini_copy(yo).start()

                @pl.when(yo == y)
                def _():
                    pltpu.make_async_copy(
                        isrc.at[yo], ini.at[:, pl.ds(pl.multiple_of(y * RL, 8), RL)], ini_r
                    ).start()

    owner_tables()
    for part in range(SPANS):
        wait_edges(0, part)
        for j in range(part * SPAN // LANES, (part + 1) * SPAN // LANES):
            cols = lanes_of(j)
            new = []
            for f in range(3):
                one = s0[f, :, cols] + s1[f, :, cols] + outer_rate(0, f, cols)
                s1[f, :, cols] = one
                new.append(
                    0.5 * one - (1.0 / 24.0) * u_ref[0, f, :, cols] - (1.0 / 6.0) * u_ref[1, f, :, cols]
                    + (5.0 / 24.0) * u_ref[2, f, :, cols]
                )
                g[f, :, cols] = new[f]
            put_edges(1, cols, [v[0:1] for v in new], [v[RL - 1 : RL] for v in new])
        send_edges(1, part)
    inner_rate(lambda j: ([g[f, :, lanes_of(j)] for f in range(3)], depth_ref[:, lanes_of(j)]), b)

    relay_chunks(range(NC))

    my_rows = pl.ds(pl.multiple_of(y * RL, 8), RL)

    def a2a(i, k):
        j = owner_of(k)
        if i == 0:
            src, dst = b.at[:, :, pl.ds(pl.multiple_of(k * W, LANES), W)], main.at[pb, :, my_rows]
        else:
            src, dst = halo_src.at[:, :, pl.ds(pl.multiple_of(k * LANES, LANES), LANES)], halo.at[pb, :, my_rows]

        @pl.when(j * stride != local)
        def _():
            pltpu.make_async_remote_copy(
                src_ref=src, dst_ref=dst, send_sem=a2a_s.at[i], recv_sem=a2a_r.at[i, pb],
                device_id=where(block * TG * SP + j * stride), device_id_type=MESH,
            ).start()

        @pl.when(j * stride == local)
        def _():
            pltpu.make_async_copy(src, dst, a2a_r.at[i, pb]).start()

    for part in range(SPANS):
        wait_edges(1, part)
        for j in range(part * SPAN // LANES, (part + 1) * SPAN // LANES):
            cols = lanes_of(j)
            for f in range(3):
                start, one = s0[f, :, cols], s1[f, :, cols]
                two = one + b[f, :, cols] + outer_rate(1, f, cols)
                b[f, :, cols] = (1.0 / 6.0) * two + (2.0 / 3.0) * one - (5.0 / 6.0) * start
                mid[f, :, cols] = one - 0.5 * (start + two)

    slot_of = lax.rem(lane_h + hw, LANES) // (2 * hw)

    def send_halo(k):
        lo, hi = ((k + 1) % K) * W, (k * W - LANES) % NX
        packed = [jnp.zeros((RL, LANES), jnp.float32) for _ in range(nh)]
        for f in range(3):
            z = jnp.where(lane_h < LANES // 2, b[f, :, lo : lo + LANES], b[f, :, hi : hi + LANES])
            slot = f % per
            if slot:
                z = pltpu.roll(z, 2 * hw * slot, 1)
            packed[f // per] = jnp.where(slot_of == slot, z, packed[f // per])
        for i in range(nh):
            halo_src[i, :, k * LANES : (k + 1) * LANES] = packed[i]

    def send_halos(ks):
        for k in ks:
            send_halo(k)
        for k in ks:
            a2a(1, k)

    def extended(own, tile):
        return jnp.concatenate([own, tile], axis=0)

    def late_chunk(c):
        tiles = [outer_tile([window(rdst.at[side, f], c) for side in range(sides)]) for f in range(3)]
        depth_tile = outer_tile([window(dhdst.at[side], c) for side in range(sides)])
        depth = extended(window(depth_ref, c), depth_tile)
        start = [extended(window(w.at[f], c), tiles[f]) for f in range(3)]
        once = periodic_rate(start, depth)
        twice = periodic_rate(once, depth)
        for f in range(3):
            one, two = once[f][:RL, :WC], twice[f][:RL, :WC]
            b[f, :, chunk(c)] = b[f, :, chunk(c)] + (0.5 * one + (1.0 / 24.0) * two)
            mid[f, :, chunk(c)] = mid[f, :, chunk(c)] - 0.125 * two

        @pl.loop(0, tpc)
        def _(i):
            a2a(0, c * tpc + lax.rem(mine + i, tpc))

    @pl.when(late)
    def _():
        for side in range(sides):
            depth_halo(side).wait_recv()
        arrived, known, sent = 0, set(), set()
        for step in range(1, NC + 1):
            c = step % NC
            while arrived < min(step + 2, NC):
                for side in range(sides):
                    relay(arrived, side).wait_recv()
                arrived += 1
            late_chunk(c)
            known.update(range(c * tpc, (c + 1) * tpc))
            ready = [k for k in range(K) if k not in sent and {(k - 1) % K, k, (k + 1) % K} <= known]
            sent.update(ready)
            send_halos(ready)

    @pl.when(jnp.logical_not(late))
    def _():
        @pl.loop(0, K)
        def _(i):
            c = i // tpc
            c = lax.rem(c * 2, NC) + lax.rem(y + c * 2 // NC, 2) if NC > 1 else c
            a2a(0, c * tpc + lax.rem(mine + i, tpc))

        send_halos(range(K))

    my_tile = pl.ds(pl.multiple_of(mine * W, LANES), W)
    my_group = mine // (K // GROUPS)

    def give_edges(t):
        for yo in range(SP):
            src, dst = eo.at[t * SP + yo], redge.at[:, :, :, my_tile]
            here = jnp.logical_and(t == pb, y == yo)

            @pl.when(jnp.logical_not(here))
            def _():
                pltpu.make_async_remote_copy(
                    src_ref=src, dst_ref=dst, send_sem=ret_s, recv_sem=ret_r.at[my_group],
                    device_id=(block * TG + t, yo), device_id_type=MESH,
                ).start()

            @pl.when(here)
            def _():
                pltpu.make_async_copy(src, dst, ret_r.at[my_group]).start()

    def give_begin(t, src):
        for yo in range(SP):
            dst = cb.at[:, :, my_tile]
            here = jnp.logical_and(t == pb, y == yo)

            @pl.when(jnp.logical_not(here))
            def _():
                pltpu.make_async_remote_copy(
                    src_ref=src.at[yo], dst_ref=dst, send_sem=beg_s.at[t * SP + yo], recv_sem=beg_r.at[my_group],
                    device_id=(block * TG + t, yo), device_id_type=MESH,
                ).start()

            @pl.when(here)
            def _():
                pltpu.make_async_copy(src.at[yo], dst, beg_r.at[my_group]).start()

    def give(t):
        give_edges(t)

        @pl.when(jnp.logical_and(lax.rem(t, 2) == 1, t < TG - 1))
        def _():
            give_begin(t + 1, cs.at[pl.ds(t * SP, SP)])

    def carry():
        ends = ((cs.at[pl.ds((TG - 1) * SP, SP)], cin), (chalo_src, chalo))
        return [
            pltpu.make_async_remote_copy(
                src_ref=src, dst_ref=dst, send_sem=c_s.at[i], recv_sem=c_r.at[i],
                device_id=(lax.rem(p + TG, T), y), device_id_type=MESH,
            )
            for i, (src, dst) in enumerate(ends)
        ]

    def unpack(tile, f):
        return pltpu.roll(tile, LANES - 2 * hw * (f % per), 1) if f % per else tile

    def whole(ref, sem):
        pltpu.make_async_copy(ref, ref, sem).wait()

    R = SP * RL

    @pl.when(is_owner)
    def _():
        whole(dep, dep_r)

        ring = W // LANES + 1
        tall = lax.broadcasted_iota(jnp.int32, (R, LANES), 1)

        def turn(t, carried):
            whole(main.at[t], a2a_r.at[0, t])
            whole(halo.at[t], a2a_r.at[1, t])
            cur = [[state[f, :, lanes_of(j)] for f in range(3)] for j in range(ring)]

            def load(j):
                sent = [main[t, f, :, lanes_of(j)] if j < ring - 1 else unpack(halo[t, f // per], f) for f in range(3)]
                return [cur[j][f] + sent[f] for f in range(3)], dep[:, lanes_of(j)]

            def visit(j, before, tile, after):
                for f in range(3):
                    value = cur[j][f] + (
                        column_sum(before, tile, after, f, tall) + shift_up(tile.ups[f]) + shift_down(tile.downs[f])
                    )
                    state[f, :, lanes_of(j)] = value
                    if j < ring - 1:
                        for yo in range(SP):
                            cs[t * SP + yo, f, :, lanes_of(j)] = value[yo * RL : (yo + 1) * RL]
                            below, above = (yo + 1) * RL % R, (yo * RL - 1) % R
                            eo[t * SP + yo, 0, f, :, lanes_of(j)] = tile.ups[f][below : below + 1]
                            eo[t * SP + yo, 1, f, :, lanes_of(j)] = tile.downs[f][above : above + 1]

            walk(load, range(ring), ring, visit)

            @pl.when(jnp.logical_and(t > 0, block == NG - 1))
            def _():
                give(t - 1)

            return carried

        @pl.when(block == 0)
        def _():
            whole(ini, ini_r)
            state[...] = ini[...]

        @pl.when(block > 0)
        def _():
            for copy in carry():
                copy.wait_recv()
            give_begin(0, cin)
            for f in range(3):
                for yo in range(SP):
                    state[f, yo * RL : (yo + 1) * RL, :W] = cin[yo, f]
                state[f, :, W:] = unpack(chalo[f // per], f)

        lax.fori_loop(0, TG, turn, 0)

        @pl.when(block == NG - 1)
        def _():
            give(TG - 1)

        @pl.when(block < NG - 1)
        def _():
            lanes = lax.broadcasted_iota(jnp.int32, (SP * RL, LANES), 1)
            slots = lax.rem(lanes + hw, LANES) // (2 * hw)
            for i in range(nh):
                packed = jnp.zeros((SP * RL, LANES), jnp.float32)
                for f in range(i * per, min(3, (i + 1) * per)):
                    z = state[f, :, W:]
                    if f % per:
                        z = pltpu.roll(z, 2 * hw * (f % per), 1)
                    packed = jnp.where(slots == f % per, z, packed)
                chalo_src[i] = packed
            pl.semaphore_wait(go_carry, 1)
            for copy in carry():
                copy.start()

            @pl.loop(0, TG)
            def _(t):
                give(t)

    width, part = NX // GROUPS, NX // PARTS

    def fwd(q):
        cols = pl.ds(q * part, part)
        return pltpu.make_async_remote_copy(
            src_ref=ce.at[:, :, cols], dst_ref=cb.at[:, :, cols],
            send_sem=fwd_s.at[q], recv_sem=fwd_r.at[q], device_id=(lax.rem(p + 1, T), y), device_id_type=MESH,
        )

    for q in range(GROUPS):
        whole(redge.at[:, :, :, pl.ds(q * width, width)], ret_r.at[q])

    @pl.when(p == 0)
    def _():
        cb[...] = init_ref[...]

    @pl.when(late)
    def _():
        for q in range(GROUPS):
            whole(cb.at[:, :, pl.ds(q * width, width)], beg_r.at[q])

    per_part = NT // PARTS

    def advance(q, made, visit_ends):
        def load(j):
            return [cb[f, :, lanes_of(j)] + b[f, :, lanes_of(j)] for f in range(3)], depth_ref[:, lanes_of(j)]

        def visit(j, before, tile, after):
            cols = lanes_of(j)
            visit_ends(cols, [
                cb[f, :, cols] + column_sum(before, tile, after, f, lane)
                + jnp.where(row == RL - 1, redge[0, f, :, cols], shift_up(tile.ups[f]))
                + jnp.where(row == 0, redge[1, f, :, cols], shift_down(tile.downs[f]))
                for f in range(3)
            ])

        walk(load, range(q * per_part, (q + 1) * per_part), NT, visit, made)

    def keep(cols, ends):
        for f in range(3):
            ce[f, :, cols] = ends[f]

    def emit(cols, ends):
        for f in range(3):
            start = cb[f, :, cols]
            out_ref[0, 0, f, :, cols] = start
            out_ref[0, 1, f, :, cols] = mid[f, :, cols] + 0.5 * (start + ends[f])
            out_ref[0, 2, f, :, cols] = ends[f]

    order = [PARTS - 1, *range(PARTS - 1)]

    @pl.when(even)
    def _():
        made = {}
        for q in order:
            advance(q, made, keep)
            fwd(q).start()
        for j in range(NT):
            emit(lanes_of(j), [ce[f, :, lanes_of(j)] for f in range(3)])
        for q in order:
            fwd(q).wait_send()

    @pl.when(odd)
    def _():
        made, arrived = {}, 0
        for q in range(PARTS):
            while arrived < min(q + 3, PARTS):
                fwd(order[arrived]).wait_recv()
                arrived += 1
            advance(q, made, emit)

    @pl.when(p < T - 1)
    def _():
        for c in range(NC):
            shift(c, w).wait_send()

    @pl.when(late)
    def _():
        for side in range(sides):
            depth_halo(side).wait_send()
            for c in range(NC):
                relay(c, side).wait_send()

    for stage in range(2):
        for side in range(2):
            for part in range(SPANS):
                edge_copy(stage, side, part).wait_send()
    for yo in range(SP):
        flat = pb * SP + yo

        @pl.when(jnp.logical_and(lax.rem(flat, stride) == 0, yo != y))
        def _():
            dep_copy(yo).wait_send()

            @pl.when(block == 0)
            def _():
                ini_copy(yo).wait_send()

    @pl.when(is_owner)
    def _():
        whole(b.at[:, :, pl.ds(0, (K - 1) * W)], a2a_s.at[0])
        whole(halo_src.at[:, :, pl.ds(0, (K - 1) * LANES)], a2a_s.at[1])
        whole(eo.at[pl.ds(0, TG * SP - 1)], ret_s)

        @pl.when(block < NG - 1)
        def _():
            for copy in carry():
                copy.wait_send()

        for t in range(0, TG, 2):
            for yo in range(SP):
                sent = jnp.logical_not(jnp.logical_and(t == pb, y == yo))
                if t == 0:
                    sent = jnp.logical_and(sent, block > 0)

                @pl.when(sent)
                def _():
                    pltpu.make_async_copy(cin.at[yo], cin.at[yo], beg_s.at[t * SP + yo]).wait()

    @pl.when(jnp.logical_not(is_owner))
    def _():
        whole(b, a2a_s.at[0])
        whole(halo_src, a2a_s.at[1])


def solution(mesh):
    T, SP = mesh.shape["tm"], mesh.shape["space"]

    def per_device(fine_nodes, init_state, mean_depth):
        RL, NX = mean_depth.shape
        NG = 2 if T % 4 == 0 else 1
        members = T // NG * SP
        W = max(LANES, NX // members)
        K = NX // W
        NC = CHUNKS if K % CHUNKS == 0 else 1
        stride = members // K
        hw = 8
        while hw < T:
            hw *= 2
        per = LANES // (2 * hw)
        nh = -(-3 // per)
        cfg = (T, SP, RL, NX, W, K, stride, hw, per, nh, NG, NC)
        f32, dma = jnp.float32, pltpu.SemaphoreType.DMA
        state = pltpu.VMEM((3, RL, NX), f32)
        R = RL * SP
        sides = 1 if SP == 2 else 2
        edges = pltpu.VMEM((2, 2, 3, 1, NX), f32)
        vmem = pl.BlockSpec(memory_space=pltpu.VMEM)
        return pl.pallas_call(
            functools.partial(kernel, cfg),
            out_shape=pltpu.VMEM(fine_nodes.shape, f32),
            in_specs=[pl.BlockSpec(memory_space=pl.ANY)] * 3,
            out_specs=vmem,
            scratch_shapes=[
                pltpu.VMEM((3, 3, RL, NX), f32), state, pltpu.VMEM((RL, NX), f32),
                state, state, state, state, state, state,
                pltpu.VMEM((nh, RL, K * LANES), f32),
                pltpu.VMEM((3, 2 * DEEP, NX), f32),
                pltpu.VMEM((sides, 3, 2 * DEEP, NX), f32),
                pltpu.VMEM((2 * DEEP, NX), f32),
                pltpu.VMEM((sides, 2 * DEEP, NX), f32),
                pltpu.VMEM((SP, RL, W + LANES), f32),
                pltpu.VMEM((R, W + LANES), f32),
                pltpu.VMEM((SP, 3, RL, W + LANES), f32),
                pltpu.VMEM((3, R, W + LANES), f32),
                pltpu.VMEM((T // NG, 3, R, W), f32),
                pltpu.VMEM((T // NG, nh, R, LANES), f32),
                pltpu.VMEM((members, 3, RL, W), f32),
                state, state,
                edges, edges,
                pltpu.VMEM((members, 2, 3, 1, W), f32),
                pltpu.VMEM((2, 3, 1, NX), f32),
                pltpu.VMEM((SP, 3, RL, W), f32),
                pltpu.VMEM((nh, R, LANES), f32),
                pltpu.VMEM((nh, R, LANES), f32),
                pltpu.VMEM((3, R, W + LANES), f32),
                dma((NC,)), dma((NC,)), dma((sides, NC)), dma((sides, NC)), dma((sides,)), dma((sides,)),
                dma((2, 2, SPANS)), dma((2, 2, SPANS)), dma((SP,)), dma, dma((SP,)), dma, dma((2,)), dma((2, T // NG)),
                dma, dma((GROUPS,)), dma((PARTS,)), dma((PARTS,)),
                dma((2,)), dma((2,)), dma((members,)), dma((GROUPS,)), dma((5,)),
                pltpu.SemaphoreType.REGULAR,
            ],
            compiler_params=pltpu.CompilerParams(
                collective_id=0, has_side_effects=True, vmem_limit_bytes=60 * 1024 * 1024
            ),
        )(fine_nodes, init_state, mean_depth)

    return jax.shard_map(
        per_device,
        mesh=mesh,
        in_specs=(P("tm", None, None, "space", None), P(None, "space", None), P("space", None)),
        out_specs=P("tm", None, None, "space", None),
        check_vma=False,
    )
```

```python
import functools

import jax
import jax.numpy as jnp
from jax import lax
from jax.experimental import pallas as pl
from jax.experimental.pallas import tpu as pltpu
from jax.sharding import PartitionSpec as P

MESH = pl.DeviceIdType.MESH
DT = 0.3
NU = 1.0 / 3.0
FC = 0.5
DIFF = DT * NU
HALF = DT * 0.5
TURN = DT * FC
LANES = 128
SUB = 8
DEEP = 2
CHUNKS = 4
SPREAD = 4
PARTS = 8
SPANS = 2
HOLD = 4


def shift_left(v):
    return pltpu.roll(v, v.shape[1] - 1, 1)


def shift_right(v):
    return pltpu.roll(v, 1, 1)


def shift_up(v):
    return pltpu.roll(v, v.shape[0] - 1, 0)


def shift_down(v):
    return pltpu.roll(v, 1, 0)


def row_terms(h, e, n, depth):
    dn = depth * n
    nh, ne, nn, hh = DIFF * h, DIFF * e, DIFF * n, HALF * h
    return (nh - dn, ne, nn - hh), (nh + dn, ne, nn + hh)


def column_terms(h, e, n, depth):
    de = depth * e
    nh, ne, nn, hh = DIFF * h, DIFF * e, DIFF * n, HALF * h
    return (
        shift_left(nh - de) + shift_right(nh + de) - 4.0 * nh,
        shift_left(ne - hh) + shift_right(ne + hh) - 4.0 * ne + TURN * n,
        shift_left(nn) + shift_right(nn) - 4.0 * nn - TURN * e,
    )


def periodic_rate(state, depth):
    rates = column_terms(*state, depth)
    ups, downs = row_terms(*state, depth)
    return [rates[f] + shift_up(ups[f]) + shift_down(downs[f]) for f in range(3)]


class Tile:
    def __init__(self, state, depth):
        h, e, n = state
        de, dn = depth * e, depth * n
        nh, ne, nn, hh = DIFF * h, DIFF * e, DIFF * n, HALF * h
        self.lefts = [shift_left(x) for x in (nh - de, ne - hh, nn)]
        self.rights = [shift_right(x) for x in (nh + de, ne + hh, nn)]
        self.ups, self.downs = (nh - dn, ne, nn - hh), (nh + dn, ne, nn + hh)
        self.own = (-4.0 * nh, TURN * n - 4.0 * ne, -4.0 * nn - TURN * e)


def column_sum(before, tile, after, f, lane):
    return (
        tile.own[f]
        + jnp.where(lane == LANES - 1, after.lefts[f], tile.lefts[f])
        + jnp.where(lane == 0, before.rights[f], tile.rights[f])
    )


def walk(load, tiles, count, visit, made=None):
    made = {} if made is None else made

    def tile(i):
        i %= count
        if i not in made:
            made[i] = Tile(*load(i))
        return made[i]

    for j in tiles:
        visit(j, tile(j - 1), tile(j), tile(j + 1))
        if count > 4:
            made.pop((j - 1) % count)


def kernel(
    cfg, u_hbm, init_hbm, depth_hbm, out_ref, u_ref, init_ref, depth_ref,
    w, s0, g, s1, mid, b, halo_src, rsrc, rdst, dhsrc, dhdst, dsrc, dep, isrc, ini, main, halo, cs, ce, cb,
    esrc, edst, eo, redge, cin, chalo, chalo_src, state,
    shift_s, shift_r, rel_s, rel_r, dh_s, dh_r, edge_s, edge_r, dep_s, dep_r, ini_s, ini_r, a2a_s, a2a_r, ret_s, ret_r,
    fwd_s, fwd_r, c_s, c_r, beg_s, beg_r, in_s, go_carry,
):
    T, SP, RL, NX, W, K, stride, hw, per, nh, NG, NC = cfg
    TG = T // NG
    WC = NX // NC
    tpc = K // NC
    sides = 1 if SP == 2 else 2
    p, y = lax.axis_index("tm"), lax.axis_index("space")
    block = p // TG
    pb = p - block * TG
    local = pb * SP + y
    is_owner = lax.rem(local, stride) == 0
    even = lax.rem(p, 2) == 0
    odd = jnp.logical_not(even)
    late = jnp.logical_and(even, p > 0)

    spread = SPREAD if NC % SPREAD == 0 else 1

    def tile_of(j):
        high, low = j // (tpc * spread), lax.rem(j, spread)
        return (high * spread + low) * tpc + lax.rem(j // spread, tpc)

    def owner_of(k):
        c = k // tpc
        return c // spread * (tpc * spread) + lax.rem(k, tpc) * spread + lax.rem(c, spread)

    mine = tile_of(local // stride)

    def where(flat):
        return (flat // SP, lax.rem(flat, SP))

    def row_neighbour(side):
        return lax.rem(y + SP - 1, SP) if side == 0 else lax.rem(y + 1, SP)

    barrier = pltpu.get_barrier_semaphore()

    members = TG * SP
    has_next, has_last = block < NG - 1, block > 0
    crosses = jnp.logical_and(has_next, pb == TG - 1)

    def announce(sem, pp):
        pl.semaphore_signal(sem, inc=1, device_id=(pp, y), device_id_type=MESH)

    @pl.loop(1, members)
    def _(i):
        pl.semaphore_signal(
            barrier, inc=1, device_id=where(block * members + lax.rem(local + i, members)), device_id_type=MESH
        )

    @pl.when(has_next)
    def _():
        announce(barrier, lax.rem(p + TG, T))

    @pl.when(crosses)
    def _():
        announce(barrier, lax.rem(p + 1, T))

    loads = [pltpu.make_async_copy(u_hbm.at[0, i], u_ref.at[i], in_s.at[i]) for i in (2, 0, 1)]
    loads.append(pltpu.make_async_copy(depth_hbm, depth_ref, in_s.at[3]))
    loads.append(pltpu.make_async_copy(init_hbm, init_ref, in_s.at[4]))
    for copy in loads:
        copy.start()
    loads[0].wait()
    first_of_block = jnp.logical_and(has_last, pb == 0)
    meets = jnp.logical_or(crosses, first_of_block)

    @pl.when(first_of_block)
    def _():
        announce(barrier, lax.rem(p + T - 1, T))

    pl.semaphore_wait(barrier, members - 1 + has_last.astype(jnp.int32) + meets.astype(jnp.int32))

    @pl.when(has_last)
    def _():
        announce(go_carry, lax.rem(p + T - TG, T))

    def whole(ref, sem):
        pltpu.make_async_copy(ref, ref, sem).wait()

    def chunk(c):
        return pl.ds(c * WC, WC)

    def shift(c, dst):
        return pltpu.make_async_remote_copy(
            src_ref=u_ref.at[2, :, :, chunk(c)], dst_ref=dst.at[:, :, chunk(c)],
            send_sem=shift_s, recv_sem=shift_r.at[c],
            device_id=(lax.rem(p + 1, T), y), device_id_type=MESH,
        )

    @pl.when(jnp.logical_and(odd, p < T - 1))
    def _():
        for c in range(NC):
            shift(c, w).start()

    @pl.when(even)
    def _():
        for c in range(NC):
            shift(c, s0).start()

    for copy in loads[1:]:
        copy.wait()

    depth_ref[...] = HALF * depth_ref[...]

    lane_h = lax.broadcasted_iota(jnp.int32, (RL, LANES), 1)

    def outer_rows(own):
        sub = lax.broadcasted_iota(jnp.int32, (SUB, own.shape[1]), 0)
        return jnp.where(sub < DEEP, own[:SUB], pltpu.roll(own[RL - SUB :], SUB - 2 * DEEP, 0))[: 2 * DEEP]

    def outer_tile(parts):
        if sides == 1:
            both = parts[0]
        else:
            sub = lax.broadcasted_iota(jnp.int32, parts[0].shape, 0)
            both = jnp.where(sub < DEEP, parts[0], parts[1])
        return jnp.concatenate([both] * (SUB // (2 * DEEP)), axis=0)


    def margin(ref, c, size):
        after = ref[:, pl.ds((c + 1) * size % NX, LANES)]
        before = ref[:, pl.ds((c * size - LANES) % NX, LANES)]
        lanes = lax.broadcasted_iota(jnp.int32, after.shape, 1)
        return jnp.where(lanes < LANES // 2, after, before)

    def window(ref, c, size=WC):
        return jnp.concatenate([ref[:, pl.ds(c * size, size)], margin(ref, c, size)], axis=1)

    def depth_halo(side):
        return pltpu.make_async_remote_copy(
            src_ref=dhsrc, dst_ref=dhdst.at[side], send_sem=dh_s.at[side], recv_sem=dh_r.at[side],
            device_id=(p, row_neighbour(side)), device_id_type=MESH,
        )

    @pl.when(late)
    def _():
        dhsrc[...] = outer_rows(depth_ref[...])
        for side in range(sides):
            depth_halo(side).start()
        s0[...] = jnp.zeros_like(s0)

    @pl.when(p == 0)
    def _():
        s0[...] = init_ref[...]

    @pl.when(odd)
    def _():
        for c in range(NC):
            shift(c, s0).wait_recv()

    row = lax.broadcasted_iota(jnp.int32, (RL, LANES), 0)
    lane = lax.broadcasted_iota(jnp.int32, (RL, LANES), 1)
    NT = NX // LANES
    SPAN = NX // SPANS

    def lanes_of(j):
        return slice(j * LANES, (j + 1) * LANES)

    def edge_copy(stage, side, part):
        cols = pl.ds(part * SPAN, SPAN)
        return pltpu.make_async_remote_copy(
            src_ref=esrc.at[stage, side, :, :, cols], dst_ref=edst.at[stage, side, :, :, cols],
            send_sem=edge_s, recv_sem=edge_r.at[stage, part],
            device_id=(p, row_neighbour(side)), device_id_type=MESH,
        )

    def put_edges(stage, cols, top, bottom):
        ups, _ = row_terms(*top, depth_ref[0:1, cols])
        _, downs = row_terms(*bottom, depth_ref[RL - 1 : RL, cols])
        for f in range(3):
            esrc[stage, 0, f, :, cols] = ups[f]
            esrc[stage, 1, f, :, cols] = downs[f]

    def send_edges(stage, part):
        for side in range(2):
            edge_copy(stage, side, part).start()

    def wait_edges(stage, part):
        whole(edst.at[stage, :, :, :, pl.ds(part * SPAN, SPAN)], edge_r.at[stage, part])

    def inner_rate(load, out):
        def visit(j, before, tile, after):
            for f in range(3):
                out[f, :, lanes_of(j)] = (
                    column_sum(before, tile, after, f, lane)
                    + jnp.where(row == RL - 1, 0.0, shift_up(tile.ups[f]))
                    + jnp.where(row == 0, 0.0, shift_down(tile.downs[f]))
                )

        walk(load, range(NT), NT, visit)

    def outer_rate(stage, f, cols):
        return jnp.where(
            row == RL - 1, edst[stage, 0, f, :, cols], jnp.where(row == 0, edst[stage, 1, f, :, cols], 0.0)
        )

    def relay(c, side):
        return pltpu.make_async_remote_copy(
            src_ref=rsrc.at[:, :, chunk(c)], dst_ref=rdst.at[side, :, :, chunk(c)],
            send_sem=rel_s.at[side], recv_sem=rel_r.at[side, c],
            device_id=(p, row_neighbour(side)), device_id_type=MESH,
        )

    def relay_chunks(chunks):
        @pl.when(late)
        def _():
            for c in chunks:
                shift(c, w).wait_recv()
                for f in range(3):
                    rsrc[f, :, chunk(c)] = outer_rows(w[f, :, chunk(c)])
                for side in range(sides):
                    relay(c, side).start()

    def first_g(rows, cols, f):
        return (
            (-7.0 / 24.0) * u_ref[0, f, rows, cols] + (1.0 / 3.0) * u_ref[1, f, rows, cols]
            - (1.0 / 24.0) * u_ref[2, f, rows, cols] + 0.5 * s0[f, rows, cols]
        )

    every = slice(0, RL)
    for part in range(SPANS):
        for j in range(part * SPAN // LANES, (part + 1) * SPAN // LANES):
            put_edges(0, lanes_of(j), *([first_g(slice(r, r + 1), lanes_of(j), f) for f in range(3)] for r in (0, RL - 1)))
        send_edges(0, part)
    inner_rate(
        lambda j: ([first_g(every, lanes_of(j), f) for f in range(3)], depth_ref[:, lanes_of(j)]), s1
    )

    def dep_copy(yo):
        return pltpu.make_async_remote_copy(
            src_ref=dsrc.at[yo], dst_ref=dep.at[pl.ds(pl.multiple_of(y * RL, 8), RL)],
            send_sem=dep_s.at[yo], recv_sem=dep_r, device_id=(p, yo), device_id_type=MESH,
        )

    def ini_copy(yo):
        return pltpu.make_async_remote_copy(
            src_ref=isrc.at[yo], dst_ref=ini.at[:, pl.ds(pl.multiple_of(y * RL, 8), RL)],
            send_sem=ini_s.at[yo], recv_sem=ini_r, device_id=(p, yo), device_id_type=MESH,
        )

    def owner_tables():
        for yo in range(SP):
            flat = pb * SP + yo
            k = tile_of(flat // stride)
            at_k = pl.ds(pl.multiple_of(k * W, LANES), W)
            at_after = pl.ds(pl.multiple_of(lax.rem((k + 1) * W, NX), LANES), LANES)
            at_before = pl.ds(pl.multiple_of(lax.rem(k * W + NX - LANES, NX), LANES), LANES)

            @pl.when(lax.rem(flat, stride) == 0)
            def _():
                dsrc[yo, :, :W] = depth_ref[:, at_k]
                dsrc[yo, :, W:] = jnp.where(lane_h < LANES // 2, depth_ref[:, at_after], depth_ref[:, at_before])

                @pl.when(yo != y)
                def _():
                    dep_copy(yo).start()

                @pl.when(yo == y)
                def _():
                    pltpu.make_async_copy(
                        dsrc.at[yo], dep.at[pl.ds(pl.multiple_of(y * RL, 8), RL)], dep_r
                    ).start()

            @pl.when(jnp.logical_and(lax.rem(flat, stride) == 0, block == 0))
            def _():
                for f in range(3):
                    isrc[yo, f, :, :W] = init_ref[f, :, at_k]
                    isrc[yo, f, :, W:] = jnp.where(
                        lane_h < LANES // 2, init_ref[f, :, at_after], init_ref[f, :, at_before]
                    )

                @pl.when(yo != y)
                def _():
                    ini_copy(yo).start()

                @pl.when(yo == y)
                def _():
                    pltpu.make_async_copy(
                        isrc.at[yo], ini.at[:, pl.ds(pl.multiple_of(y * RL, 8), RL)], ini_r
                    ).start()

    owner_tables()
    for part in range(SPANS):
        wait_edges(0, part)
        for j in range(part * SPAN // LANES, (part + 1) * SPAN // LANES):
            cols = lanes_of(j)
            new = []
            for f in range(3):
                one = s0[f, :, cols] + s1[f, :, cols] + outer_rate(0, f, cols)
                s1[f, :, cols] = one
                new.append(
                    0.5 * one - (1.0 / 24.0) * u_ref[0, f, :, cols] - (1.0 / 6.0) * u_ref[1, f, :, cols]
                    + (5.0 / 24.0) * u_ref[2, f, :, cols]
                )
                g[f, :, cols] = new[f]
            put_edges(1, cols, [v[0:1] for v in new], [v[RL - 1 : RL] for v in new])

        @pl.when(jnp.logical_not(late))
        def _():
            send_edges(1, part)

    inner_rate(lambda j: ([g[f, :, lanes_of(j)] for f in range(3)], depth_ref[:, lanes_of(j)]), b)

    relay_chunks(range(HOLD * NC // 8))

    @pl.when(late)
    def _():
        for part in range(SPANS):
            send_edges(1, part)

    relay_chunks(range(HOLD * NC // 8, NC))

    my_rows = pl.ds(pl.multiple_of(y * RL, 8), RL)

    def a2a(i, k):
        j = owner_of(k)
        if i == 0:
            src, dst = b.at[:, :, pl.ds(pl.multiple_of(k * W, LANES), W)], main.at[pb, :, my_rows]
        else:
            src, dst = halo_src.at[:, :, pl.ds(pl.multiple_of(k * LANES, LANES), LANES)], halo.at[pb, :, my_rows]

        @pl.when(j * stride != local)
        def _():
            pltpu.make_async_remote_copy(
                src_ref=src, dst_ref=dst, send_sem=a2a_s.at[i], recv_sem=a2a_r.at[i, pb],
                device_id=where(block * TG * SP + j * stride), device_id_type=MESH,
            ).start()

        @pl.when(j * stride == local)
        def _():
            pltpu.make_async_copy(src, dst, a2a_r.at[i, pb]).start()

    for part in range(SPANS):
        wait_edges(1, part)
        for j in range(part * SPAN // LANES, (part + 1) * SPAN // LANES):
            cols = lanes_of(j)
            for f in range(3):
                start, one = s0[f, :, cols], s1[f, :, cols]
                two = one + b[f, :, cols] + outer_rate(1, f, cols)
                b[f, :, cols] = (1.0 / 6.0) * two + (2.0 / 3.0) * one - (5.0 / 6.0) * start
                mid[f, :, cols] = one - 0.5 * (start + two)

    slot_of = lax.rem(lane_h + hw, LANES) // (2 * hw)

    def send_halo(k):
        lo, hi = ((k + 1) % K) * W, (k * W - LANES) % NX
        packed = [jnp.zeros((RL, LANES), jnp.float32) for _ in range(nh)]
        for f in range(3):
            z = jnp.where(lane_h < LANES // 2, b[f, :, lo : lo + LANES], b[f, :, hi : hi + LANES])
            slot = f % per
            if slot:
                z = pltpu.roll(z, 2 * hw * slot, 1)
            packed[f // per] = jnp.where(slot_of == slot, z, packed[f // per])
        for i in range(nh):
            halo_src[i, :, k * LANES : (k + 1) * LANES] = packed[i]

    def send_halos(ks):
        for k in ks:
            send_halo(k)
        for k in ks:
            a2a(1, k)

    def extended(own, tile):
        return jnp.concatenate([own, tile], axis=0)

    def late_chunk(c):
        tiles = [outer_tile([window(rdst.at[side, f], c) for side in range(sides)]) for f in range(3)]
        depth_tile = outer_tile([window(dhdst.at[side], c) for side in range(sides)])
        depth = extended(window(depth_ref, c), depth_tile)
        start = [extended(window(w.at[f], c), tiles[f]) for f in range(3)]
        once = periodic_rate(start, depth)
        twice = periodic_rate(once, depth)
        for f in range(3):
            one, two = once[f][:RL, :WC], twice[f][:RL, :WC]
            b[f, :, chunk(c)] = b[f, :, chunk(c)] + (0.5 * one + (1.0 / 24.0) * two)
            mid[f, :, chunk(c)] = mid[f, :, chunk(c)] - 0.125 * two

        @pl.loop(0, tpc)
        def _(i):
            a2a(0, c * tpc + lax.rem(mine + i, tpc))

    @pl.when(late)
    def _():
        for side in range(sides):
            depth_halo(side).wait_recv()
        arrived, known, sent = 0, set(), set()
        for step in range(1, NC + 1):
            c = step % NC
            while arrived < min(step + 2, NC):
                for side in range(sides):
                    relay(arrived, side).wait_recv()
                arrived += 1
            late_chunk(c)
            known.update(range(c * tpc, (c + 1) * tpc))
            ready = [k for k in range(K) if k not in sent and {(k - 1) % K, k, (k + 1) % K} <= known]
            sent.update(ready)
            send_halos(ready)

    @pl.when(jnp.logical_not(late))
    def _():
        @pl.loop(0, K)
        def _(i):
            c = i // tpc
            c = lax.rem(c * 2, NC) + lax.rem(y + c * 2 // NC, 2) if NC > 1 else c
            a2a(0, c * tpc + lax.rem(mine + i, tpc))

        send_halos(range(K))

    NS = W // LANES

    def my_lanes(i):
        return pl.ds(pl.multiple_of(mine * W + i * LANES, LANES), LANES)

    def hand(src, dst, send, recv, t, yo):
        here = jnp.logical_and(t == pb, y == yo)

        @pl.when(jnp.logical_not(here))
        def _():
            pltpu.make_async_remote_copy(
                src_ref=src, dst_ref=dst, send_sem=send, recv_sem=recv,
                device_id=(block * TG + t, yo), device_id_type=MESH,
            ).start()

        @pl.when(here)
        def _():
            pltpu.make_async_copy(src, dst, recv).start()

    def give_begin(i, t, src):
        for yo in range(SP):
            hand(src.at[yo], cb.at[:, :, my_lanes(i)], beg_s, beg_r, t, yo)

    def give(i, t):
        for yo in range(SP):
            hand(eo.at[i, t * SP + yo], redge.at[:, :, :, my_lanes(i)], ret_s, ret_r, t, yo)

        @pl.when(jnp.logical_and(lax.rem(t, 2) == 1, t < TG - 1))
        def _():
            give_begin(i, t + 1, cs.at[i, pl.ds(t * SP, SP)])

    def carry(i):
        ends = ((cs.at[i, pl.ds((TG - 1) * SP, SP)], cin.at[i]), (chalo_src.at[i], chalo.at[i]))
        return [
            pltpu.make_async_remote_copy(
                src_ref=src, dst_ref=dst, send_sem=c_s.at[i, e], recv_sem=c_r.at[i, e],
                device_id=(lax.rem(p + TG, T), y), device_id_type=MESH,
            )
            for e, (src, dst) in enumerate(ends)
        ]

    def unpack(tile, f):
        return pltpu.roll(tile, LANES - 2 * hw * (f % per), 1) if f % per else tile

    R = SP * RL

    @pl.when(is_owner)
    def _():
        whole(dep, dep_r)

        tall = lax.broadcasted_iota(jnp.int32, (R, LANES), 1)
        slots = lax.rem(tall + hw, LANES) // (2 * hw)

        def beside(block_of, outer, i):
            if NS == 1:
                return outer()
            after = block_of(i + 1) if i < NS - 1 else outer()
            before = block_of(i - 1) if i > 0 else outer()
            return jnp.where(tall < LANES // 2, after, before)

        def turn(i, t, carried):
            if i == 0:
                whole(main.at[t], a2a_r.at[0, t])
                whole(halo.at[t], a2a_r.at[1, t])
            cur = [[state[i, f, :, lanes_of(j)] for f in range(3)] for j in range(2)]
            depths = [dep[:, lanes_of(i)], beside(lambda m: dep[:, lanes_of(m)], lambda: dep[:, W:], i)]

            def load(j):
                if j == 0:
                    sent = [main[t, f, :, lanes_of(i)] for f in range(3)]
                else:
                    sent = [
                        beside(lambda m: main[t, f, :, lanes_of(m)], lambda: unpack(halo[t, f // per], f), i)
                        for f in range(3)
                    ]
                return [cur[j][f] + sent[f] for f in range(3)], depths[j]

            def visit(j, before, tile, after):
                for f in range(3):
                    value = cur[j][f] + (
                        column_sum(before, tile, after, f, tall) + shift_up(tile.ups[f]) + shift_down(tile.downs[f])
                    )
                    state[i, f, :, lanes_of(j)] = value
                    if j == 0:
                        for yo in range(SP):
                            cs[i, t * SP + yo, f] = value[yo * RL : (yo + 1) * RL]
                            below, above = (yo + 1) * RL % R, (yo * RL - 1) % R
                            eo[i, t * SP + yo, 0, f] = tile.ups[f][below : below + 1]
                            eo[i, t * SP + yo, 1, f] = tile.downs[f][above : above + 1]

            walk(load, range(2), 2, visit)

            @pl.when(jnp.logical_and(t > 0, block == NG - 1))
            def _():
                give(i, t - 1)

            return carried

        @pl.when(block == 0)
        def _():
            whole(ini, ini_r)
            for i in range(NS):
                for f in range(3):
                    state[i, f, :, :LANES] = ini[f, :, lanes_of(i)]
                    state[i, f, :, LANES:] = beside(lambda m: ini[f, :, lanes_of(m)], lambda: ini[f, :, W:], i)

        for i in range(NS):
            @pl.when(block > 0)
            def _():
                for copy in carry(i):
                    copy.wait_recv()
                give_begin(i, 0, cin.at[i])
                for f in range(3):
                    for yo in range(SP):
                        state[i, f, yo * RL : (yo + 1) * RL, :LANES] = cin[i, yo, f]
                    state[i, f, :, LANES:] = unpack(chalo[i, f // per], f)

            lax.fori_loop(0, TG, functools.partial(turn, i), 0)

            @pl.when(block == NG - 1)
            def _():
                give(i, TG - 1)

            @pl.when(block < NG - 1)
            def _():
                for e in range(nh):
                    packed = jnp.zeros((R, LANES), jnp.float32)
                    for f in range(e * per, min(3, (e + 1) * per)):
                        z = state[i, f, :, LANES:]
                        if f % per:
                            z = pltpu.roll(z, 2 * hw * (f % per), 1)
                        packed = jnp.where(slots == f % per, z, packed)
                    chalo_src[i, e] = packed
                if i == 0:
                    pl.semaphore_wait(go_carry, 1)
                for copy in carry(i):
                    copy.start()

        @pl.when(block < NG - 1)
        def _():
            @pl.loop(0, TG)
            def _(t):
                for i in range(NS):
                    give(i, t)

    part = NX // PARTS

    def fwd(q):
        cols = pl.ds(q * part, part)
        return pltpu.make_async_remote_copy(
            src_ref=ce.at[:, :, cols], dst_ref=cb.at[:, :, cols],
            send_sem=fwd_s, recv_sem=fwd_r.at[q], device_id=(lax.rem(p + 1, T), y), device_id_type=MESH,
        )

    whole(redge, ret_r)

    @pl.when(p == 0)
    def _():
        cb[...] = init_ref[...]

    @pl.when(late)
    def _():
        whole(cb, beg_r)

    per_part = NT // PARTS

    def advance(q, made, visit_ends):
        def load(j):
            return [cb[f, :, lanes_of(j)] + b[f, :, lanes_of(j)] for f in range(3)], depth_ref[:, lanes_of(j)]

        def visit(j, before, tile, after):
            cols = lanes_of(j)
            visit_ends(cols, [
                cb[f, :, cols] + column_sum(before, tile, after, f, lane)
                + jnp.where(row == RL - 1, redge[0, f, :, cols], shift_up(tile.ups[f]))
                + jnp.where(row == 0, redge[1, f, :, cols], shift_down(tile.downs[f]))
                for f in range(3)
            ])

        walk(load, range(q * per_part, (q + 1) * per_part), NT, visit, made)

    def keep(cols, ends):
        for f in range(3):
            ce[f, :, cols] = ends[f]

    def emit(cols, ends):
        for f in range(3):
            start = cb[f, :, cols]
            out_ref[0, 0, f, :, cols] = start
            out_ref[0, 1, f, :, cols] = mid[f, :, cols] + 0.5 * (start + ends[f])
            out_ref[0, 2, f, :, cols] = ends[f]

    order = [PARTS - 1, *range(PARTS - 1)]

    @pl.when(even)
    def _():
        made = {}
        for q in order:
            advance(q, made, keep)
            fwd(q).start()
        for j in range(NT):
            emit(lanes_of(j), [ce[f, :, lanes_of(j)] for f in range(3)])
        whole(ce, fwd_s)

    @pl.when(odd)
    def _():
        made, arrived = {}, 0
        for q in range(PARTS):
            while arrived < min(q + 3, PARTS):
                fwd(order[arrived]).wait_recv()
                arrived += 1
            advance(q, made, emit)

    @pl.when(p < T - 1)
    def _():
        whole(u_ref.at[2], shift_s)

    @pl.when(late)
    def _():
        for side in range(sides):
            depth_halo(side).wait_send()
            whole(rsrc, rel_s.at[side])

    whole(esrc, edge_s)
    for yo in range(SP):
        flat = pb * SP + yo

        @pl.when(jnp.logical_and(lax.rem(flat, stride) == 0, yo != y))
        def _():
            dep_copy(yo).wait_send()

            @pl.when(block == 0)
            def _():
                ini_copy(yo).wait_send()

    @pl.when(is_owner)
    def _():
        whole(b.at[:, :, pl.ds(0, (K - 1) * W)], a2a_s.at[0])
        whole(halo_src.at[:, :, pl.ds(0, (K - 1) * LANES)], a2a_s.at[1])
        for i in range(NS):
            whole(eo.at[i, pl.ds(0, TG * SP - 1)], ret_s)

        @pl.when(block < NG - 1)
        def _():
            for i in range(NS):
                for copy in carry(i):
                    copy.wait_send()

        own = jnp.logical_and(even, p > 0).astype(jnp.int32)
        begins = (TG + 1) // 2 * SP - own - jnp.where(block == 0, SP, 0)
        for n in ((TG + 1) // 2 * SP - a - c for a in range(2) for c in (0, SP)):
            @pl.when(begins == n)
            def _():
                for i in range(NS):
                    whole(cs.at[i, pl.ds(0, n)], beg_s)

    @pl.when(jnp.logical_not(is_owner))
    def _():
        whole(b, a2a_s.at[0])
        whole(halo_src, a2a_s.at[1])


def solution(mesh):
    T, SP = mesh.shape["tm"], mesh.shape["space"]

    def per_device(fine_nodes, init_state, mean_depth):
        RL, NX = mean_depth.shape
        NG = 2 if T % 4 == 0 else 1
        members = T // NG * SP
        W = max(LANES, NX // members)
        K = NX // W
        NC = CHUNKS if K % CHUNKS == 0 else 1
        stride = members // K
        hw = 8
        while hw < T:
            hw *= 2
        per = LANES // (2 * hw)
        nh = -(-3 // per)
        cfg = (T, SP, RL, NX, W, K, stride, hw, per, nh, NG, NC)
        f32, dma = jnp.float32, pltpu.SemaphoreType.DMA
        state = pltpu.VMEM((3, RL, NX), f32)
        R = RL * SP
        sides = 1 if SP == 2 else 2
        edges = pltpu.VMEM((2, 2, 3, 1, NX), f32)
        vmem = pl.BlockSpec(memory_space=pltpu.VMEM)
        return pl.pallas_call(
            functools.partial(kernel, cfg),
            out_shape=pltpu.VMEM(fine_nodes.shape, f32),
            in_specs=[pl.BlockSpec(memory_space=pl.ANY)] * 3,
            out_specs=vmem,
            scratch_shapes=[
                pltpu.VMEM((3, 3, RL, NX), f32), state, pltpu.VMEM((RL, NX), f32),
                state, state, state, state, state, state,
                pltpu.VMEM((nh, RL, K * LANES), f32),
                pltpu.VMEM((3, 2 * DEEP, NX), f32),
                pltpu.VMEM((sides, 3, 2 * DEEP, NX), f32),
                pltpu.VMEM((2 * DEEP, NX), f32),
                pltpu.VMEM((sides, 2 * DEEP, NX), f32),
                pltpu.VMEM((SP, RL, W + LANES), f32),
                pltpu.VMEM((R, W + LANES), f32),
                pltpu.VMEM((SP, 3, RL, W + LANES), f32),
                pltpu.VMEM((3, R, W + LANES), f32),
                pltpu.VMEM((T // NG, 3, R, W), f32),
                pltpu.VMEM((T // NG, nh, R, LANES), f32),
                pltpu.VMEM((W // LANES, members, 3, RL, LANES), f32),
                state, state,
                edges, edges,
                pltpu.VMEM((W // LANES, members, 2, 3, 1, LANES), f32),
                pltpu.VMEM((2, 3, 1, NX), f32),
                pltpu.VMEM((W // LANES, SP, 3, RL, LANES), f32),
                pltpu.VMEM((W // LANES, nh, R, LANES), f32),
                pltpu.VMEM((W // LANES, nh, R, LANES), f32),
                pltpu.VMEM((W // LANES, 3, R, 2 * LANES), f32),
                dma, dma((NC,)), dma((sides,)), dma((sides, NC)), dma((sides,)), dma((sides,)),
                dma, dma((2, SPANS)), dma((SP,)), dma, dma((SP,)), dma, dma((2,)), dma((2, T // NG)),
                dma, dma, dma, dma((PARTS,)),
                dma((W // LANES, 2)), dma((W // LANES, 2)), dma, dma, dma((5,)),
                pltpu.SemaphoreType.REGULAR,
            ],
            compiler_params=pltpu.CompilerParams(
                collective_id=0, has_side_effects=True, vmem_limit_bytes=60 * 1024 * 1024
            ),
        )(fine_nodes, init_state, mean_depth)

    return jax.shard_map(
        per_device,
        mesh=mesh,
        in_specs=(P("tm", None, None, "space", None), P(None, "space", None), P("space", None)),
        out_specs=P("tm", None, None, "space", None),
        check_vma=False,
    )
```

```python
import functools

import jax
import jax.numpy as jnp
from jax import lax
from jax.experimental import pallas as pl
from jax.experimental.pallas import tpu as pltpu
from jax.sharding import PartitionSpec as P

MESH = pl.DeviceIdType.MESH
DT = 0.3
NU = 1.0 / 3.0
FC = 0.5
DIFF = DT * NU
HALF = DT * 0.5
TURN = DT * FC
LANES = 128
SUB = 8
DEEP = 2
CHUNKS = 4
SPREAD = 4
PARTS = 8
SPANS = 2
HOLD = 4


def shift_left(v):
    return pltpu.roll(v, v.shape[1] - 1, 1)


def shift_right(v):
    return pltpu.roll(v, 1, 1)


def shift_up(v):
    return pltpu.roll(v, v.shape[0] - 1, 0)


def shift_down(v):
    return pltpu.roll(v, 1, 0)


def row_terms(h, e, n, depth):
    dn = depth * n
    nh, ne, nn, hh = DIFF * h, DIFF * e, DIFF * n, HALF * h
    return (nh - dn, ne, nn - hh), (nh + dn, ne, nn + hh)


def column_terms(h, e, n, depth):
    de = depth * e
    nh, ne, nn, hh = DIFF * h, DIFF * e, DIFF * n, HALF * h
    return (
        shift_left(nh - de) + shift_right(nh + de) - 4.0 * nh,
        shift_left(ne - hh) + shift_right(ne + hh) - 4.0 * ne + TURN * n,
        shift_left(nn) + shift_right(nn) - 4.0 * nn - TURN * e,
    )


def periodic_rate(state, depth):
    rates = column_terms(*state, depth)
    ups, downs = row_terms(*state, depth)
    return [rates[f] + shift_up(ups[f]) + shift_down(downs[f]) for f in range(3)]


class Tile:
    def __init__(self, state, depth):
        h, e, n = state
        de, dn = depth * e, depth * n
        nh, ne, nn, hh = DIFF * h, DIFF * e, DIFF * n, HALF * h
        self.lefts = [shift_left(x) for x in (nh - de, ne - hh, nn)]
        self.rights = [shift_right(x) for x in (nh + de, ne + hh, nn)]
        self.ups, self.downs = (nh - dn, ne, nn - hh), (nh + dn, ne, nn + hh)
        self.own = (-4.0 * nh, TURN * n - 4.0 * ne, -4.0 * nn - TURN * e)


def column_sum(before, tile, after, f, lane):
    return (
        tile.own[f]
        + jnp.where(lane == LANES - 1, after.lefts[f], tile.lefts[f])
        + jnp.where(lane == 0, before.rights[f], tile.rights[f])
    )


def walk(load, tiles, count, visit, made=None):
    made = {} if made is None else made

    def tile(i):
        i %= count
        if i not in made:
            made[i] = Tile(*load(i))
        return made[i]

    for j in tiles:
        visit(j, tile(j - 1), tile(j), tile(j + 1))
        if count > 4:
            made.pop((j - 1) % count)


def kernel(
    cfg, u_hbm, init_hbm, depth_hbm, out_ref, u_ref, init_ref, depth_ref,
    w, s0, g, s1, mid, b, halo_src, rsrc, rdst, dhsrc, dhdst, dsrc, dep, isrc, ini, main, halo, cs, ce, cb,
    esrc, edst, eo, redge, cin, chalo, chalo_src, state,
    shift_s, shift_r, rel_s, rel_r, dh_s, dh_r, edge_s, edge_r, dep_s, dep_r, ini_s, ini_r, a2a_s, a2a_r, ret_s, ret_r,
    fwd_s, fwd_r, c_s, c_r, beg_s, beg_r, in_s, go_carry,
):
    T, SP, RL, NX, W, K, stride, hw, per, nh, NG, NC, carry_hw = cfg
    carry_slots = LANES // (2 * carry_hw)
    TG = T // NG
    WC = NX // NC
    tpc = K // NC
    sides = 1 if SP == 2 else 2
    p, y = lax.axis_index("tm"), lax.axis_index("space")
    block = p // TG
    pb = p - block * TG
    local = pb * SP + y
    is_owner = lax.rem(local, stride) == 0
    even = lax.rem(p, 2) == 0
    odd = jnp.logical_not(even)
    late = jnp.logical_and(even, p > 0)

    spread = SPREAD if NC % SPREAD == 0 else 1

    def tile_of(j):
        high, low = j // (tpc * spread), lax.rem(j, spread)
        return (high * spread + low) * tpc + lax.rem(j // spread, tpc)

    def owner_of(k):
        c = k // tpc
        return c // spread * (tpc * spread) + lax.rem(k, tpc) * spread + lax.rem(c, spread)

    mine = tile_of(local // stride)

    def where(flat):
        return (flat // SP, lax.rem(flat, SP))

    def row_neighbour(side):
        return lax.rem(y + SP - 1, SP) if side == 0 else lax.rem(y + 1, SP)

    barrier = pltpu.get_barrier_semaphore()

    members = TG * SP
    has_next, has_last = block < NG - 1, block > 0
    crosses = jnp.logical_and(has_next, pb == TG - 1)

    def announce(sem, pp):
        pl.semaphore_signal(sem, inc=1, device_id=(pp, y), device_id_type=MESH)

    @pl.loop(1, members)
    def _(i):
        pl.semaphore_signal(
            barrier, inc=1, device_id=where(block * members + lax.rem(local + i, members)), device_id_type=MESH
        )

    @pl.when(has_next)
    def _():
        announce(barrier, lax.rem(p + TG, T))

    @pl.when(crosses)
    def _():
        announce(barrier, lax.rem(p + 1, T))

    loads = [pltpu.make_async_copy(u_hbm.at[0, i], u_ref.at[i], in_s.at[i]) for i in (2, 0, 1)]
    loads.append(pltpu.make_async_copy(depth_hbm, depth_ref, in_s.at[3]))
    loads.append(pltpu.make_async_copy(init_hbm, init_ref, in_s.at[4]))
    for copy in loads:
        copy.start()
    loads[0].wait()
    first_of_block = jnp.logical_and(has_last, pb == 0)
    meets = jnp.logical_or(crosses, first_of_block)

    @pl.when(first_of_block)
    def _():
        announce(barrier, lax.rem(p + T - 1, T))

    pl.semaphore_wait(barrier, members - 1 + has_last.astype(jnp.int32) + meets.astype(jnp.int32))

    @pl.when(has_last)
    def _():
        announce(go_carry, lax.rem(p + T - TG, T))

    def whole(ref, sem):
        pltpu.make_async_copy(ref, ref, sem).wait()

    def chunk(c):
        return pl.ds(c * WC, WC)

    def shift(c, dst):
        return pltpu.make_async_remote_copy(
            src_ref=u_ref.at[2, :, :, chunk(c)], dst_ref=dst.at[:, :, chunk(c)],
            send_sem=shift_s, recv_sem=shift_r.at[c],
            device_id=(lax.rem(p + 1, T), y), device_id_type=MESH,
        )

    @pl.when(jnp.logical_and(odd, p < T - 1))
    def _():
        for c in range(NC):
            shift(c, w).start()

    @pl.when(even)
    def _():
        for c in range(NC):
            shift(c, s0).start()

    for copy in loads[1:]:
        copy.wait()

    depth_ref[...] = HALF * depth_ref[...]

    lane_h = lax.broadcasted_iota(jnp.int32, (RL, LANES), 1)

    def outer_rows(own):
        sub = lax.broadcasted_iota(jnp.int32, (SUB, own.shape[1]), 0)
        return jnp.where(sub < DEEP, own[:SUB], pltpu.roll(own[RL - SUB :], SUB - 2 * DEEP, 0))[: 2 * DEEP]

    def outer_tile(parts):
        if sides == 1:
            both = parts[0]
        else:
            sub = lax.broadcasted_iota(jnp.int32, parts[0].shape, 0)
            both = jnp.where(sub < DEEP, parts[0], parts[1])
        return jnp.concatenate([both] * (SUB // (2 * DEEP)), axis=0)


    def margin(ref, c, size):
        after = ref[:, pl.ds((c + 1) * size % NX, LANES)]
        before = ref[:, pl.ds((c * size - LANES) % NX, LANES)]
        lanes = lax.broadcasted_iota(jnp.int32, after.shape, 1)
        return jnp.where(lanes < LANES // 2, after, before)

    def window(ref, c, size=WC):
        return jnp.concatenate([ref[:, pl.ds(c * size, size)], margin(ref, c, size)], axis=1)

    def depth_halo(side):
        return pltpu.make_async_remote_copy(
            src_ref=dhsrc, dst_ref=dhdst.at[side], send_sem=dh_s.at[side], recv_sem=dh_r.at[side],
            device_id=(p, row_neighbour(side)), device_id_type=MESH,
        )

    @pl.when(late)
    def _():
        dhsrc[...] = outer_rows(depth_ref[...])
        for side in range(sides):
            depth_halo(side).start()
        s0[...] = jnp.zeros_like(s0)

    @pl.when(p == 0)
    def _():
        s0[...] = init_ref[...]

    @pl.when(odd)
    def _():
        for c in range(NC):
            shift(c, s0).wait_recv()

    row = lax.broadcasted_iota(jnp.int32, (RL, LANES), 0)
    lane = lax.broadcasted_iota(jnp.int32, (RL, LANES), 1)
    NT = NX // LANES
    SPAN = NX // SPANS

    def lanes_of(j):
        return slice(j * LANES, (j + 1) * LANES)

    def edge_copy(stage, side, part):
        cols = pl.ds(part * SPAN, SPAN)
        return pltpu.make_async_remote_copy(
            src_ref=esrc.at[stage, side, :, :, cols], dst_ref=edst.at[stage, side, :, :, cols],
            send_sem=edge_s, recv_sem=edge_r.at[stage, part],
            device_id=(p, row_neighbour(side)), device_id_type=MESH,
        )

    def put_edges(stage, cols, top, bottom):
        ups, _ = row_terms(*top, depth_ref[0:1, cols])
        _, downs = row_terms(*bottom, depth_ref[RL - 1 : RL, cols])
        for f in range(3):
            esrc[stage, 0, f, :, cols] = ups[f]
            esrc[stage, 1, f, :, cols] = downs[f]

    def send_edges(stage, part):
        for side in range(2):
            edge_copy(stage, side, part).start()

    def wait_edges(stage, part):
        whole(edst.at[stage, :, :, :, pl.ds(part * SPAN, SPAN)], edge_r.at[stage, part])

    def inner_rate(load, out):
        def visit(j, before, tile, after):
            for f in range(3):
                out[f, :, lanes_of(j)] = (
                    column_sum(before, tile, after, f, lane)
                    + jnp.where(row == RL - 1, 0.0, shift_up(tile.ups[f]))
                    + jnp.where(row == 0, 0.0, shift_down(tile.downs[f]))
                )

        walk(load, range(NT), NT, visit)

    def outer_rate(stage, f, cols):
        return jnp.where(
            row == RL - 1, edst[stage, 0, f, :, cols], jnp.where(row == 0, edst[stage, 1, f, :, cols], 0.0)
        )

    def relay(c, side):
        return pltpu.make_async_remote_copy(
            src_ref=rsrc.at[:, :, chunk(c)], dst_ref=rdst.at[side, :, :, chunk(c)],
            send_sem=rel_s.at[side], recv_sem=rel_r.at[side, c],
            device_id=(p, row_neighbour(side)), device_id_type=MESH,
        )

    def relay_chunks(chunks):
        @pl.when(late)
        def _():
            for c in chunks:
                shift(c, w).wait_recv()
                for f in range(3):
                    rsrc[f, :, chunk(c)] = outer_rows(w[f, :, chunk(c)])
                for side in range(sides):
                    relay(c, side).start()

    def first_g(rows, cols, f):
        return (
            (-7.0 / 24.0) * u_ref[0, f, rows, cols] + (1.0 / 3.0) * u_ref[1, f, rows, cols]
            - (1.0 / 24.0) * u_ref[2, f, rows, cols] + 0.5 * s0[f, rows, cols]
        )

    every = slice(0, RL)
    for part in range(SPANS):
        for j in range(part * SPAN // LANES, (part + 1) * SPAN // LANES):
            put_edges(0, lanes_of(j), *([first_g(slice(r, r + 1), lanes_of(j), f) for f in range(3)] for r in (0, RL - 1)))
        send_edges(0, part)
    inner_rate(
        lambda j: ([first_g(every, lanes_of(j), f) for f in range(3)], depth_ref[:, lanes_of(j)]), s1
    )

    def dep_copy(yo):
        return pltpu.make_async_remote_copy(
            src_ref=dsrc.at[yo], dst_ref=dep.at[pl.ds(pl.multiple_of(y * RL, 8), RL)],
            send_sem=dep_s.at[yo], recv_sem=dep_r, device_id=(p, yo), device_id_type=MESH,
        )

    def ini_copy(yo):
        return pltpu.make_async_remote_copy(
            src_ref=isrc.at[yo], dst_ref=ini.at[:, pl.ds(pl.multiple_of(y * RL, 8), RL)],
            send_sem=ini_s.at[yo], recv_sem=ini_r, device_id=(p, yo), device_id_type=MESH,
        )

    def owner_tables():
        for yo in range(SP):
            flat = pb * SP + yo
            k = tile_of(flat // stride)
            at_k = pl.ds(pl.multiple_of(k * W, LANES), W)
            at_after = pl.ds(pl.multiple_of(lax.rem((k + 1) * W, NX), LANES), LANES)
            at_before = pl.ds(pl.multiple_of(lax.rem(k * W + NX - LANES, NX), LANES), LANES)

            @pl.when(lax.rem(flat, stride) == 0)
            def _():
                dsrc[yo, :, :W] = depth_ref[:, at_k]
                dsrc[yo, :, W:] = jnp.where(lane_h < LANES // 2, depth_ref[:, at_after], depth_ref[:, at_before])

                @pl.when(yo != y)
                def _():
                    dep_copy(yo).start()

                @pl.when(yo == y)
                def _():
                    pltpu.make_async_copy(
                        dsrc.at[yo], dep.at[pl.ds(pl.multiple_of(y * RL, 8), RL)], dep_r
                    ).start()

            @pl.when(jnp.logical_and(lax.rem(flat, stride) == 0, block == 0))
            def _():
                for f in range(3):
                    isrc[yo, f, :, :W] = init_ref[f, :, at_k]
                    isrc[yo, f, :, W:] = jnp.where(
                        lane_h < LANES // 2, init_ref[f, :, at_after], init_ref[f, :, at_before]
                    )

                @pl.when(yo != y)
                def _():
                    ini_copy(yo).start()

                @pl.when(yo == y)
                def _():
                    pltpu.make_async_copy(
                        isrc.at[yo], ini.at[:, pl.ds(pl.multiple_of(y * RL, 8), RL)], ini_r
                    ).start()

    owner_tables()
    for part in range(SPANS):
        wait_edges(0, part)
        for j in range(part * SPAN // LANES, (part + 1) * SPAN // LANES):
            cols = lanes_of(j)
            new = []
            for f in range(3):
                one = s0[f, :, cols] + s1[f, :, cols] + outer_rate(0, f, cols)
                s1[f, :, cols] = one
                new.append(
                    0.5 * one - (1.0 / 24.0) * u_ref[0, f, :, cols] - (1.0 / 6.0) * u_ref[1, f, :, cols]
                    + (5.0 / 24.0) * u_ref[2, f, :, cols]
                )
                g[f, :, cols] = new[f]
            put_edges(1, cols, [v[0:1] for v in new], [v[RL - 1 : RL] for v in new])

        @pl.when(jnp.logical_not(late))
        def _():
            send_edges(1, part)

    inner_rate(lambda j: ([g[f, :, lanes_of(j)] for f in range(3)], depth_ref[:, lanes_of(j)]), b)

    relay_chunks(range(HOLD * NC // 8))

    @pl.when(late)
    def _():
        for part in range(SPANS):
            send_edges(1, part)

    relay_chunks(range(HOLD * NC // 8, NC))

    my_rows = pl.ds(pl.multiple_of(y * RL, 8), RL)

    def a2a(i, k):
        j = owner_of(k)
        if i == 0:
            src, dst = b.at[:, :, pl.ds(pl.multiple_of(k * W, LANES), W)], main.at[pb, :, my_rows]
        else:
            src, dst = halo_src.at[:, :, pl.ds(pl.multiple_of(k * LANES, LANES), LANES)], halo.at[pb, :, my_rows]

        @pl.when(j * stride != local)
        def _():
            pltpu.make_async_remote_copy(
                src_ref=src, dst_ref=dst, send_sem=a2a_s.at[i], recv_sem=a2a_r.at[i, pb],
                device_id=where(block * TG * SP + j * stride), device_id_type=MESH,
            ).start()

        @pl.when(j * stride == local)
        def _():
            pltpu.make_async_copy(src, dst, a2a_r.at[i, pb]).start()

    for part in range(SPANS):
        wait_edges(1, part)
        for j in range(part * SPAN // LANES, (part + 1) * SPAN // LANES):
            cols = lanes_of(j)
            for f in range(3):
                start, one = s0[f, :, cols], s1[f, :, cols]
                two = one + b[f, :, cols] + outer_rate(1, f, cols)
                b[f, :, cols] = (1.0 / 6.0) * two + (2.0 / 3.0) * one - (5.0 / 6.0) * start
                mid[f, :, cols] = one - 0.5 * (start + two)

    slot_of = lax.rem(lane_h + hw, LANES) // (2 * hw)

    def send_halo(k):
        lo, hi = ((k + 1) % K) * W, (k * W - LANES) % NX
        packed = [jnp.zeros((RL, LANES), jnp.float32) for _ in range(nh)]
        for f in range(3):
            z = jnp.where(lane_h < LANES // 2, b[f, :, lo : lo + LANES], b[f, :, hi : hi + LANES])
            slot = f % per
            if slot:
                z = pltpu.roll(z, 2 * hw * slot, 1)
            packed[f // per] = jnp.where(slot_of == slot, z, packed[f // per])
        for i in range(nh):
            halo_src[i, :, k * LANES : (k + 1) * LANES] = packed[i]

    def send_halos(ks):
        for k in ks:
            send_halo(k)
        for k in ks:
            a2a(1, k)

    def extended(own, tile):
        return jnp.concatenate([own, tile], axis=0)

    def late_chunk(c):
        tiles = [outer_tile([window(rdst.at[side, f], c) for side in range(sides)]) for f in range(3)]
        depth_tile = outer_tile([window(dhdst.at[side], c) for side in range(sides)])
        depth = extended(window(depth_ref, c), depth_tile)
        start = [extended(window(w.at[f], c), tiles[f]) for f in range(3)]
        once = periodic_rate(start, depth)
        twice = periodic_rate(once, depth)
        for f in range(3):
            one, two = once[f][:RL, :WC], twice[f][:RL, :WC]
            b[f, :, chunk(c)] = b[f, :, chunk(c)] + (0.5 * one + (1.0 / 24.0) * two)
            mid[f, :, chunk(c)] = mid[f, :, chunk(c)] - 0.125 * two

        @pl.loop(0, tpc)
        def _(i):
            a2a(0, c * tpc + lax.rem(mine + i, tpc))

    @pl.when(late)
    def _():
        for side in range(sides):
            depth_halo(side).wait_recv()
        arrived, known, sent = 0, set(), set()
        for step in range(1, NC + 1):
            c = step % NC
            while arrived < min(step + 2, NC):
                for side in range(sides):
                    relay(arrived, side).wait_recv()
                arrived += 1
            late_chunk(c)
            known.update(range(c * tpc, (c + 1) * tpc))
            ready = [k for k in range(K) if k not in sent and {(k - 1) % K, k, (k + 1) % K} <= known]
            sent.update(ready)
            send_halos(ready)

    @pl.when(jnp.logical_not(late))
    def _():
        @pl.loop(0, K)
        def _(i):
            c = i // tpc
            c = lax.rem(c * 2, NC) + lax.rem(y + c * 2 // NC, 2) if NC > 1 else c
            a2a(0, c * tpc + lax.rem(mine + i, tpc))

        send_halos(range(K))

    NS = W // LANES

    def my_lanes(i):
        return pl.ds(pl.multiple_of(mine * W + i * LANES, LANES), LANES)

    def hand(src, dst, send, recv, t, yo):
        here = jnp.logical_and(t == pb, y == yo)

        @pl.when(jnp.logical_not(here))
        def _():
            pltpu.make_async_remote_copy(
                src_ref=src, dst_ref=dst, send_sem=send, recv_sem=recv,
                device_id=(block * TG + t, yo), device_id_type=MESH,
            ).start()

        @pl.when(here)
        def _():
            pltpu.make_async_copy(src, dst, recv).start()

    def give_begin(i, t, src):
        for yo in range(SP):
            hand(src.at[yo], cb.at[:, :, my_lanes(i)], beg_s, beg_r, t, yo)

    def give(i, t):
        for yo in range(SP):
            hand(eo.at[i, t * SP + yo], redge.at[:, :, :, my_lanes(i)], ret_s, ret_r, t, yo)

        @pl.when(jnp.logical_and(lax.rem(t, 2) == 1, t < TG - 1))
        def _():
            give_begin(i, t + 1, cs.at[i, pl.ds(t * SP, SP)])

    def carry(i):
        ends = ((cs.at[i, pl.ds((TG - 1) * SP, SP)], cin.at[i]), (chalo_src.at[i], chalo.at[i]))
        return [
            pltpu.make_async_remote_copy(
                src_ref=src, dst_ref=dst, send_sem=c_s.at[i, e], recv_sem=c_r.at[i, e],
                device_id=(lax.rem(p + TG, T), y), device_id_type=MESH,
            )
            for e, (src, dst) in enumerate(ends)
        ]

    def unpack(tile, f):
        return pltpu.roll(tile, LANES - 2 * hw * (f % per), 1) if f % per else tile

    R = SP * RL

    @pl.when(is_owner)
    def _():
        whole(dep, dep_r)

        tall = lax.broadcasted_iota(jnp.int32, (R, LANES), 1)
        half = lax.broadcasted_iota(jnp.int32, (R // 2, LANES), 1)
        slots = lax.rem(half + carry_hw, LANES) // (2 * carry_hw)

        def beside(block_of, outer, i):
            if NS == 1:
                return outer()
            after = block_of(i + 1) if i < NS - 1 else outer()
            before = block_of(i - 1) if i > 0 else outer()
            return jnp.where(tall < LANES // 2, after, before)

        def turn(i, t, carried):
            if i == 0:
                whole(main.at[t], a2a_r.at[0, t])
                whole(halo.at[t], a2a_r.at[1, t])
            cur = [[state[i, f, :, lanes_of(j)] for f in range(3)] for j in range(2)]
            depths = [dep[:, lanes_of(i)], beside(lambda m: dep[:, lanes_of(m)], lambda: dep[:, W:], i)]

            def load(j):
                if j == 0:
                    sent = [main[t, f, :, lanes_of(i)] for f in range(3)]
                else:
                    sent = [
                        beside(lambda m: main[t, f, :, lanes_of(m)], lambda: unpack(halo[t, f // per], f), i)
                        for f in range(3)
                    ]
                return [cur[j][f] + sent[f] for f in range(3)], depths[j]

            def visit(j, before, tile, after):
                for f in range(3):
                    value = cur[j][f] + (
                        column_sum(before, tile, after, f, tall) + shift_up(tile.ups[f]) + shift_down(tile.downs[f])
                    )
                    state[i, f, :, lanes_of(j)] = value
                    if j == 0:
                        for yo in range(SP):
                            cs[i, t * SP + yo, f] = value[yo * RL : (yo + 1) * RL]
                            below, above = (yo + 1) * RL % R, (yo * RL - 1) % R
                            eo[i, t * SP + yo, 0, f] = tile.ups[f][below : below + 1]
                            eo[i, t * SP + yo, 1, f] = tile.downs[f][above : above + 1]

            walk(load, range(2), 2, visit)

            @pl.when(jnp.logical_and(t > 0, block == NG - 1))
            def _():
                give(i, t - 1)

            return carried

        @pl.when(block == 0)
        def _():
            whole(ini, ini_r)
            for i in range(NS):
                for f in range(3):
                    state[i, f, :, :LANES] = ini[f, :, lanes_of(i)]
                    state[i, f, :, LANES:] = beside(lambda m: ini[f, :, lanes_of(m)], lambda: ini[f, :, W:], i)

        for i in range(NS):
            @pl.when(block > 0)
            def _():
                for copy in carry(i):
                    copy.wait_recv()
                give_begin(i, 0, cin.at[i])
                for f in range(3):
                    for yo in range(SP):
                        state[i, f, yo * RL : (yo + 1) * RL, :LANES] = cin[i, yo, f]
                    for r in range(2):
                        slot = 2 * f + r
                        tile = chalo[i, slot // carry_slots]
                        if slot % carry_slots:
                            tile = pltpu.roll(tile, LANES - 2 * carry_hw * (slot % carry_slots), 1)
                        state[i, f, r * R // 2 : (r + 1) * R // 2, LANES:] = tile

            lax.fori_loop(0, TG, functools.partial(turn, i), 0)

            @pl.when(block == NG - 1)
            def _():
                give(i, TG - 1)

            @pl.when(block < NG - 1)
            def _():
                for e in range(chalo.shape[1]):
                    packed = jnp.zeros((R // 2, LANES), jnp.float32)
                    for slot in range(e * carry_slots, min(6, (e + 1) * carry_slots)):
                        f, r = slot // 2, slot % 2
                        z = state[i, f, r * R // 2 : (r + 1) * R // 2, LANES:]
                        if slot % carry_slots:
                            z = pltpu.roll(z, 2 * carry_hw * (slot % carry_slots), 1)
                        packed = jnp.where(slots == slot % carry_slots, z, packed)
                    chalo_src[i, e] = packed
                if i == 0:
                    pl.semaphore_wait(go_carry, 1)
                for copy in carry(i):
                    copy.start()

        @pl.when(block < NG - 1)
        def _():
            @pl.loop(0, TG)
            def _(t):
                for i in range(NS):
                    give(i, t)

    part = NX // PARTS

    def fwd(q):
        cols = pl.ds(q * part, part)
        return pltpu.make_async_remote_copy(
            src_ref=ce.at[:, :, cols], dst_ref=cb.at[:, :, cols],
            send_sem=fwd_s, recv_sem=fwd_r.at[q], device_id=(lax.rem(p + 1, T), y), device_id_type=MESH,
        )

    whole(redge, ret_r)

    @pl.when(p == 0)
    def _():
        cb[...] = init_ref[...]

    @pl.when(late)
    def _():
        whole(cb, beg_r)

    per_part = NT // PARTS

    def advance(q, made, visit_ends):
        def load(j):
            return [cb[f, :, lanes_of(j)] + b[f, :, lanes_of(j)] for f in range(3)], depth_ref[:, lanes_of(j)]

        def visit(j, before, tile, after):
            cols = lanes_of(j)
            visit_ends(cols, [
                cb[f, :, cols] + column_sum(before, tile, after, f, lane)
                + jnp.where(row == RL - 1, redge[0, f, :, cols], shift_up(tile.ups[f]))
                + jnp.where(row == 0, redge[1, f, :, cols], shift_down(tile.downs[f]))
                for f in range(3)
            ])

        walk(load, range(q * per_part, (q + 1) * per_part), NT, visit, made)

    def keep(cols, ends):
        for f in range(3):
            ce[f, :, cols] = ends[f]

    def emit(cols, ends):
        for f in range(3):
            start = cb[f, :, cols]
            out_ref[0, 0, f, :, cols] = start
            out_ref[0, 1, f, :, cols] = mid[f, :, cols] + 0.5 * (start + ends[f])
            out_ref[0, 2, f, :, cols] = ends[f]

    order = [PARTS - 1, *range(PARTS - 1)]

    @pl.when(even)
    def _():
        made = {}
        for q in order:
            advance(q, made, keep)
            fwd(q).start()
        for j in range(NT):
            emit(lanes_of(j), [ce[f, :, lanes_of(j)] for f in range(3)])
        whole(ce, fwd_s)

    @pl.when(odd)
    def _():
        made, arrived = {}, 0
        for q in range(PARTS):
            while arrived < min(q + 3, PARTS):
                fwd(order[arrived]).wait_recv()
                arrived += 1
            advance(q, made, emit)

    @pl.when(p < T - 1)
    def _():
        whole(u_ref.at[2], shift_s)

    @pl.when(late)
    def _():
        for side in range(sides):
            depth_halo(side).wait_send()
            whole(rsrc, rel_s.at[side])

    whole(esrc, edge_s)
    for yo in range(SP):
        flat = pb * SP + yo

        @pl.when(jnp.logical_and(lax.rem(flat, stride) == 0, yo != y))
        def _():
            dep_copy(yo).wait_send()

            @pl.when(block == 0)
            def _():
                ini_copy(yo).wait_send()

    @pl.when(is_owner)
    def _():
        whole(b.at[:, :, pl.ds(0, (K - 1) * W)], a2a_s.at[0])
        whole(halo_src.at[:, :, pl.ds(0, (K - 1) * LANES)], a2a_s.at[1])
        for i in range(NS):
            whole(eo.at[i, pl.ds(0, TG * SP - 1)], ret_s)

        @pl.when(block < NG - 1)
        def _():
            for i in range(NS):
                for copy in carry(i):
                    copy.wait_send()

        own = jnp.logical_and(even, p > 0).astype(jnp.int32)
        begins = (TG + 1) // 2 * SP - own - jnp.where(block == 0, SP, 0)
        for n in ((TG + 1) // 2 * SP - a - c for a in range(2) for c in (0, SP)):
            @pl.when(begins == n)
            def _():
                for i in range(NS):
                    whole(cs.at[i, pl.ds(0, n)], beg_s)

    @pl.when(jnp.logical_not(is_owner))
    def _():
        whole(b, a2a_s.at[0])
        whole(halo_src, a2a_s.at[1])


def solution(mesh):
    T, SP = mesh.shape["tm"], mesh.shape["space"]

    def per_device(fine_nodes, init_state, mean_depth):
        RL, NX = mean_depth.shape
        NG = 2 if T % 4 == 0 else 1
        members = T // NG * SP
        W = max(LANES, NX // members)
        K = NX // W
        NC = CHUNKS if K % CHUNKS == 0 else 1
        stride = members // K
        hw = 8
        while hw < T:
            hw *= 2
        per = LANES // (2 * hw)
        nh = -(-3 // per)
        carry_hw = 8
        while carry_hw < T // NG:
            carry_hw *= 2
        carried = -(-6 * 2 * carry_hw // LANES)
        cfg = (T, SP, RL, NX, W, K, stride, hw, per, nh, NG, NC, carry_hw)
        f32, dma = jnp.float32, pltpu.SemaphoreType.DMA
        state = pltpu.VMEM((3, RL, NX), f32)
        R = RL * SP
        sides = 1 if SP == 2 else 2
        edges = pltpu.VMEM((2, 2, 3, 1, NX), f32)
        vmem = pl.BlockSpec(memory_space=pltpu.VMEM)
        return pl.pallas_call(
            functools.partial(kernel, cfg),
            out_shape=pltpu.VMEM(fine_nodes.shape, f32),
            in_specs=[pl.BlockSpec(memory_space=pl.ANY)] * 3,
            out_specs=vmem,
            scratch_shapes=[
                pltpu.VMEM((3, 3, RL, NX), f32), state, pltpu.VMEM((RL, NX), f32),
                state, state, state, state, state, state,
                pltpu.VMEM((nh, RL, K * LANES), f32),
                pltpu.VMEM((3, 2 * DEEP, NX), f32),
                pltpu.VMEM((sides, 3, 2 * DEEP, NX), f32),
                pltpu.VMEM((2 * DEEP, NX), f32),
                pltpu.VMEM((sides, 2 * DEEP, NX), f32),
                pltpu.VMEM((SP, RL, W + LANES), f32),
                pltpu.VMEM((R, W + LANES), f32),
                pltpu.VMEM((SP, 3, RL, W + LANES), f32),
                pltpu.VMEM((3, R, W + LANES), f32),
                pltpu.VMEM((T // NG, 3, R, W), f32),
                pltpu.VMEM((T // NG, nh, R, LANES), f32),
                pltpu.VMEM((W // LANES, members, 3, RL, LANES), f32),
                state, state,
                edges, edges,
                pltpu.VMEM((W // LANES, members, 2, 3, 1, LANES), f32),
                pltpu.VMEM((2, 3, 1, NX), f32),
                pltpu.VMEM((W // LANES, SP, 3, RL, LANES), f32),
                pltpu.VMEM((W // LANES, carried, R // 2, LANES), f32),
                pltpu.VMEM((W // LANES, carried, R // 2, LANES), f32),
                pltpu.VMEM((W // LANES, 3, R, 2 * LANES), f32),
                dma, dma((NC,)), dma((sides,)), dma((sides, NC)), dma((sides,)), dma((sides,)),
                dma, dma((2, SPANS)), dma((SP,)), dma, dma((SP,)), dma, dma((2,)), dma((2, T // NG)),
                dma, dma, dma, dma((PARTS,)),
                dma((W // LANES, 2)), dma((W // LANES, 2)), dma, dma, dma((5,)),
                pltpu.SemaphoreType.REGULAR,
            ],
            compiler_params=pltpu.CompilerParams(
                collective_id=0, has_side_effects=True, vmem_limit_bytes=60 * 1024 * 1024
            ),
        )(fine_nodes, init_state, mean_depth)

    return jax.shard_map(
        per_device,
        mesh=mesh,
        in_specs=(P("tm", None, None, "space", None), P(None, "space", None), P("space", None)),
        out_specs=P("tm", None, None, "space", None),
        check_vma=False,
    )
```

```python
import functools

import jax
import jax.numpy as jnp
from jax import lax
from jax.experimental import pallas as pl
from jax.experimental.pallas import tpu as pltpu
from jax.sharding import PartitionSpec as P

MESH = pl.DeviceIdType.MESH
DT = 0.3
NU = 1.0 / 3.0
FC = 0.5
DIFF = DT * NU
HALF = DT * 0.5
TURN = DT * FC
LANES = 128
SUB = 8
DEEP = 2
CHUNKS = 4
SPREAD = 4
PARTS = 8
SPANS = 2
HOLD = 4


def shift_left(v):
    return pltpu.roll(v, v.shape[1] - 1, 1)


def shift_right(v):
    return pltpu.roll(v, 1, 1)


def shift_up(v):
    return pltpu.roll(v, v.shape[0] - 1, 0)


def shift_down(v):
    return pltpu.roll(v, 1, 0)


def row_terms(h, e, n, depth):
    dn = depth * n
    nh, ne, nn, hh = DIFF * h, DIFF * e, DIFF * n, HALF * h
    return (nh - dn, ne, nn - hh), (nh + dn, ne, nn + hh)


def column_terms(h, e, n, depth):
    de = depth * e
    nh, ne, nn, hh = DIFF * h, DIFF * e, DIFF * n, HALF * h
    return (
        shift_left(nh - de) + shift_right(nh + de) - 4.0 * nh,
        shift_left(ne - hh) + shift_right(ne + hh) - 4.0 * ne + TURN * n,
        shift_left(nn) + shift_right(nn) - 4.0 * nn - TURN * e,
    )


def periodic_rate(state, depth):
    rates = column_terms(*state, depth)
    ups, downs = row_terms(*state, depth)
    return [rates[f] + shift_up(ups[f]) + shift_down(downs[f]) for f in range(3)]


class Tile:
    def __init__(self, state, depth):
        h, e, n = state
        de, dn = depth * e, depth * n
        nh, ne, nn, hh = DIFF * h, DIFF * e, DIFF * n, HALF * h
        self.lefts = [shift_left(x) for x in (nh - de, ne - hh, nn)]
        self.rights = [shift_right(x) for x in (nh + de, ne + hh, nn)]
        self.ups, self.downs = (nh - dn, ne, nn - hh), (nh + dn, ne, nn + hh)
        self.own = (-4.0 * nh, TURN * n - 4.0 * ne, -4.0 * nn - TURN * e)


def column_sum(before, tile, after, f, lane):
    return (
        tile.own[f]
        + jnp.where(lane == LANES - 1, after.lefts[f], tile.lefts[f])
        + jnp.where(lane == 0, before.rights[f], tile.rights[f])
    )


def walk(load, tiles, count, visit, made=None):
    made = {} if made is None else made

    def tile(i):
        i %= count
        if i not in made:
            made[i] = Tile(*load(i))
        return made[i]

    for j in tiles:
        visit(j, tile(j - 1), tile(j), tile(j + 1))
        if count > 4:
            made.pop((j - 1) % count)


def kernel(
    cfg, u_hbm, init_hbm, depth_hbm, out_ref, u_ref, init_ref, depth_ref,
    w, s0, g, s1, mid, b, halo_src, rsrc, rdst, dhsrc, dhdst, dsrc, dep, isrc, ini, main, halo, cs, ce, cb,
    esrc, edst, eo, redge, cin, chalo, chalo_src, state,
    shift_s, shift_r, rel_s, rel_r, dh_s, dh_r, edge_s, edge_r, dep_s, dep_r, ini_s, ini_r, a2a_s, a2a_r, ret_s, ret_r,
    fwd_s, fwd_r, c_s, c_r, beg_s, beg_r, in_s, go_carry,
):
    T, SP, RL, NX, W, K, stride, hw, per, nh, NG, NC, carry_hw = cfg
    carry_slots = LANES // (2 * carry_hw)
    TG = T // NG
    WC = NX // NC
    tpc = K // NC
    sides = 1 if SP == 2 else 2
    p, y = lax.axis_index("tm"), lax.axis_index("space")
    block = p // TG
    pb = p - block * TG
    local = pb * SP + y
    is_owner = lax.rem(local, stride) == 0
    even = lax.rem(p, 2) == 0
    odd = jnp.logical_not(even)
    late = jnp.logical_and(even, p > 0)

    spread = SPREAD if NC % SPREAD == 0 else 1

    def tile_of(j):
        high, low = j // (tpc * spread), lax.rem(j, spread)
        return (high * spread + low) * tpc + lax.rem(j // spread, tpc)

    def owner_of(k):
        c = k // tpc
        return c // spread * (tpc * spread) + lax.rem(k, tpc) * spread + lax.rem(c, spread)

    mine = tile_of(local // stride)

    def where(flat):
        return (flat // SP, lax.rem(flat, SP))

    def row_neighbour(side):
        return lax.rem(y + SP - 1, SP) if side == 0 else lax.rem(y + 1, SP)

    barrier = pltpu.get_barrier_semaphore()

    members = TG * SP
    has_next, has_last = block < NG - 1, block > 0
    crosses = jnp.logical_and(has_next, pb == TG - 1)

    first_of_block = jnp.logical_and(has_last, pb == 0)
    meets = jnp.logical_or(crosses, first_of_block)

    def announce(sem, pp):
        pl.semaphore_signal(sem, inc=1, device_id=(pp, y), device_id_type=MESH)

    @pl.when(first_of_block)
    def _():
        announce(barrier, lax.rem(p + T - 1, T))

    @pl.loop(1, members)
    def _(i):
        pl.semaphore_signal(
            barrier, inc=1, device_id=where(block * members + lax.rem(local + i, members)), device_id_type=MESH
        )

    @pl.when(has_next)
    def _():
        announce(barrier, lax.rem(p + TG, T))

    @pl.when(crosses)
    def _():
        announce(barrier, lax.rem(p + 1, T))

    loads = [pltpu.make_async_copy(u_hbm.at[0, i], u_ref.at[i], in_s.at[i]) for i in (2, 0, 1)]
    loads.append(pltpu.make_async_copy(depth_hbm, depth_ref, in_s.at[3]))
    loads.append(pltpu.make_async_copy(init_hbm, init_ref, in_s.at[4]))
    for copy in loads:
        copy.start()
    loads[0].wait()
    pl.semaphore_wait(barrier, members - 1 + has_last.astype(jnp.int32) + meets.astype(jnp.int32))

    @pl.when(has_last)
    def _():
        announce(go_carry, lax.rem(p + T - TG, T))

    def whole(ref, sem):
        pltpu.make_async_copy(ref, ref, sem).wait()

    def chunk(c):
        return pl.ds(c * WC, WC)

    def shift(c, dst):
        return pltpu.make_async_remote_copy(
            src_ref=u_ref.at[2, :, :, chunk(c)], dst_ref=dst.at[:, :, chunk(c)],
            send_sem=shift_s, recv_sem=shift_r.at[c],
            device_id=(lax.rem(p + 1, T), y), device_id_type=MESH,
        )

    @pl.when(jnp.logical_and(odd, p < T - 1))
    def _():
        for c in range(NC):
            shift(c, w).start()

    @pl.when(even)
    def _():
        for c in range(NC):
            shift(c, s0).start()

    for copy in loads[1:]:
        copy.wait()

    depth_ref[...] = HALF * depth_ref[...]

    lane_h = lax.broadcasted_iota(jnp.int32, (RL, LANES), 1)

    def outer_rows(own):
        sub = lax.broadcasted_iota(jnp.int32, (SUB, own.shape[1]), 0)
        return jnp.where(sub < DEEP, own[:SUB], pltpu.roll(own[RL - SUB :], SUB - 2 * DEEP, 0))[: 2 * DEEP]

    def outer_tile(parts):
        if sides == 1:
            both = parts[0]
        else:
            sub = lax.broadcasted_iota(jnp.int32, parts[0].shape, 0)
            both = jnp.where(sub < DEEP, parts[0], parts[1])
        return jnp.concatenate([both] * (SUB // (2 * DEEP)), axis=0)


    def margin(ref, c, size):
        after = ref[:, pl.ds((c + 1) * size % NX, LANES)]
        before = ref[:, pl.ds((c * size - LANES) % NX, LANES)]
        lanes = lax.broadcasted_iota(jnp.int32, after.shape, 1)
        return jnp.where(lanes < LANES // 2, after, before)

    def window(ref, c, size=WC):
        return jnp.concatenate([ref[:, pl.ds(c * size, size)], margin(ref, c, size)], axis=1)

    def depth_halo(side):
        return pltpu.make_async_remote_copy(
            src_ref=dhsrc, dst_ref=dhdst.at[side], send_sem=dh_s.at[side], recv_sem=dh_r.at[side],
            device_id=(p, row_neighbour(side)), device_id_type=MESH,
        )

    @pl.when(late)
    def _():
        dhsrc[...] = outer_rows(depth_ref[...])
        for side in range(sides):
            depth_halo(side).start()
        s0[...] = jnp.zeros_like(s0)

    @pl.when(p == 0)
    def _():
        s0[...] = init_ref[...]

    @pl.when(odd)
    def _():
        for c in range(NC):
            shift(c, s0).wait_recv()

    row = lax.broadcasted_iota(jnp.int32, (RL, LANES), 0)
    lane = lax.broadcasted_iota(jnp.int32, (RL, LANES), 1)
    NT = NX // LANES
    SPAN = NX // SPANS

    def lanes_of(j):
        return slice(j * LANES, (j + 1) * LANES)

    def edge_copy(stage, side, part):
        cols = pl.ds(part * SPAN, SPAN)
        return pltpu.make_async_remote_copy(
            src_ref=esrc.at[stage, side, :, :, cols], dst_ref=edst.at[stage, side, :, :, cols],
            send_sem=edge_s, recv_sem=edge_r.at[stage, part],
            device_id=(p, row_neighbour(side)), device_id_type=MESH,
        )

    def put_edges(stage, cols, top, bottom):
        ups, _ = row_terms(*top, depth_ref[0:1, cols])
        _, downs = row_terms(*bottom, depth_ref[RL - 1 : RL, cols])
        for f in range(3):
            esrc[stage, 0, f, :, cols] = ups[f]
            esrc[stage, 1, f, :, cols] = downs[f]

    def send_edges(stage, part):
        for side in range(2):
            edge_copy(stage, side, part).start()

    def wait_edges(stage, part):
        whole(edst.at[stage, :, :, :, pl.ds(part * SPAN, SPAN)], edge_r.at[stage, part])

    def inner_rate(load, out):
        def visit(j, before, tile, after):
            for f in range(3):
                out[f, :, lanes_of(j)] = (
                    column_sum(before, tile, after, f, lane)
                    + jnp.where(row == RL - 1, 0.0, shift_up(tile.ups[f]))
                    + jnp.where(row == 0, 0.0, shift_down(tile.downs[f]))
                )

        walk(load, range(NT), NT, visit)

    def outer_rate(stage, f, cols):
        return jnp.where(
            row == RL - 1, edst[stage, 0, f, :, cols], jnp.where(row == 0, edst[stage, 1, f, :, cols], 0.0)
        )

    def relay(c, side):
        return pltpu.make_async_remote_copy(
            src_ref=rsrc.at[:, :, chunk(c)], dst_ref=rdst.at[side, :, :, chunk(c)],
            send_sem=rel_s.at[side], recv_sem=rel_r.at[side, c],
            device_id=(p, row_neighbour(side)), device_id_type=MESH,
        )

    def relay_chunks(chunks):
        @pl.when(late)
        def _():
            for c in chunks:
                shift(c, w).wait_recv()
                for f in range(3):
                    rsrc[f, :, chunk(c)] = outer_rows(w[f, :, chunk(c)])
                for side in range(sides):
                    relay(c, side).start()

    def first_g(rows, cols, f):
        return (
            (-7.0 / 24.0) * u_ref[0, f, rows, cols] + (1.0 / 3.0) * u_ref[1, f, rows, cols]
            - (1.0 / 24.0) * u_ref[2, f, rows, cols] + 0.5 * s0[f, rows, cols]
        )

    every = slice(0, RL)
    for part in range(SPANS):
        for j in range(part * SPAN // LANES, (part + 1) * SPAN // LANES):
            put_edges(0, lanes_of(j), *([first_g(slice(r, r + 1), lanes_of(j), f) for f in range(3)] for r in (0, RL - 1)))
        send_edges(0, part)
    inner_rate(
        lambda j: ([first_g(every, lanes_of(j), f) for f in range(3)], depth_ref[:, lanes_of(j)]), s1
    )

    def dep_copy(yo):
        return pltpu.make_async_remote_copy(
            src_ref=dsrc.at[yo], dst_ref=dep.at[pl.ds(pl.multiple_of(y * RL, 8), RL)],
            send_sem=dep_s.at[yo], recv_sem=dep_r, device_id=(p, yo), device_id_type=MESH,
        )

    def ini_copy(yo):
        return pltpu.make_async_remote_copy(
            src_ref=isrc.at[yo], dst_ref=ini.at[:, pl.ds(pl.multiple_of(y * RL, 8), RL)],
            send_sem=ini_s.at[yo], recv_sem=ini_r, device_id=(p, yo), device_id_type=MESH,
        )

    def owner_tables():
        for yo in range(SP):
            flat = pb * SP + yo
            k = tile_of(flat // stride)
            at_k = pl.ds(pl.multiple_of(k * W, LANES), W)
            at_after = pl.ds(pl.multiple_of(lax.rem((k + 1) * W, NX), LANES), LANES)
            at_before = pl.ds(pl.multiple_of(lax.rem(k * W + NX - LANES, NX), LANES), LANES)

            @pl.when(lax.rem(flat, stride) == 0)
            def _():
                dsrc[yo, :, :W] = depth_ref[:, at_k]
                dsrc[yo, :, W:] = jnp.where(lane_h < LANES // 2, depth_ref[:, at_after], depth_ref[:, at_before])

                @pl.when(yo != y)
                def _():
                    dep_copy(yo).start()

                @pl.when(yo == y)
                def _():
                    pltpu.make_async_copy(
                        dsrc.at[yo], dep.at[pl.ds(pl.multiple_of(y * RL, 8), RL)], dep_r
                    ).start()

            @pl.when(jnp.logical_and(lax.rem(flat, stride) == 0, block == 0))
            def _():
                for f in range(3):
                    isrc[yo, f, :, :W] = init_ref[f, :, at_k]
                    isrc[yo, f, :, W:] = jnp.where(
                        lane_h < LANES // 2, init_ref[f, :, at_after], init_ref[f, :, at_before]
                    )

                @pl.when(yo != y)
                def _():
                    ini_copy(yo).start()

                @pl.when(yo == y)
                def _():
                    pltpu.make_async_copy(
                        isrc.at[yo], ini.at[:, pl.ds(pl.multiple_of(y * RL, 8), RL)], ini_r
                    ).start()

    owner_tables()
    for part in range(SPANS):
        wait_edges(0, part)
        for j in range(part * SPAN // LANES, (part + 1) * SPAN // LANES):
            cols = lanes_of(j)
            new = []
            for f in range(3):
                one = s0[f, :, cols] + s1[f, :, cols] + outer_rate(0, f, cols)
                s1[f, :, cols] = one
                new.append(
                    0.5 * one - (1.0 / 24.0) * u_ref[0, f, :, cols] - (1.0 / 6.0) * u_ref[1, f, :, cols]
                    + (5.0 / 24.0) * u_ref[2, f, :, cols]
                )
                g[f, :, cols] = new[f]
            put_edges(1, cols, [v[0:1] for v in new], [v[RL - 1 : RL] for v in new])

        @pl.when(jnp.logical_not(late))
        def _():
            send_edges(1, part)

    inner_rate(lambda j: ([g[f, :, lanes_of(j)] for f in range(3)], depth_ref[:, lanes_of(j)]), b)

    relay_chunks(range(HOLD * NC // 8))

    @pl.when(late)
    def _():
        for part in range(SPANS):
            send_edges(1, part)

    relay_chunks(range(HOLD * NC // 8, NC))

    my_rows = pl.ds(pl.multiple_of(y * RL, 8), RL)

    def a2a(i, k):
        j = owner_of(k)
        if i == 0:
            src, dst = b.at[:, :, pl.ds(pl.multiple_of(k * W, LANES), W)], main.at[pb, :, my_rows]
        else:
            src, dst = halo_src.at[:, :, pl.ds(pl.multiple_of(k * LANES, LANES), LANES)], halo.at[pb, :, my_rows]

        @pl.when(j * stride != local)
        def _():
            pltpu.make_async_remote_copy(
                src_ref=src, dst_ref=dst, send_sem=a2a_s.at[i], recv_sem=a2a_r.at[i, pb],
                device_id=where(block * TG * SP + j * stride), device_id_type=MESH,
            ).start()

        @pl.when(j * stride == local)
        def _():
            pltpu.make_async_copy(src, dst, a2a_r.at[i, pb]).start()

    for part in range(SPANS):
        wait_edges(1, part)
        for j in range(part * SPAN // LANES, (part + 1) * SPAN // LANES):
            cols = lanes_of(j)
            for f in range(3):
                start, one = s0[f, :, cols], s1[f, :, cols]
                two = one + b[f, :, cols] + outer_rate(1, f, cols)
                b[f, :, cols] = (1.0 / 6.0) * two + (2.0 / 3.0) * one - (5.0 / 6.0) * start
                mid[f, :, cols] = one - 0.5 * (start + two)

    slot_of = lax.rem(lane_h + hw, LANES) // (2 * hw)

    def send_halo(k):
        lo, hi = ((k + 1) % K) * W, (k * W - LANES) % NX
        packed = [jnp.zeros((RL, LANES), jnp.float32) for _ in range(nh)]
        for f in range(3):
            z = jnp.where(lane_h < LANES // 2, b[f, :, lo : lo + LANES], b[f, :, hi : hi + LANES])
            slot = f % per
            if slot:
                z = pltpu.roll(z, 2 * hw * slot, 1)
            packed[f // per] = jnp.where(slot_of == slot, z, packed[f // per])
        for i in range(nh):
            halo_src[i, :, k * LANES : (k + 1) * LANES] = packed[i]

    def send_halos(ks):
        for k in ks:
            send_halo(k)
        for k in ks:
            a2a(1, k)

    def extended(own, tile):
        return jnp.concatenate([own, tile], axis=0)

    def late_chunk(c):
        tiles = [outer_tile([window(rdst.at[side, f], c) for side in range(sides)]) for f in range(3)]
        depth_tile = outer_tile([window(dhdst.at[side], c) for side in range(sides)])
        depth = extended(window(depth_ref, c), depth_tile)
        start = [extended(window(w.at[f], c), tiles[f]) for f in range(3)]
        once = periodic_rate(start, depth)
        twice = periodic_rate(once, depth)
        for f in range(3):
            one, two = once[f][:RL, :WC], twice[f][:RL, :WC]
            b[f, :, chunk(c)] = b[f, :, chunk(c)] + (0.5 * one + (1.0 / 24.0) * two)
            mid[f, :, chunk(c)] = mid[f, :, chunk(c)] - 0.125 * two

        @pl.loop(0, tpc)
        def _(i):
            a2a(0, c * tpc + lax.rem(mine + i, tpc))

    @pl.when(late)
    def _():
        for side in range(sides):
            depth_halo(side).wait_recv()
        arrived, known, sent = 0, set(), set()
        for step in range(1, NC + 1):
            c = step % NC
            while arrived < min(step + 2, NC):
                for side in range(sides):
                    relay(arrived, side).wait_recv()
                arrived += 1
            late_chunk(c)
            known.update(range(c * tpc, (c + 1) * tpc))
            ready = [k for k in range(K) if k not in sent and {(k - 1) % K, k, (k + 1) % K} <= known]
            sent.update(ready)
            send_halos(ready)

    @pl.when(jnp.logical_not(late))
    def _():
        @pl.loop(0, K)
        def _(i):
            c = i // tpc
            c = lax.rem(c * 2, NC) + lax.rem(y + c * 2 // NC, 2) if NC > 1 else c
            a2a(0, c * tpc + lax.rem(mine + i, tpc))

        send_halos(range(K))

    NS = W // LANES

    def my_lanes(i):
        return pl.ds(pl.multiple_of(mine * W + i * LANES, LANES), LANES)

    def hand(src, dst, send, recv, t, yo):
        here = jnp.logical_and(t == pb, y == yo)

        @pl.when(jnp.logical_not(here))
        def _():
            pltpu.make_async_remote_copy(
                src_ref=src, dst_ref=dst, send_sem=send, recv_sem=recv,
                device_id=(block * TG + t, yo), device_id_type=MESH,
            ).start()

        @pl.when(here)
        def _():
            pltpu.make_async_copy(src, dst, recv).start()

    def give_begin(i, t, src):
        for yo in range(SP):
            hand(src.at[yo], cb.at[:, :, my_lanes(i)], beg_s, beg_r, t, yo)

    def give(i, t):
        for yo in range(SP):
            hand(eo.at[i, t * SP + yo], redge.at[:, :, :, my_lanes(i)], ret_s, ret_r, t, yo)

        @pl.when(jnp.logical_and(lax.rem(t, 2) == 1, t < TG - 1))
        def _():
            give_begin(i, t + 1, cs.at[i, pl.ds(t * SP, SP)])

    def carry(i):
        ends = ((cs.at[i, pl.ds((TG - 1) * SP, SP)], cin.at[i]), (chalo_src.at[i], chalo.at[i]))
        return [
            pltpu.make_async_remote_copy(
                src_ref=src, dst_ref=dst, send_sem=c_s.at[i, e], recv_sem=c_r.at[i, e],
                device_id=(lax.rem(p + TG, T), y), device_id_type=MESH,
            )
            for e, (src, dst) in enumerate(ends)
        ]

    def unpack(tile, f):
        return pltpu.roll(tile, LANES - 2 * hw * (f % per), 1) if f % per else tile

    R = SP * RL

    @pl.when(is_owner)
    def _():
        whole(dep, dep_r)

        tall = lax.broadcasted_iota(jnp.int32, (R, LANES), 1)
        half = lax.broadcasted_iota(jnp.int32, (R // 2, LANES), 1)
        slots = lax.rem(half + carry_hw, LANES) // (2 * carry_hw)

        def beside(block_of, outer, i):
            if NS == 1:
                return outer()
            after = block_of(i + 1) if i < NS - 1 else outer()
            before = block_of(i - 1) if i > 0 else outer()
            return jnp.where(tall < LANES // 2, after, before)

        def turn(i, t, carried):
            if i == 0:
                whole(main.at[t], a2a_r.at[0, t])
                whole(halo.at[t], a2a_r.at[1, t])
            cur = [[state[i, f, :, lanes_of(j)] for f in range(3)] for j in range(2)]
            depths = [dep[:, lanes_of(i)], beside(lambda m: dep[:, lanes_of(m)], lambda: dep[:, W:], i)]

            def load(j):
                if j == 0:
                    sent = [main[t, f, :, lanes_of(i)] for f in range(3)]
                else:
                    sent = [
                        beside(lambda m: main[t, f, :, lanes_of(m)], lambda: unpack(halo[t, f // per], f), i)
                        for f in range(3)
                    ]
                return [cur[j][f] + sent[f] for f in range(3)], depths[j]

            def visit(j, before, tile, after):
                for f in range(3):
                    value = cur[j][f] + (
                        column_sum(before, tile, after, f, tall) + shift_up(tile.ups[f]) + shift_down(tile.downs[f])
                    )
                    state[i, f, :, lanes_of(j)] = value
                    if j == 0:
                        for yo in range(SP):
                            cs[i, t * SP + yo, f] = value[yo * RL : (yo + 1) * RL]
                            below, above = (yo + 1) * RL % R, (yo * RL - 1) % R
                            eo[i, t * SP + yo, 0, f] = tile.ups[f][below : below + 1]
                            eo[i, t * SP + yo, 1, f] = tile.downs[f][above : above + 1]

            walk(load, range(2), 2, visit)

            @pl.when(jnp.logical_and(t > 0, block == NG - 1))
            def _():
                give(i, t - 1)

            return carried

        @pl.when(block == 0)
        def _():
            whole(ini, ini_r)
            for i in range(NS):
                for f in range(3):
                    state[i, f, :, :LANES] = ini[f, :, lanes_of(i)]
                    state[i, f, :, LANES:] = beside(lambda m: ini[f, :, lanes_of(m)], lambda: ini[f, :, W:], i)

        for i in range(NS):
            @pl.when(block > 0)
            def _():
                for copy in carry(i):
                    copy.wait_recv()
                give_begin(i, 0, cin.at[i])
                for f in range(3):
                    for yo in range(SP):
                        state[i, f, yo * RL : (yo + 1) * RL, :LANES] = cin[i, yo, f]
                    for r in range(2):
                        slot = 2 * f + r
                        tile = chalo[i, slot // carry_slots]
                        if slot % carry_slots:
                            tile = pltpu.roll(tile, LANES - 2 * carry_hw * (slot % carry_slots), 1)
                        state[i, f, r * R // 2 : (r + 1) * R // 2, LANES:] = tile

            lax.fori_loop(0, TG, functools.partial(turn, i), 0)

            @pl.when(block == NG - 1)
            def _():
                give(i, TG - 1)

            @pl.when(block < NG - 1)
            def _():
                for e in range(chalo.shape[1]):
                    packed = jnp.zeros((R // 2, LANES), jnp.float32)
                    for slot in range(e * carry_slots, min(6, (e + 1) * carry_slots)):
                        f, r = slot // 2, slot % 2
                        z = state[i, f, r * R // 2 : (r + 1) * R // 2, LANES:]
                        if slot % carry_slots:
                            z = pltpu.roll(z, 2 * carry_hw * (slot % carry_slots), 1)
                        packed = jnp.where(slots == slot % carry_slots, z, packed)
                    chalo_src[i, e] = packed
                if i == 0:
                    pl.semaphore_wait(go_carry, 1)
                for copy in carry(i):
                    copy.start()

        @pl.when(block < NG - 1)
        def _():
            @pl.loop(0, TG)
            def _(t):
                for i in range(NS):
                    give(i, t)

    part = NX // PARTS

    def fwd(q):
        cols = pl.ds(q * part, part)
        return pltpu.make_async_remote_copy(
            src_ref=ce.at[:, :, cols], dst_ref=cb.at[:, :, cols],
            send_sem=fwd_s, recv_sem=fwd_r.at[q], device_id=(lax.rem(p + 1, T), y), device_id_type=MESH,
        )

    whole(redge, ret_r)

    @pl.when(p == 0)
    def _():
        cb[...] = init_ref[...]

    @pl.when(late)
    def _():
        whole(cb, beg_r)

    per_part = NT // PARTS

    def advance(q, made, visit_ends):
        def load(j):
            return [cb[f, :, lanes_of(j)] + b[f, :, lanes_of(j)] for f in range(3)], depth_ref[:, lanes_of(j)]

        def visit(j, before, tile, after):
            cols = lanes_of(j)
            visit_ends(cols, [
                cb[f, :, cols] + column_sum(before, tile, after, f, lane)
                + jnp.where(row == RL - 1, redge[0, f, :, cols], shift_up(tile.ups[f]))
                + jnp.where(row == 0, redge[1, f, :, cols], shift_down(tile.downs[f]))
                for f in range(3)
            ])

        walk(load, range(q * per_part, (q + 1) * per_part), NT, visit, made)

    def keep(cols, ends):
        for f in range(3):
            ce[f, :, cols] = ends[f]

    def emit(cols, ends):
        for f in range(3):
            start = cb[f, :, cols]
            out_ref[0, 0, f, :, cols] = start
            out_ref[0, 1, f, :, cols] = mid[f, :, cols] + 0.5 * (start + ends[f])
            out_ref[0, 2, f, :, cols] = ends[f]

    order = [PARTS - 1, *range(PARTS - 1)]

    @pl.when(even)
    def _():
        made = {}
        for q in order:
            advance(q, made, keep)
            fwd(q).start()
        for j in range(NT):
            emit(lanes_of(j), [ce[f, :, lanes_of(j)] for f in range(3)])
        whole(ce, fwd_s)

    @pl.when(odd)
    def _():
        made, arrived = {}, 0
        for q in range(PARTS):
            while arrived < min(q + 3, PARTS):
                fwd(order[arrived]).wait_recv()
                arrived += 1
            advance(q, made, emit)

    @pl.when(p < T - 1)
    def _():
        whole(u_ref.at[2], shift_s)

    @pl.when(late)
    def _():
        for side in range(sides):
            depth_halo(side).wait_send()
            whole(rsrc, rel_s.at[side])

    whole(esrc, edge_s)
    for yo in range(SP):
        flat = pb * SP + yo

        @pl.when(jnp.logical_and(lax.rem(flat, stride) == 0, yo != y))
        def _():
            dep_copy(yo).wait_send()

            @pl.when(block == 0)
            def _():
                ini_copy(yo).wait_send()

    @pl.when(is_owner)
    def _():
        whole(b.at[:, :, pl.ds(0, (K - 1) * W)], a2a_s.at[0])
        whole(halo_src.at[:, :, pl.ds(0, (K - 1) * LANES)], a2a_s.at[1])
        for i in range(NS):
            whole(eo.at[i, pl.ds(0, TG * SP - 1)], ret_s)

        @pl.when(block < NG - 1)
        def _():
            for i in range(NS):
                for copy in carry(i):
                    copy.wait_send()

        own = jnp.logical_and(even, p > 0).astype(jnp.int32)
        begins = (TG + 1) // 2 * SP - own - jnp.where(block == 0, SP, 0)
        for n in ((TG + 1) // 2 * SP - a - c for a in range(2) for c in (0, SP)):
            @pl.when(begins == n)
            def _():
                for i in range(NS):
                    whole(cs.at[i, pl.ds(0, n)], beg_s)

    @pl.when(jnp.logical_not(is_owner))
    def _():
        whole(b, a2a_s.at[0])
        whole(halo_src, a2a_s.at[1])


def solution(mesh):
    T, SP = mesh.shape["tm"], mesh.shape["space"]

    def per_device(fine_nodes, init_state, mean_depth):
        RL, NX = mean_depth.shape
        NG = 2 if T % 4 == 0 else 1
        members = T // NG * SP
        W = max(LANES, NX // members)
        K = NX // W
        NC = CHUNKS if K % CHUNKS == 0 else 1
        stride = members // K
        hw = 8
        while hw < T:
            hw *= 2
        per = LANES // (2 * hw)
        nh = -(-3 // per)
        carry_hw = 8
        while carry_hw < T // NG:
            carry_hw *= 2
        carried = -(-6 * 2 * carry_hw // LANES)
        cfg = (T, SP, RL, NX, W, K, stride, hw, per, nh, NG, NC, carry_hw)
        f32, dma = jnp.float32, pltpu.SemaphoreType.DMA
        state = pltpu.VMEM((3, RL, NX), f32)
        R = RL * SP
        sides = 1 if SP == 2 else 2
        edges = pltpu.VMEM((2, 2, 3, 1, NX), f32)
        vmem = pl.BlockSpec(memory_space=pltpu.VMEM)
        return pl.pallas_call(
            functools.partial(kernel, cfg),
            out_shape=pltpu.VMEM(fine_nodes.shape, f32),
            in_specs=[pl.BlockSpec(memory_space=pl.ANY)] * 3,
            out_specs=vmem,
            scratch_shapes=[
                pltpu.VMEM((3, 3, RL, NX), f32), state, pltpu.VMEM((RL, NX), f32),
                state, state, state, state, state, state,
                pltpu.VMEM((nh, RL, K * LANES), f32),
                pltpu.VMEM((3, 2 * DEEP, NX), f32),
                pltpu.VMEM((sides, 3, 2 * DEEP, NX), f32),
                pltpu.VMEM((2 * DEEP, NX), f32),
                pltpu.VMEM((sides, 2 * DEEP, NX), f32),
                pltpu.VMEM((SP, RL, W + LANES), f32),
                pltpu.VMEM((R, W + LANES), f32),
                pltpu.VMEM((SP, 3, RL, W + LANES), f32),
                pltpu.VMEM((3, R, W + LANES), f32),
                pltpu.VMEM((T // NG, 3, R, W), f32),
                pltpu.VMEM((T // NG, nh, R, LANES), f32),
                pltpu.VMEM((W // LANES, members, 3, RL, LANES), f32),
                state, state,
                edges, edges,
                pltpu.VMEM((W // LANES, members, 2, 3, 1, LANES), f32),
                pltpu.VMEM((2, 3, 1, NX), f32),
                pltpu.VMEM((W // LANES, SP, 3, RL, LANES), f32),
                pltpu.VMEM((W // LANES, carried, R // 2, LANES), f32),
                pltpu.VMEM((W // LANES, carried, R // 2, LANES), f32),
                pltpu.VMEM((W // LANES, 3, R, 2 * LANES), f32),
                dma, dma((NC,)), dma((sides,)), dma((sides, NC)), dma((sides,)), dma((sides,)),
                dma, dma((2, SPANS)), dma((SP,)), dma, dma((SP,)), dma, dma((2,)), dma((2, T // NG)),
                dma, dma, dma, dma((PARTS,)),
                dma((W // LANES, 2)), dma((W // LANES, 2)), dma, dma, dma((5,)),
                pltpu.SemaphoreType.REGULAR,
            ],
            compiler_params=pltpu.CompilerParams(
                collective_id=0, has_side_effects=True, vmem_limit_bytes=60 * 1024 * 1024
            ),
        )(fine_nodes, init_state, mean_depth)

    return jax.shard_map(
        per_device,
        mesh=mesh,
        in_specs=(P("tm", None, None, "space", None), P(None, "space", None), P("space", None)),
        out_specs=P("tm", None, None, "space", None),
        check_vma=False,
    )
```
